256 devices in a mesh: groups: 2 (over z), seq: 128 (over x, y, core).
Axes of the slice: x: 8, y: 8, z: 2, core: 2. Of those that a mesh axis runs over, the one named last changes fastest.
The devices are a block of a 8x8x16 slice.
Arguments:
- latents: bfloat16 [2048, 64, 640], P(('groups', 'seq')), parts along dimension 0, may hold values from -6 to 6
- norm_gain: float32 [640], replicated, may hold values from 0.25 to 1.75
- norm_bias: float32 [640], replicated, may hold values from -3 to 3
- conv_weight: bfloat16 [5760, 640], P('seq'), may hold values from -0.078125 to 0.078125
- time_weight: bfloat16 [320, 640], replicated, may hold values from -0.3125 to 0.3125
- first_gain: float32 [640], replicated, may hold values from 0.25 to 1.75
- tconv_weight: bfloat16 [1920, 640], P('seq'), may hold values from -0.125 to 0.125
- second_gain: float32 [640], replicated, may hold values from 0.25 to 1.75
- qkv_weight: bfloat16 [640, 1920], P('seq'), may hold values from -0.25 to 0.25
- out_weight: bfloat16 [640, 640], P('seq'), may hold values from -0.25 to 0.25
- timesteps: int32 [8], P('groups'), parts along dimension 0, may hold values from 0 to 999
Outputs:
- mixed: bfloat16 [2048, 64, 640], P(('groups', 'seq')), parts along dimension 0
The draws below stay inside these ranges and needn't reach their ends.
There are 2 independent parts, one for each index of `groups`. The reference program is written for one: setup_inputs(seed, part) draws one part's arguments, and reference() takes and returns one part's arrays. A program takes and returns all parts, laid end to end along the dimension named above; an argument that names none is the same for every part. Nothing has to cross between parts.
All inputs are finite; a program needn't handle non-finite values.
Results may differ from the reference program's by a relative error of at most 0.008.
Values may be sent and summed in bfloat16 or wider, within the bound.
No kernel may reach another device: no remote copies, remote signals or barrier semaphores. Data moves between devices by JAX's collectives and lax.ppermute only.
A program may use at most 128 MiB of HBM per device.

```python
import jax
import jax.numpy as jnp
from jax import lax

C = 640
HEAD = 64
GROUPS = 32
TFEAT = 320
FRAMES = 16
W = 64
ROWS_DEV = 8
CLIPS = 4
SPLIT = 2
H = 16
IMAGES = 64


def set_ends(drawn, key, low, top_value):
    longest = drawn.shape.index(max(drawn.shape))
    spots = []
    for shift in (0, 1):
        where = [jax.random.randint(jax.random.fold_in(key, axis), (), 0, length) for axis, length in enumerate(drawn.shape)]
        where[longest] = (where[longest] + shift) % drawn.shape[longest]
        spots.append(tuple(where))
    return drawn.at[spots[0]].set(low).at[spots[1]].set(top_value)


def block_scale(stream_key, shape, split, low, top_value):
    loudness = 1.0
    for axis_at, blocks in split:
        steps = jax.random.uniform(jax.random.fold_in(jax.random.fold_in(stream_key, 6), axis_at), (blocks,), jnp.float32, low / len(split), top_value / len(split))
        loudness = loudness * jnp.repeat(jnp.exp(steps), shape[axis_at] // blocks).reshape((-1,) + (1,) * (len(shape) - 1 - axis_at))
    return loudness


def bell_draw(stream_key, dims, deviation, limit, shards=(), held_as=jnp.bfloat16):
    array = jax.random.normal(stream_key, dims, jnp.float32) * deviation
    if len(shards) > 0:
        array = block_scale(stream_key, dims, shards, -0.22, 0.18) * array
    return jnp.clip(array, min=-limit, max=limit).astype(held_as)


def setup_inputs(seed: int = 0, part: int = 0) -> dict:
    arg_keys = jax.random.split(jax.random.key(seed), 12)
    own_keys = jax.random.split(jax.random.fold_in(arg_keys[11], part), 12)
    return {
        "latents": bell_draw(own_keys[0], (IMAGES * H, W, C), 1.0, 6.0, ((0, 128),)),
        "norm_gain": jnp.clip(1.0 + 0.15 * jax.random.normal(arg_keys[1], (C,), jnp.float32), 0.25, 1.75),
        "norm_bias": bell_draw(arg_keys[2], (C,), 0.5, 3.0, (), jnp.float32),
        "conv_weight": bell_draw(arg_keys[3], (9 * C, C), (9 * C) ** -0.5, 0.078125, ((0, 128),)),
        "time_weight": bell_draw(arg_keys[4], (TFEAT, C), TFEAT ** -0.5, 0.3125),
        "first_gain": jnp.clip(1.0 + 0.15 * jax.random.normal(arg_keys[5], (C,), jnp.float32), 0.25, 1.75),
        "tconv_weight": bell_draw(arg_keys[6], (3 * C, C), (3 * C) ** -0.5, 0.125, ((0, 128),)),
        "second_gain": jnp.clip(1.0 + 0.15 * jax.random.normal(arg_keys[7], (C,), jnp.float32), 0.25, 1.75),
        "qkv_weight": bell_draw(arg_keys[8], (C, 3 * C), C ** -0.5, 0.25, ((0, 128),)),
        "out_weight": bell_draw(arg_keys[9], (C, C), C ** -0.5, 0.25, ((0, 128),)),
        "timesteps": set_ends(jax.random.randint(own_keys[10], (CLIPS,), 0, 1000), jax.random.fold_in(own_keys[10], 1), 0, 999).astype(jnp.int32),
    }


def time_embed(timesteps, time_weight):
    half = TFEAT // 2
    freqs = jnp.exp(-jnp.log(10000.0) * jnp.arange(half, dtype=jnp.float32) / half)
    angles = timesteps.astype(jnp.float32)[:, None] * freqs[None, :]
    feats = jnp.concatenate([jnp.cos(angles), jnp.sin(angles)], axis=-1)
    return jnp.dot(feats, time_weight.astype(jnp.float32), precision=lax.Precision.HIGHEST)

def layer_norm(values):
    mean = lax.optimization_barrier(jnp.mean(values, axis=-1, keepdims=True))
    centered = values - mean
    var = lax.optimization_barrier(jnp.mean(centered * centered, axis=-1, keepdims=True))
    return centered * lax.rsqrt(var + 1e-05)

def temporal_block(spatial, first_gain, tconv_weight, second_gain, qkv_weight, out_weight):
    clips, frames, places, chans = spatial.shape
    heads = chans // HEAD
    values = spatial.astype(jnp.float32)
    first = (layer_norm(values) * first_gain).astype(jnp.bfloat16)
    zero = jnp.zeros_like(first[:, :1])
    before = jnp.concatenate([zero, first[:, :-1]], axis=1)
    after = jnp.concatenate([first[:, 1:], zero], axis=1)
    stacked = jnp.concatenate([before, first, after], axis=-1).reshape(-1, 3 * chans)
    mid = values + jnp.dot(stacked, tconv_weight, preferred_element_type=jnp.float32).reshape(values.shape)
    second = (layer_norm(mid) * second_gain).astype(jnp.bfloat16)
    qkv = jnp.dot(second.reshape(-1, chans), qkv_weight, preferred_element_type=jnp.float32).astype(jnp.bfloat16)
    qkv = qkv.reshape(clips, frames, places, 3, heads, HEAD).astype(jnp.float32)
    query, key, value = (qkv[:, :, :, 0], qkv[:, :, :, 1], qkv[:, :, :, 2])
    scores = jnp.einsum('cfphd,cgphd->cphfg', query, key) * HEAD ** (-0.5)
    weights = jax.nn.softmax(scores, axis=-1).astype(jnp.bfloat16).astype(jnp.float32)
    attended = jnp.einsum('cphfg,cgphd->cfphd', weights, value).astype(jnp.bfloat16)
    projected = jnp.dot(attended.reshape(-1, chans), out_weight, preferred_element_type=jnp.float32)
    return (mid + projected.reshape(mid.shape)).astype(jnp.bfloat16)

def reference(latents, norm_gain, norm_bias, conv_weight, time_weight, first_gain, tconv_weight, second_gain, qkv_weight, out_weight, timesteps):
    images = CLIPS * FRAMES
    tiled = latents.reshape(SPLIT, images, ROWS_DEV, W, C)
    frames_in = jnp.transpose(tiled, (1, 0, 2, 3, 4)).reshape(images, H, W, C)
    temb = time_embed(timesteps, time_weight)
    temb_rows = temb[jnp.arange(images) // FRAMES]

    def spatial_one(inputs):
        image, bias_row = inputs
        values = image.astype(jnp.float32).reshape(H * W, GROUPS, C // GROUPS)
        mean = lax.optimization_barrier(jnp.mean(values, axis=(0, 2)))
        var = lax.optimization_barrier(jnp.mean(values * values, axis=(0, 2))) - mean * mean
        normed = (values - mean[None, :, None]) * lax.rsqrt(var + 1e-05)[None, :, None]
        normed = normed.reshape(H, W, C) * norm_gain + norm_bias
        normed = jax.nn.silu(normed).astype(jnp.bfloat16)
        padded = jnp.pad(normed, ((1, 1), (1, 1), (0, 0)))
        taps = [padded[dy:dy + H, dx:dx + W] for dy in range(3) for dx in range(3)]
        columns = jnp.concatenate(taps, axis=-1).reshape(H * W, 9 * C)
        conv = jnp.dot(columns, conv_weight, preferred_element_type=jnp.float32)
        return (image.reshape(H * W, C).astype(jnp.float32) + conv + bias_row[None, :]).astype(jnp.bfloat16)
    spatial = lax.map(spatial_one, (frames_in, temb_rows)).reshape(CLIPS, FRAMES, H * W, C)

    def temporal_one(clip_rows):
        return temporal_block(clip_rows[None], first_gain, tconv_weight, second_gain, qkv_weight, out_weight)[0]
    mixed = lax.map(temporal_one, spatial).reshape(images, SPLIT, ROWS_DEV, W, C)
    return jnp.transpose(mixed, (1, 0, 2, 3, 4)).reshape(images * H, W, C)
```

```python
import jax
import jax.numpy as jnp
from jax import lax
from jax.experimental import pallas as pl
from jax.experimental.pallas import tpu as pltpu
from jax.sharding import Mesh
from jax.sharding import PartitionSpec as P

HEAD = 64
GROUPS = 32
TFEAT = 320
FRAMES = 16
SEQ = ("seq_0", "seq_1", "seq_2")
GROUPS_SEQ = ("groups", "seq_0", "seq_1", "seq_2")
SIDE = 8
CONV_BLOCK = 48
TCONV_BLOCK = 16
VMEM_LIMIT = 56 * 2**20
OFFSETS = (0, -1, -2, -3, -4, 1, 2, 3)
FIRST_SWAP = (0, 1, 2, 5, 6)
SECOND_SWAP = (3, 4, 7)


def route(target):
    pairs = []
    for x in range(SIDE):
        for y in range(SIDE):
            for core in range(2):
                there = target(x, y, core)
                if there is not None:
                    tx, ty, tcore = there
                    to = (tx % SIDE * SIDE + ty % SIDE) * 2 + tcore
                    pairs.append(((x * SIDE + y) * 2 + core, to))
    return pairs


def send(block, target):
    return lax.ppermute(block, SEQ, route(target))


def inner(step):
    return lambda x, y, core: (x + step, y, core) if core == 0 else (x, y + step, core)


def outer(step):
    return lambda x, y, core: (x, y + step, core) if core == 0 else (x + step, y, core)


def swap(x, y, core):
    return x, y, 1 - core


def ring(block, towards):
    ahead, behind = [block], [block]
    for step in range(SIDE // 2):
        ahead.append(send(ahead[-1], towards(1)))
        if step < SIDE // 2 - 1:
            behind.append(send(behind[-1], towards(-1)))
    return ahead + behind[1:]


def time_embed(timestep, time_weight):
    half = TFEAT // 2
    freqs = jnp.exp(-jnp.log(10000.0) * jnp.arange(half, dtype=jnp.float32) / half)
    angles = timestep.astype(jnp.float32)[None, None] * freqs[None, :]
    feats = jnp.concatenate([jnp.cos(angles), jnp.sin(angles)], axis=-1)
    return jnp.dot(feats, time_weight.astype(jnp.float32), precision=lax.Precision.HIGHEST)


def wrap(value):
    return lax.rem(value + 2 * SIDE, SIDE)


def offset_of(slot):
    return jnp.where(slot <= SIDE // 2, -slot, slot - SIDE // 2)


def piece_refs(mine, first, second):
    other = {}
    for i, at in enumerate(FIRST_SWAP):
        other[at] = first.at[i]
    for i, at in enumerate(SECOND_SWAP):
        other[at] = second.at[i]
    return [(0, i, mine[i]) for i in range(SIDE)] + [(1, i, other[i]) for i in range(SIDE)]


def fetch_blocks(where, pieces, weight, size, sem):
    x, y, core = where[0], where[1], where[2]
    for swapped, slot, ref in pieces:
        holder = core if swapped == 0 else 1 - core
        across = OFFSETS[slot]

        def one(b, carry, ref=ref, holder=holder, across=across):
            along = offset_of(b)
            px = wrap(x + jnp.where(holder == 0, along, across))
            py = wrap(y + jnp.where(holder == 0, across, along))
            inside = 2 * py + holder

            @pl.when(inside < 2 * SIDE - 1)
            def _():
                at = pl.multiple_of((px * (2 * SIDE - 1) + inside) * size, size)
                source = ref.at[pl.ds(pl.multiple_of(b * size, size), size)]
                pltpu.make_async_copy(source, weight.at[pl.ds(at, size)], sem).start()

            return carry

        lax.fori_loop(0, SIDE, one, 0)


def conv_kernel(where, latents, halo, vectors, *refs):
    mine, (first, second, out, weight, shifted, total, sem) = refs[:SIDE], refs[SIDE:]
    fetch_blocks(where, piece_refs(mine, first, second), weight, CONV_BLOCK, sem)
    rows, width, chans = latents.shape
    mean, scale, bias = vectors[0:1, :], vectors[1:2, :], vectors[2:3, :]
    column = lax.broadcasted_iota(jnp.int32, (width, 1), 0)
    lower = where[3]

    def fill(at, raw):
        values = (raw.astype(jnp.float32) - mean) * scale + bias
        values = values / (1.0 + jnp.exp(-values))
        left = jnp.where(column == 0, 0.0, pltpu.roll(values, 1, 0))
        right = jnp.where(column == width - 1, 0.0, pltpu.roll(values, width - 1, 0))
        shifted[0, at] = left.astype(jnp.bfloat16)
        shifted[1, at] = values.astype(jnp.bfloat16)
        shifted[2, at] = right.astype(jnp.bfloat16)

    def one_row(r, carry):
        fill(r + 1, latents[r])
        return carry

    lax.fori_loop(0, rows, one_row, 0)
    fill(jnp.where(lower == 1, 0, rows + 1), halo[0])
    empty = jnp.where(lower == 1, rows + 1, 0)
    for dx in range(3):
        shifted[dx, empty] = jnp.zeros((width, chans), jnp.bfloat16)
    pltpu.make_async_copy(weight, weight, sem).wait()
    for tap in range(9):
        dy, dx = divmod(tap, 3)
        taken = shifted[dx, dy : dy + rows].reshape(rows * width, chans)
        part = jnp.dot(
            taken,
            weight[tap * chans : (tap + 1) * chans, :],
            preferred_element_type=jnp.float32,
        )
        if tap == 0:
            total[...] = part
        elif tap < 8:
            total[...] += part
        else:
            base = latents[...].astype(jnp.float32).reshape(rows * width, chans)
            out[...] = (base + (total[...] + part) + vectors[3:4, :]).astype(jnp.bfloat16)


def layer_norm(values):
    mean = jnp.mean(values, axis=-1, keepdims=True)
    centered = values - mean
    var = jnp.mean(centered * centered, axis=-1, keepdims=True)
    return centered * lax.rsqrt(var + 1e-05)


def temporal_kernel(where, moved, gains, *refs):
    mine = refs[:SIDE]
    first_swap, second_swap, out, tconv, dense, mid, qkv, attended, sem, dense_sem = refs[SIDE:]
    x, y, core = where[0], where[1], where[2]
    frames, places, chans = moved.shape
    pieces = piece_refs(mine, first_swap, second_swap)
    fetch_blocks(where, pieces, tconv, TCONV_BLOCK, sem)
    share = chans // SIDE
    for swapped, slot, ref in pieces:
        holder = core if swapped == 0 else 1 - core
        at = wrap(jnp.where(holder == 0, y, x) + OFFSETS[slot])
        for m in range(2):
            source = ref.at[pl.ds(SIDE * TCONV_BLOCK + m * share, share)]
            target = dense.at[2 * holder + m, pl.ds(pl.multiple_of(at * share, 16), share)]
            pltpu.make_async_copy(source, target, dense_sem).start()
    rows = frames * places
    values = moved[...].astype(jnp.float32).reshape(rows, chans)
    first = (layer_norm(values) * gains[0:1, :]).astype(jnp.bfloat16)
    zero = jnp.zeros((places, chans), jnp.bfloat16)
    before = jnp.concatenate([zero, first[:-places]], axis=0)
    after = jnp.concatenate([first[places:], zero], axis=0)
    pltpu.make_async_copy(tconv, tconv, sem).wait()
    mid[...] = values + jnp.dot(
        before, tconv[:chans, :], preferred_element_type=jnp.float32
    )
    mid[...] += jnp.dot(first, tconv[chans : 2 * chans, :], preferred_element_type=jnp.float32)
    mid[...] += jnp.dot(after, tconv[2 * chans :, :], preferred_element_type=jnp.float32)
    second = (layer_norm(mid[...]) * gains[1:2, :]).astype(jnp.bfloat16)
    pltpu.make_async_copy(dense, dense, dense_sem).wait()
    for m in range(3):
        part = jnp.dot(second, dense[m], preferred_element_type=jnp.float32)
        qkv[m] = part.astype(jnp.bfloat16).reshape(frames, places, chans)
    some = 16
    many = frames * some
    row_place = lax.broadcasted_iota(jnp.int32, (many, many), 0) % some
    col_place = lax.broadcasted_iota(jnp.int32, (many, many), 1) % some
    same = row_place == col_place
    lane = lax.broadcasted_iota(jnp.int32, (1, 2 * HEAD), 1)
    for group in range(places // some):
        spot = slice(group * some, (group + 1) * some)
        for pair in range(chans // (2 * HEAD)):
            lanes = slice(pair * 2 * HEAD, (pair + 1) * 2 * HEAD)
            query = qkv[0, :, spot, lanes].reshape(many, 2 * HEAD)
            key = qkv[1, :, spot, lanes].reshape(many, 2 * HEAD)
            value = qkv[2, :, spot, lanes].reshape(many, 2 * HEAD)
            both = []
            for side in range(2):
                own = (lane < HEAD) if side == 0 else (lane >= HEAD)
                only = jnp.where(own, query, jnp.zeros_like(query))
                scores = lax.dot_general(
                    only, key, (((1,), (1,)), ((), ())), preferred_element_type=jnp.float32
                )
                scores = jnp.where(same, scores * HEAD ** (-0.5), -1e30)
                top = jnp.max(scores, axis=-1, keepdims=True)
                raised = jnp.exp(scores - top)
                weights = raised / jnp.sum(raised, axis=-1, keepdims=True)
                both.append(
                    jnp.dot(weights.astype(jnp.bfloat16), value, preferred_element_type=jnp.float32)
                )
            mixed = jnp.where(lane < HEAD, both[0], both[1]).astype(jnp.bfloat16)
            attended[:, spot, lanes] = mixed.reshape(frames, some, 2 * HEAD)
    projected = jnp.dot(
        attended[...].reshape(rows, chans), dense[3], preferred_element_type=jnp.float32
    )
    out[...] = (mid[...] + projected).astype(jnp.bfloat16).reshape(frames, places, chans)


def specs(count):
    return [pl.BlockSpec(memory_space=pl.ANY)] * count


def shards(
    latents,
    norm_gain,
    norm_bias,
    conv_weight,
    time_weight,
    first_gain,
    tconv_weight,
    second_gain,
    qkv_weight,
    out_weight,
    timesteps,
):
    devices = lax.axis_size(SEQ)
    device = lax.axis_index(SEQ)
    x, y, core = (lax.axis_index(name) for name in SEQ)
    clips = timesteps.shape[0]
    images = clips * FRAMES
    sharing = devices // images
    rows, width, chans = latents.shape
    height = sharing * rows
    image = device % images
    clip = image // FRAMES
    lower = device // images
    bf16, f32 = jnp.bfloat16, jnp.float32

    conv_rows, tconv_rows = conv_weight.shape[0], tconv_weight.shape[0]
    both = jnp.concatenate([conv_weight, tconv_weight], axis=0)

    def to_previous(px, py, pcore):
        spot = 2 * py + pcore - 1
        return None if spot < 0 else (px, spot // 2, spot % 2)

    following = send(both, to_previous)
    inside = 2 * y + core
    conv_two = jnp.concatenate([both[:conv_rows], following[:conv_rows]], axis=0)
    tconv_two = jnp.concatenate([both[conv_rows:], following[conv_rows:]], axis=0)
    conv_at = jnp.minimum((CONV_BLOCK - conv_rows) * inside, 2 * conv_rows - CONV_BLOCK)
    tconv_at = jnp.minimum((TCONV_BLOCK - tconv_rows) * inside, 2 * tconv_rows - TCONV_BLOCK)
    conv_block = lax.dynamic_slice_in_dim(conv_two, conv_at, CONV_BLOCK, 0)
    tconv_block = lax.dynamic_slice_in_dim(tconv_two, tconv_at, TCONV_BLOCK, 0)

    few = qkv_weight.shape[0]
    query_key = jnp.concatenate([qkv_weight[:, :chans], qkv_weight[:, chans : 2 * chans]], axis=0)
    value_out = jnp.concatenate([qkv_weight[:, 2 * chans :], out_weight], axis=0)
    same_core = send(query_key, lambda px, py, pcore: (py, px, 0) if pcore == 0 else None)
    crossed = send(
        jnp.where(core == 0, value_out, query_key),
        lambda px, py, pcore: (px, py, 1) if pcore == 0 else (py, px, 0),
    )
    from_even = jnp.where(core == 0, same_core, crossed).reshape(2, few, chans)
    from_odd = jnp.where(core == 0, crossed, value_out).reshape(2, few, chans)
    dense_block = jnp.concatenate([from_even, from_odd], axis=1).reshape(4 * few, chans)

    pairs = [(i, (i + images) % devices) for i in range(devices)]
    edge = lax.dynamic_slice_in_dim(latents, jnp.where(lower == 1, 0, rows - 1), 1, 0)
    halo = lax.ppermute(edge, SEQ, pairs)
    values = latents.astype(f32).reshape(rows * width, chans)
    sums = jnp.stack([jnp.sum(values, axis=0), jnp.sum(values * values, axis=0)])
    sums = jnp.sum(sums.reshape(2, GROUPS, chans // GROUPS), axis=2)
    sums = sums + lax.ppermute(sums, SEQ, pairs)
    entries = height * width * (chans // GROUPS)
    mean = sums[0] / entries
    var = sums[1] / entries - mean * mean
    spread = lax.rsqrt(var + 1e-05)
    wide = lambda v: jnp.repeat(v, chans // GROUPS)
    temb = time_embed(lax.dynamic_index_in_dim(timesteps, clip, 0, False), time_weight)
    vectors = jnp.stack([wide(mean), wide(spread) * norm_gain, norm_bias, temb[0]])

    line = jnp.stack(ring(jnp.concatenate([conv_block, tconv_block, dense_block], axis=0), inner))
    order = jnp.array([OFFSETS.index((k + 4) % SIDE - 4) for k in range(SIDE)])
    along = jnp.where(core == 0, x, y)
    conv_line = line[:, :CONV_BLOCK].reshape(SIDE * CONV_BLOCK, chans)
    conv_pieces = ring(conv_line, outer)
    conv_first = send(jnp.stack([conv_pieces[i] for i in FIRST_SWAP]), swap)
    conv_second = send(jnp.stack([conv_pieces[i] for i in SECOND_SWAP]), swap)
    tconv_line = line[:, CONV_BLOCK : CONV_BLOCK + TCONV_BLOCK].reshape(SIDE * TCONV_BLOCK, chans)
    sorted_line = jnp.take(line[:, CONV_BLOCK + TCONV_BLOCK :], order[(jnp.arange(SIDE) - along) % SIDE], axis=0)
    sorted_line = sorted_line.reshape(SIDE, 2, 2 * few, chans)
    dense_line = jnp.transpose(sorted_line, (1, 0, 2, 3)).reshape(4 * few * SIDE, chans)
    rest_line = jnp.concatenate([tconv_line, dense_line], axis=0)
    rest_line, _ = lax.optimization_barrier((rest_line, conv_pieces[4]))
    rest_pieces = ring(rest_line, outer)
    rest_first = send(jnp.stack([rest_pieces[i] for i in FIRST_SWAP]), swap)
    rest_second = send(jnp.stack([rest_pieces[i] for i in SECOND_SWAP]), swap)

    where = jnp.stack([x, y, core, lower]).astype(jnp.int32)
    smem = pl.BlockSpec(memory_space=pltpu.SMEM)
    vmem = pl.BlockSpec(memory_space=pltpu.VMEM)
    params = pltpu.CompilerParams(vmem_limit_bytes=VMEM_LIMIT)
    spatial = pl.pallas_call(
        conv_kernel,
        out_shape=jax.ShapeDtypeStruct((rows * width, chans), bf16),
        in_specs=[smem, vmem, vmem, vmem] + specs(SIDE + 2),
        out_specs=vmem,
        scratch_shapes=[
            pltpu.VMEM((9 * chans, chans), bf16),
            pltpu.VMEM((3, rows + 2, width, chans), bf16),
            pltpu.VMEM((rows * width, chans), f32),
            pltpu.SemaphoreType.DMA,
        ],
        compiler_params=params,
        name="conv",
    )(where, latents, halo, vectors, *conv_pieces, conv_first, conv_second)
    moved = lax.all_to_all(spatial, SEQ[1:], split_axis=0, concat_axis=0, tiled=True)
    places = rows * width // FRAMES
    result = pl.pallas_call(
        temporal_kernel,
        out_shape=jax.ShapeDtypeStruct((FRAMES, places, chans), bf16),
        in_specs=[smem, vmem, vmem] + specs(SIDE + 2),
        out_specs=vmem,
        scratch_shapes=[
            pltpu.VMEM((3 * chans, chans), bf16),
            pltpu.VMEM((4, chans, chans), bf16),
            pltpu.VMEM((FRAMES * places, chans), f32),
            pltpu.VMEM((3, FRAMES, places, chans), bf16),
            pltpu.VMEM((FRAMES, places, chans), bf16),
            pltpu.SemaphoreType.DMA,
            pltpu.SemaphoreType.DMA,
        ],
        compiler_params=params,
        name="temporal",
    )(
        where,
        moved.reshape(FRAMES, places, chans),
        jnp.stack([first_gain, second_gain]),
        *rest_pieces,
        rest_first,
        rest_second,
    )
    returned = lax.all_to_all(
        result.reshape(rows * width, chans), SEQ[1:], split_axis=0, concat_axis=0, tiled=True
    )
    return returned.reshape(rows, width, chans)


def solution(mesh):
    torus = Mesh(
        mesh.devices.reshape(mesh.shape["groups"], SIDE, SIDE, 2),
        ("groups", "seq_0", "seq_1", "seq_2"),
    )
    return jax.shard_map(
        shards,
        mesh=torus,
        in_specs=(
            P(GROUPS_SEQ, None, None),
            P(),
            P(),
            P(SEQ, None),
            P(),
            P(),
            P(SEQ, None),
            P(),
            P(SEQ, None),
            P(SEQ, None),
            P("groups"),
        ),
        out_specs=P(GROUPS_SEQ, None, None),
        check_vma=False,
    )
```

```python
import jax
import jax.numpy as jnp
from jax import lax
from jax.experimental import pallas as pl
from jax.experimental.pallas import tpu as pltpu
from jax.sharding import Mesh
from jax.sharding import PartitionSpec as P

HEAD = 64
GROUPS = 32
TFEAT = 320
FRAMES = 16
SEQ = ("seq_0", "seq_1", "seq_2")
GROUPS_SEQ = ("groups", "seq_0", "seq_1", "seq_2")
SIDE = 8
CONV_BLOCK = 48
TCONV_BLOCK = 16
VMEM_LIMIT = 56 * 2**20
OFFSETS = (0, -1, -2, -3, -4, 1, 2, 3)


def route(target):
    pairs = []
    for x in range(SIDE):
        for y in range(SIDE):
            for core in range(2):
                there = target(x, y, core)
                if there is not None:
                    tx, ty, tcore = there
                    to = (tx % SIDE * SIDE + ty % SIDE) * 2 + tcore
                    pairs.append(((x * SIDE + y) * 2 + core, to))
    return pairs


def send(block, target):
    return lax.ppermute(block, SEQ, route(target))


def inner(step):
    return lambda x, y, core: (x + step, y, core) if core == 0 else (x, y + step, core)


def outer(step):
    return lambda x, y, core: (x, y + step, core) if core == 0 else (x + step, y, core)


def swap(x, y, core):
    return x, y, 1 - core


def ring(block, towards):
    ahead, behind = [block], [block]
    for step in range(SIDE // 2):
        ahead.append(send(ahead[-1], towards(1)))
        if step < SIDE // 2 - 1:
            behind.append(send(behind[-1], towards(-1)))
    return ahead + behind[1:]


def two_rings(blocks, towards, early):
    ahead, behind = [[b] for b in blocks], [[b] for b in blocks]
    for step in range(SIDE // 2):
        if step == 2:
            ahead[0][-1], early = lax.optimization_barrier((ahead[0][-1], early))
        for i in range(len(blocks)):
            ahead[i].append(send(ahead[i][-1], towards(1)))
            if step < SIDE // 2 - 1:
                behind[i].append(send(behind[i][-1], towards(-1)))
    pieces = [ahead[i] + behind[i][1:] for i in range(len(blocks))]
    return [own + [send(piece, swap) for piece in own] for own in pieces], early


def time_embed(timestep, time_weight):
    half = TFEAT // 2
    freqs = jnp.exp(-jnp.log(10000.0) * jnp.arange(half, dtype=jnp.float32) / half)
    angles = timestep.astype(jnp.float32)[None, None] * freqs[None, :]
    feats = jnp.concatenate([jnp.cos(angles), jnp.sin(angles)], axis=-1)
    return jnp.dot(feats, time_weight.astype(jnp.float32), precision=lax.Precision.HIGHEST)


def wrap(value):
    return lax.rem(value + 2 * SIDE, SIDE)


def offset_of(slot):
    return jnp.where(slot <= SIDE // 2, -slot, slot - SIDE // 2)


def holder_of(core, slot):
    return core if slot < SIDE else 1 - core


def fetch_blocks(where, pieces, weight, size, sems):
    x, y, core = where[0], where[1], where[2]
    for slot, ref in enumerate(pieces):
        holder = holder_of(core, slot)
        across = OFFSETS[slot % SIDE]

        def one(b, carry, ref=ref, holder=holder, across=across):
            along = offset_of(b)
            px = wrap(x + jnp.where(holder == 0, along, across))
            py = wrap(y + jnp.where(holder == 0, across, along))
            inside = 2 * py + holder

            @pl.when(inside < 2 * SIDE - 1)
            def _():
                at = pl.multiple_of((px * (2 * SIDE - 1) + inside) * size, size)
                source = ref.at[pl.ds(pl.multiple_of(b * size, size), size)]
                target = weight.at[pl.ds(at, size)]
                pltpu.make_async_copy(source, target, sems.at[px]).start()

            return carry

        lax.fori_loop(0, SIDE, one, 0)


def await_line(weight, sems, px):
    size = weight.shape[0] // SIDE
    part = weight.at[pl.ds(px * size, size)]
    pltpu.make_async_copy(part, part, sems.at[px]).wait()


def pack_kernel(where, conv, tconv, qkv, last, both, query_key, crossed, value_out, rows, few):
    conv_rows, chans = conv.shape
    count = qkv.shape[0]
    f32, bf16 = jnp.float32, jnp.bfloat16
    rows[pl.ds(0, conv_rows), :] = conv[...].astype(f32)
    rows[pl.ds(conv_rows, tconv.shape[0]), :] = tconv[...].astype(f32)
    both[...] = rows[pl.ds(0, both.shape[0]), :].astype(bf16)
    for m in range(3):
        few[pl.ds(m * count, count), :] = qkv[:, m * chans : (m + 1) * chans].astype(f32)
    few[pl.ds(3 * count, count), :] = last[...].astype(f32)
    head = few[pl.ds(0, 2 * count), :].astype(bf16)
    tail = few[pl.ds(2 * count, 2 * count), :].astype(bf16)
    query_key[...] = head
    value_out[...] = tail
    crossed[...] = jnp.where(where[2] == 0, tail.astype(f32), head.astype(f32)).astype(bf16)


def cut_kernel(where, both, following, same_core, crossed, value_out, block, conv, tconv, few):
    f32, bf16 = jnp.float32, jnp.bfloat16
    count = same_core.shape[0] // 2
    tconv_rows = TCONV_BLOCK - 1
    conv_rows = both.shape[0] - tconv_rows
    inside = 2 * where[1] + where[2]
    own, next_rows = both[...].astype(f32), following[...].astype(f32)
    conv[pl.ds(0, both.shape[0]), :] = own
    tconv[pl.ds(0, tconv_rows), :] = conv[pl.ds(conv_rows, tconv_rows), :]
    conv[pl.ds(conv_rows, both.shape[0]), :] = next_rows
    tconv[pl.ds(tconv_rows, tconv_rows), :] = conv[pl.ds(2 * conv_rows, tconv_rows), :]
    conv_at = jnp.minimum((CONV_BLOCK - conv_rows) * inside, 2 * conv_rows - CONV_BLOCK)
    tconv_at = jnp.minimum(inside, 2 * tconv_rows - TCONV_BLOCK)
    turned = pltpu.roll(conv[...], lax.rem(conv.shape[0] - conv_at, conv.shape[0]), 0)
    block[pl.ds(0, CONV_BLOCK), :] = turned[:CONV_BLOCK].astype(bf16)
    turned = pltpu.roll(tconv[...], lax.rem(tconv.shape[0] - tconv_at, tconv.shape[0]), 0)
    block[pl.ds(CONV_BLOCK, TCONV_BLOCK), :] = turned[:TCONV_BLOCK].astype(bf16)
    near, far, kept = same_core[...].astype(f32), crossed[...].astype(f32), value_out[...].astype(f32)
    even = jnp.where(where[2] == 0, near, far)
    odd = jnp.where(where[2] == 0, far, kept)
    conv[pl.ds(0, 2 * count), :] = even
    conv[pl.ds(2 * count, 2 * count), :] = odd
    for m in range(2):
        for parity in range(2):
            source = conv[pl.ds((2 * parity + m) * count, count), :]
            few[pl.ds((2 * m + parity) * count, count), :] = source
    dense = few[pl.ds(0, 4 * count), :].astype(bf16)
    block[pl.ds(CONV_BLOCK + TCONV_BLOCK, 4 * count), :] = dense


def line_kernel(where, *refs):
    pieces, (conv, rest, dense, few) = refs[:SIDE], refs[SIDE:]
    along = jnp.where(where[2] == 0, where[0], where[1])
    start = CONV_BLOCK + TCONV_BLOCK
    share = pieces[0].shape[0] - start
    half = share // 2
    for slot, piece in enumerate(pieces):
        conv[pl.ds(slot * CONV_BLOCK, CONV_BLOCK), :] = piece[pl.ds(0, CONV_BLOCK), :]
        rest[pl.ds(slot * TCONV_BLOCK, TCONV_BLOCK), :] = piece[pl.ds(CONV_BLOCK, TCONV_BLOCK), :]
        few[slot] = piece[pl.ds(start, share), :].astype(jnp.float32)
    for b in range(SIDE):
        ahead = wrap(b - along)
        slot = jnp.where(ahead < SIDE // 2, jnp.where(ahead == 0, 0, SIDE // 2 + ahead), SIDE - ahead)
        rows = few[slot]
        for m in range(2):
            target = pl.ds((m * SIDE + b) * half, half)
            dense[target, :] = rows[m * half : (m + 1) * half]
    rest[pl.ds(SIDE * TCONV_BLOCK, share * SIDE), :] = dense[...].astype(jnp.bfloat16)


def norm_kernel(where, latents, halo, sums, other, gain, offset, shifted):
    rows, width, chans = latents.shape
    size = chans // GROUPS
    group = lax.broadcasted_iota(jnp.int32, (chans, chans), 0) // size
    same = group == lax.broadcasted_iota(jnp.int32, (chans, chans), 1) // size
    total = jnp.dot(
        jnp.broadcast_to(jnp.concatenate([sums[...] + other[...]] * 4, axis=0), (8, chans)),
        same.astype(jnp.float32),
        precision=lax.Precision.HIGHEST,
        preferred_element_type=jnp.float32,
    )
    entries = 2 * rows * width * size
    mean = total[0:1] / entries
    var = total[1:2] / entries - mean * mean
    scale = lax.rsqrt(var + 1e-05) * gain[...]
    bias = offset[...]
    column = lax.broadcasted_iota(jnp.int32, (width, 1), 0)
    lower = where[3]

    def fill(at, raw):
        values = (raw.astype(jnp.float32) - mean) * scale + bias
        values = values / (1.0 + jnp.exp(-values))
        left = jnp.where(column == 0, 0.0, pltpu.roll(values, 1, 0))
        right = jnp.where(column == width - 1, 0.0, pltpu.roll(values, width - 1, 0))
        shifted[0, at] = left.astype(jnp.bfloat16)
        shifted[1, at] = values.astype(jnp.bfloat16)
        shifted[2, at] = right.astype(jnp.bfloat16)

    def one_row(r, carry):
        fill(r + 1, latents[r])
        return carry

    lax.fori_loop(0, rows, one_row, 0)
    fill(jnp.where(lower == 1, 0, rows + 1), halo[0])
    empty = jnp.where(lower == 1, rows + 1, 0)
    for dx in range(3):
        shifted[dx, empty] = jnp.zeros((width, chans), jnp.bfloat16)


def conv_kernel(where, latents, temb, shifted, *refs):
    pieces, (out, weight, total, sems) = refs[: 2 * SIDE], refs[2 * SIDE :]
    fetch_blocks(where, pieces, weight, CONV_BLOCK, sems)
    rows, width, chans = latents.shape
    for px in range(SIDE):
        await_line(weight, sems, px)

    def one_tap(tap, carry):
        dy, dx = lax.div(tap, 3), lax.rem(tap, 3)
        taken = shifted[dx, pl.ds(dy, rows)].reshape(rows * width, chans)
        total[...] += jnp.dot(
            taken,
            weight[pl.ds(pl.multiple_of(tap * chans, 128), chans), :],
            preferred_element_type=jnp.float32,
        )
        return carry

    base = latents[...].astype(jnp.float32).reshape(rows * width, chans)
    total[...] = base + temb[...]
    lax.fori_loop(0, 9, one_tap, 0)
    out[...] = total[...].astype(jnp.bfloat16)


def layer_norm(values):
    mean = jnp.mean(values, axis=-1, keepdims=True)
    centered = values - mean
    var = jnp.mean(centered * centered, axis=-1, keepdims=True)
    return centered * lax.rsqrt(var + 1e-05)


def temporal_kernel(where, moved, gains, *refs):
    pieces, (out, tconv, dense, mid, qkv, attended, sems, dense_sem) = (
        refs[: 2 * SIDE],
        refs[2 * SIDE :],
    )
    x, y, core = where[0], where[1], where[2]
    frames, places, chans = moved.shape
    fetch_blocks(where, pieces, tconv, TCONV_BLOCK, sems)
    share = chans // SIDE
    for slot, ref in enumerate(pieces):
        holder = holder_of(core, slot)
        at = wrap(jnp.where(holder == 0, y, x) + OFFSETS[slot % SIDE])
        for m in range(2):
            source = ref.at[pl.ds(SIDE * TCONV_BLOCK + m * share, share)]
            target = dense.at[2 * holder + m, pl.ds(pl.multiple_of(at * share, 16), share)]
            pltpu.make_async_copy(source, target, dense_sem).start()
    rows = frames * places
    values = moved[...].astype(jnp.float32).reshape(rows, chans)
    first = (layer_norm(values) * gains[0:1, :]).astype(jnp.bfloat16)
    zero = jnp.zeros((places, chans), jnp.bfloat16)
    before = jnp.concatenate([zero, first[:-places]], axis=0)
    after = jnp.concatenate([first[places:], zero], axis=0)
    for px in range(SIDE):
        await_line(tconv, sems, px)
    mid[...] = values + jnp.dot(
        before, tconv[:chans, :], preferred_element_type=jnp.float32
    )
    mid[...] += jnp.dot(first, tconv[chans : 2 * chans, :], preferred_element_type=jnp.float32)
    mid[...] += jnp.dot(after, tconv[2 * chans :, :], preferred_element_type=jnp.float32)
    second = (layer_norm(mid[...]) * gains[1:2, :]).astype(jnp.bfloat16)
    pltpu.make_async_copy(dense, dense, dense_sem).wait()
    for m in range(3):
        part = jnp.dot(second, dense[m], preferred_element_type=jnp.float32)
        qkv[m] = part.astype(jnp.bfloat16).reshape(frames, places, chans)
    some = 16
    many = frames * some
    row_place = lax.broadcasted_iota(jnp.int32, (many, many), 0) % some
    col_place = lax.broadcasted_iota(jnp.int32, (many, many), 1) % some
    same = row_place == col_place
    lane = lax.broadcasted_iota(jnp.int32, (1, 2 * HEAD), 1)

    def one_pair(pair, carry):
        lanes = pl.ds(pl.multiple_of(pair * 2 * HEAD, 2 * HEAD), 2 * HEAD)
        for group in range(places // some):
            spot = slice(group * some, (group + 1) * some)
            query = qkv[0, :, spot, lanes].reshape(many, 2 * HEAD)
            key = qkv[1, :, spot, lanes].reshape(many, 2 * HEAD)
            value = qkv[2, :, spot, lanes].reshape(many, 2 * HEAD)
            both = []
            for side in range(2):
                own = (lane < HEAD) if side == 0 else (lane >= HEAD)
                only = jnp.where(own, query, jnp.zeros_like(query))
                scores = lax.dot_general(
                    only, key, (((1,), (1,)), ((), ())), preferred_element_type=jnp.float32
                )
                scores = jnp.where(same, scores * HEAD ** (-0.5), -1e30)
                top = jnp.max(scores, axis=-1, keepdims=True)
                raised = jnp.exp(scores - top)
                weights = raised / jnp.sum(raised, axis=-1, keepdims=True)
                both.append(
                    jnp.dot(weights.astype(jnp.bfloat16), value, preferred_element_type=jnp.float32)
                )
            mixed = jnp.where(lane < HEAD, both[0], both[1]).astype(jnp.bfloat16)
            attended[:, spot, lanes] = mixed.reshape(frames, some, 2 * HEAD)
        return carry

    lax.fori_loop(0, chans // (2 * HEAD), one_pair, 0)
    projected = jnp.dot(
        attended[...].reshape(rows, chans), dense[3], preferred_element_type=jnp.float32
    )
    out[...] = (mid[...] + projected).astype(jnp.bfloat16).reshape(frames, places, chans)


def specs(count):
    return [pl.BlockSpec(memory_space=pl.ANY)] * count


def shards(
    latents,
    norm_gain,
    norm_bias,
    conv_weight,
    time_weight,
    first_gain,
    tconv_weight,
    second_gain,
    qkv_weight,
    out_weight,
    timesteps,
):
    devices = lax.axis_size(SEQ)
    device = lax.axis_index(SEQ)
    x, y, core = (lax.axis_index(name) for name in SEQ)
    clips = timesteps.shape[0]
    images = clips * FRAMES
    rows, width, chans = latents.shape
    image = device % images
    clip = image // FRAMES
    lower = device // images
    bf16, f32 = jnp.bfloat16, jnp.float32

    where = jnp.stack([x, y, core, lower]).astype(jnp.int32)
    smem = pl.BlockSpec(memory_space=pltpu.SMEM)
    vmem = pl.BlockSpec(memory_space=pltpu.VMEM)
    params = pltpu.CompilerParams(vmem_limit_bytes=VMEM_LIMIT)

    conv_rows, tconv_rows = conv_weight.shape[0], tconv_weight.shape[0]
    few = qkv_weight.shape[0]

    def to_previous(px, py, pcore):
        spot = 2 * py + pcore - 1
        return None if spot < 0 else (px, spot // 2, spot % 2)

    some_rows = jax.ShapeDtypeStruct((2 * few, chans), bf16)
    both, query_key, crossed, value_out = pl.pallas_call(
        pack_kernel,
        out_shape=[
            jax.ShapeDtypeStruct((conv_rows + tconv_rows, chans), bf16),
            some_rows,
            some_rows,
            some_rows,
        ],
        in_specs=[smem] + [vmem] * 4,
        out_specs=[vmem] * 4,
        scratch_shapes=[pltpu.VMEM((64, chans), f32), pltpu.VMEM((24, chans), f32)],
        name="pack",
    )(where, conv_weight, tconv_weight, qkv_weight, out_weight)
    following = send(both, to_previous)
    same_core = send(query_key, lambda px, py, pcore: (py, px, 0) if pcore == 0 else None)
    crossed = send(crossed, lambda px, py, pcore: (px, py, 1) if pcore == 0 else (py, px, 0))

    pairs = [(i, (i + images) % devices) for i in range(devices)]
    edge = lax.dynamic_slice_in_dim(latents, jnp.where(lower == 1, 0, rows - 1), 1, 0)
    halo = lax.ppermute(edge, SEQ, pairs)
    values = latents.astype(f32).reshape(rows * width, chans)
    sums = jnp.stack([jnp.sum(values, axis=0), jnp.sum(values * values, axis=0)])
    other = lax.ppermute(sums, SEQ, pairs)
    temb = time_embed(lax.dynamic_index_in_dim(timesteps, clip, 0, False), time_weight)
    shifted = pl.pallas_call(
        norm_kernel,
        out_shape=jax.ShapeDtypeStruct((3, rows + 2, width, chans), bf16),
        in_specs=[smem] + [vmem] * 6,
        out_specs=vmem,
        compiler_params=params,
        name="norm",
    )(where, latents, halo, sums, other, norm_gain[None], norm_bias[None])

    block = pl.pallas_call(
        cut_kernel,
        out_shape=jax.ShapeDtypeStruct((CONV_BLOCK + TCONV_BLOCK + 4 * few, chans), bf16),
        in_specs=[smem] + [vmem] * 5,
        out_specs=vmem,
        scratch_shapes=[
            pltpu.VMEM((112, chans), f32),
            pltpu.VMEM((32, chans), f32),
            pltpu.VMEM((24, chans), f32),
        ],
        name="cut",
    )(where, both, following, same_core, crossed, value_out)

    line = ring(block, inner)
    conv_line, rest_line = pl.pallas_call(
        line_kernel,
        out_shape=[
            jax.ShapeDtypeStruct((SIDE * CONV_BLOCK, chans), bf16),
            jax.ShapeDtypeStruct((SIDE * (TCONV_BLOCK + 4 * few), chans), bf16),
        ],
        in_specs=[smem] + [vmem] * SIDE,
        out_specs=[vmem] * 2,
        scratch_shapes=[
            pltpu.VMEM((SIDE * 4 * few, chans), f32),
            pltpu.VMEM((SIDE, 4 * few, chans), f32),
        ],
        name="line",
    )(where, *line)
    (conv_pieces, rest_pieces), shifted = two_rings([conv_line, rest_line], outer, shifted)

    spatial = pl.pallas_call(
        conv_kernel,
        out_shape=jax.ShapeDtypeStruct((rows * width, chans), bf16),
        in_specs=[smem] + [vmem] * 3 + specs(2 * SIDE),
        out_specs=vmem,
        scratch_shapes=[
            pltpu.VMEM((9 * chans, chans), bf16),
            pltpu.VMEM((rows * width, chans), f32),
            pltpu.SemaphoreType.DMA((SIDE,)),
        ],
        compiler_params=params,
        name="conv",
    )(where, latents, temb, shifted, *conv_pieces)
    moved = lax.all_to_all(spatial, SEQ[1:], split_axis=0, concat_axis=0, tiled=True)
    places = rows * width // FRAMES
    result = pl.pallas_call(
        temporal_kernel,
        out_shape=jax.ShapeDtypeStruct((FRAMES, places, chans), bf16),
        in_specs=[smem, vmem, vmem] + specs(2 * SIDE),
        out_specs=vmem,
        scratch_shapes=[
            pltpu.VMEM((3 * chans, chans), bf16),
            pltpu.VMEM((4, chans, chans), bf16),
            pltpu.VMEM((FRAMES * places, chans), f32),
            pltpu.VMEM((3, FRAMES, places, chans), bf16),
            pltpu.VMEM((FRAMES, places, chans), bf16),
            pltpu.SemaphoreType.DMA((SIDE,)),
            pltpu.SemaphoreType.DMA,
        ],
        compiler_params=params,
        name="temporal",
    )(
        where,
        moved.reshape(FRAMES, places, chans),
        jnp.stack([first_gain, second_gain]),
        *rest_pieces,
    )
    returned = lax.all_to_all(
        result.reshape(rows * width, chans), SEQ[1:], split_axis=0, concat_axis=0, tiled=True
    )
    return returned.reshape(rows, width, chans)


def solution(mesh):
    torus = Mesh(
        mesh.devices.reshape(mesh.shape["groups"], SIDE, SIDE, 2),
        ("groups", "seq_0", "seq_1", "seq_2"),
    )
    return jax.shard_map(
        shards,
        mesh=torus,
        in_specs=(
            P(GROUPS_SEQ, None, None),
            P(),
            P(),
            P(SEQ, None),
            P(),
            P(),
            P(SEQ, None),
            P(),
            P(SEQ, None),
            P(SEQ, None),
            P("groups"),
        ),
        out_specs=P(GROUPS_SEQ, None, None),
        check_vma=False,
    )
```

```python
import jax
import jax.numpy as jnp
from jax import lax
from jax.experimental import pallas as pl
from jax.experimental.pallas import tpu as pltpu
from jax.sharding import Mesh
from jax.sharding import PartitionSpec as P

HEAD = 64
GROUPS = 32
TFEAT = 320
FRAMES = 16
SEQ = ("seq_0", "seq_1", "seq_2")
GROUPS_SEQ = ("groups", "seq_0", "seq_1", "seq_2")
SIDE = 8
CONV_BLOCK = 48
TCONV_BLOCK = 16
VMEM_LIMIT = 56 * 2**20
OFFSETS = (0, -1, -2, -3, -4, 1, 2, 3)


def route(target):
    pairs = []
    for x in range(SIDE):
        for y in range(SIDE):
            for core in range(2):
                there = target(x, y, core)
                if there is not None:
                    tx, ty, tcore = there
                    to = (tx % SIDE * SIDE + ty % SIDE) * 2 + tcore
                    pairs.append(((x * SIDE + y) * 2 + core, to))
    return pairs


def send(block, target):
    return lax.ppermute(block, SEQ, route(target))


def inner(step):
    return lambda x, y, core: (x + step, y, core) if core == 0 else (x, y + step, core)


def outer(step):
    return lambda x, y, core: (x, y + step, core) if core == 0 else (x + step, y, core)


def swap(x, y, core):
    return x, y, 1 - core


def ring(block, towards):
    ahead, behind = [block], [block]
    for step in range(SIDE // 2):
        ahead.append(send(ahead[-1], towards(1)))
        if step < SIDE // 2 - 1:
            behind.append(send(behind[-1], towards(-1)))
    return ahead + behind[1:]


def outer_ring(block, early):
    ahead, behind = [block], [block]
    for step in range(SIDE // 2):
        if step == 2:
            ahead[-1], early = lax.optimization_barrier((ahead[-1], early))
        ahead.append(send(ahead[-1], outer(1)))
        if step < SIDE // 2 - 1:
            behind.append(send(behind[-1], outer(-1)))
    own = ahead + behind[1:]
    return own + [send(piece, swap) for piece in own], early


def time_embed(timestep, time_weight):
    half = TFEAT // 2
    freqs = jnp.exp(-jnp.log(10000.0) * jnp.arange(half, dtype=jnp.float32) / half)
    angles = timestep.astype(jnp.float32)[None, None] * freqs[None, :]
    feats = jnp.concatenate([jnp.cos(angles), jnp.sin(angles)], axis=-1)
    return jnp.dot(feats, time_weight.astype(jnp.float32), precision=lax.Precision.HIGHEST)


def wrap(value):
    return lax.rem(value + 2 * SIDE, SIDE)


def offset_of(slot):
    return jnp.where(slot <= SIDE // 2, -slot, slot - SIDE // 2)


def holder_of(core, slot):
    return core if slot < SIDE else 1 - core


def fetch_blocks(where, pieces, start, weight, size, sems):
    x, y, core = where[0], where[1], where[2]
    for slot, ref in enumerate(pieces):
        holder = holder_of(core, slot)
        across = OFFSETS[slot % SIDE]

        def one(b, carry, ref=ref, holder=holder, across=across):
            along = offset_of(b)
            px = wrap(x + jnp.where(holder == 0, along, across))
            py = wrap(y + jnp.where(holder == 0, across, along))
            inside = 2 * py + holder

            @pl.when(inside < 2 * SIDE - 1)
            def _():
                at = pl.multiple_of((px * (2 * SIDE - 1) + inside) * size, size)
                source = ref.at[pl.ds(pl.multiple_of(start + b * size, size), size)]
                target = weight.at[pl.ds(at, size)]
                pltpu.make_async_copy(source, target, sems.at[px]).start()

            return carry

        lax.fori_loop(0, SIDE, one, 0)


def await_line(weight, sems, px):
    size = weight.shape[0] // SIDE
    part = weight.at[pl.ds(px * size, size)]
    pltpu.make_async_copy(part, part, sems.at[px]).wait()


def pack_kernel(where, conv, tconv, qkv, last, both, query_key, crossed, value_out, rows, few):
    conv_rows, chans = conv.shape
    count = qkv.shape[0]
    f32, bf16 = jnp.float32, jnp.bfloat16
    rows[pl.ds(0, conv_rows), :] = conv[...].astype(f32)
    rows[pl.ds(conv_rows, tconv.shape[0]), :] = tconv[...].astype(f32)
    both[...] = rows[pl.ds(0, both.shape[0]), :].astype(bf16)
    for m in range(3):
        few[pl.ds(m * count, count), :] = qkv[:, m * chans : (m + 1) * chans].astype(f32)
    few[pl.ds(3 * count, count), :] = last[...].astype(f32)
    head = few[pl.ds(0, 2 * count), :].astype(bf16)
    tail = few[pl.ds(2 * count, 2 * count), :].astype(bf16)
    query_key[...] = head
    value_out[...] = tail
    crossed[...] = jnp.where(where[2] == 0, tail.astype(f32), head.astype(f32)).astype(bf16)


def cut_kernel(where, both, following, same_core, crossed, value_out, block, conv, tconv, few):
    f32, bf16 = jnp.float32, jnp.bfloat16
    count = same_core.shape[0] // 2
    tconv_rows = TCONV_BLOCK - 1
    conv_rows = both.shape[0] - tconv_rows
    inside = 2 * where[1] + where[2]
    own, next_rows = both[...].astype(f32), following[...].astype(f32)
    conv[pl.ds(0, both.shape[0]), :] = own
    tconv[pl.ds(0, tconv_rows), :] = conv[pl.ds(conv_rows, tconv_rows), :]
    conv[pl.ds(conv_rows, both.shape[0]), :] = next_rows
    tconv[pl.ds(tconv_rows, tconv_rows), :] = conv[pl.ds(2 * conv_rows, tconv_rows), :]
    conv_at = jnp.minimum((CONV_BLOCK - conv_rows) * inside, 2 * conv_rows - CONV_BLOCK)
    tconv_at = jnp.minimum(inside, 2 * tconv_rows - TCONV_BLOCK)
    turned = pltpu.roll(conv[...], lax.rem(conv.shape[0] - conv_at, conv.shape[0]), 0)
    block[pl.ds(0, CONV_BLOCK), :] = turned[:CONV_BLOCK].astype(bf16)
    turned = pltpu.roll(tconv[...], lax.rem(tconv.shape[0] - tconv_at, tconv.shape[0]), 0)
    block[pl.ds(CONV_BLOCK, TCONV_BLOCK), :] = turned[:TCONV_BLOCK].astype(bf16)
    near, far, kept = same_core[...].astype(f32), crossed[...].astype(f32), value_out[...].astype(f32)
    even = jnp.where(where[2] == 0, near, far)
    odd = jnp.where(where[2] == 0, far, kept)
    conv[pl.ds(0, 2 * count), :] = even
    conv[pl.ds(2 * count, 2 * count), :] = odd
    for m in range(2):
        for parity in range(2):
            source = conv[pl.ds((2 * parity + m) * count, count), :]
            few[pl.ds((2 * m + parity) * count, count), :] = source
    dense = few[pl.ds(0, 4 * count), :].astype(bf16)
    block[pl.ds(CONV_BLOCK + TCONV_BLOCK, 4 * count), :] = dense


def line_kernel(where, *refs):
    pieces, (out, dense, few) = refs[:SIDE], refs[SIDE:]
    along = jnp.where(where[2] == 0, where[0], where[1])
    start = CONV_BLOCK + TCONV_BLOCK
    share = pieces[0].shape[0] - start
    half = share // 2
    for slot, piece in enumerate(pieces):
        out[pl.ds(slot * CONV_BLOCK, CONV_BLOCK), :] = piece[pl.ds(0, CONV_BLOCK), :]
        target = pl.ds(SIDE * CONV_BLOCK + slot * TCONV_BLOCK, TCONV_BLOCK)
        out[target, :] = piece[pl.ds(CONV_BLOCK, TCONV_BLOCK), :]
        few[slot] = piece[pl.ds(start, share), :].astype(jnp.float32)
    for b in range(SIDE):
        ahead = wrap(b - along)
        slot = jnp.where(ahead < SIDE // 2, jnp.where(ahead == 0, 0, SIDE // 2 + ahead), SIDE - ahead)
        rows = few[slot]
        for m in range(2):
            target = pl.ds((m * SIDE + b) * half, half)
            dense[target, :] = rows[m * half : (m + 1) * half]
    out[pl.ds(SIDE * start, share * SIDE), :] = dense[...].astype(jnp.bfloat16)


def norm_kernel(where, latents, halo, sums, other, gain, offset, shifted):
    rows, width, chans = latents.shape
    size = chans // GROUPS
    group = lax.broadcasted_iota(jnp.int32, (chans, chans), 0) // size
    same = group == lax.broadcasted_iota(jnp.int32, (chans, chans), 1) // size
    total = jnp.dot(
        jnp.broadcast_to(jnp.concatenate([sums[...] + other[...]] * 4, axis=0), (8, chans)),
        same.astype(jnp.float32),
        precision=lax.Precision.HIGHEST,
        preferred_element_type=jnp.float32,
    )
    entries = 2 * rows * width * size
    mean = total[0:1] / entries
    var = total[1:2] / entries - mean * mean
    scale = lax.rsqrt(var + 1e-05) * gain[...]
    bias = offset[...]
    column = lax.broadcasted_iota(jnp.int32, (width, 1), 0)
    lower = where[3]

    def fill(at, raw):
        values = (raw.astype(jnp.float32) - mean) * scale + bias
        values = values / (1.0 + jnp.exp(-values))
        left = jnp.where(column == 0, 0.0, pltpu.roll(values, 1, 0))
        right = jnp.where(column == width - 1, 0.0, pltpu.roll(values, width - 1, 0))
        shifted[0, at] = left.astype(jnp.bfloat16)
        shifted[1, at] = values.astype(jnp.bfloat16)
        shifted[2, at] = right.astype(jnp.bfloat16)

    def one_row(r, carry):
        fill(r + 1, latents[r])
        return carry

    lax.fori_loop(0, rows, one_row, 0)
    fill(jnp.where(lower == 1, 0, rows + 1), halo[0])
    empty = jnp.where(lower == 1, rows + 1, 0)
    for dx in range(3):
        shifted[dx, empty] = jnp.zeros((width, chans), jnp.bfloat16)


def conv_kernel(where, latents, temb, shifted, *refs):
    pieces, (out, weight, total, sems) = refs[: 2 * SIDE], refs[2 * SIDE :]
    fetch_blocks(where, pieces, 0, weight, CONV_BLOCK, sems)
    rows, width, chans = latents.shape
    waited = 0
    for tap in range(9):
        dy, dx = divmod(tap, 3)
        while waited * weight.shape[0] < (tap + 1) * chans * SIDE:
            await_line(weight, sems, waited)
            waited += 1
        taken = shifted[dx, dy : dy + rows].reshape(rows * width, chans)
        part = jnp.dot(
            taken,
            weight[tap * chans : (tap + 1) * chans, :],
            preferred_element_type=jnp.float32,
        )
        if tap == 0:
            total[...] = part
        elif tap < 8:
            total[...] += part
        else:
            base = latents[...].astype(jnp.float32).reshape(rows * width, chans)
            out[...] = (base + (total[...] + part) + temb[...]).astype(jnp.bfloat16)


def layer_norm(values):
    mean = jnp.mean(values, axis=-1, keepdims=True)
    centered = values - mean
    var = jnp.mean(centered * centered, axis=-1, keepdims=True)
    return centered * lax.rsqrt(var + 1e-05)


def temporal_kernel(where, moved, gains, *refs):
    pieces, (out, tconv, dense, mid, qkv, attended, sems, dense_sem) = (
        refs[: 2 * SIDE],
        refs[2 * SIDE :],
    )
    x, y, core = where[0], where[1], where[2]
    frames, places, chans = moved.shape
    fetch_blocks(where, pieces, SIDE * CONV_BLOCK, tconv, TCONV_BLOCK, sems)
    share = chans // SIDE
    for slot, ref in enumerate(pieces):
        holder = holder_of(core, slot)
        at = wrap(jnp.where(holder == 0, y, x) + OFFSETS[slot % SIDE])
        for m in range(2):
            source = ref.at[pl.ds(SIDE * (CONV_BLOCK + TCONV_BLOCK) + m * share, share)]
            target = dense.at[2 * holder + m, pl.ds(pl.multiple_of(at * share, 16), share)]
            pltpu.make_async_copy(source, target, dense_sem).start()
    rows = frames * places
    values = moved[...].astype(jnp.float32).reshape(rows, chans)
    first = (layer_norm(values) * gains[0:1, :]).astype(jnp.bfloat16)
    zero = jnp.zeros((places, chans), jnp.bfloat16)
    before = jnp.concatenate([zero, first[:-places]], axis=0)
    after = jnp.concatenate([first[places:], zero], axis=0)
    for px in range(SIDE):
        await_line(tconv, sems, px)
    mid[...] = values + jnp.dot(
        before, tconv[:chans, :], preferred_element_type=jnp.float32
    )
    mid[...] += jnp.dot(first, tconv[chans : 2 * chans, :], preferred_element_type=jnp.float32)
    mid[...] += jnp.dot(after, tconv[2 * chans :, :], preferred_element_type=jnp.float32)
    second = (layer_norm(mid[...]) * gains[1:2, :]).astype(jnp.bfloat16)
    pltpu.make_async_copy(dense, dense, dense_sem).wait()
    for m in range(3):
        part = jnp.dot(second, dense[m], preferred_element_type=jnp.float32)
        qkv[m] = part.astype(jnp.bfloat16).reshape(frames, places, chans)
    some = 16
    many = frames * some
    row_place = lax.broadcasted_iota(jnp.int32, (many, many), 0) % some
    col_place = lax.broadcasted_iota(jnp.int32, (many, many), 1) % some
    same = row_place == col_place
    lane = lax.broadcasted_iota(jnp.int32, (1, 2 * HEAD), 1)
    for pair in range(chans // (2 * HEAD)):
        lanes = slice(pair * 2 * HEAD, (pair + 1) * 2 * HEAD)
        for group in range(places // some):
            spot = slice(group * some, (group + 1) * some)
            query = qkv[0, :, spot, lanes].reshape(many, 2 * HEAD)
            key = qkv[1, :, spot, lanes].reshape(many, 2 * HEAD)
            value = qkv[2, :, spot, lanes].reshape(many, 2 * HEAD)
            both = []
            for side in range(2):
                own = (lane < HEAD) if side == 0 else (lane >= HEAD)
                only = jnp.where(own, query, jnp.zeros_like(query))
                scores = lax.dot_general(
                    only, key, (((1,), (1,)), ((), ())), preferred_element_type=jnp.float32
                )
                scores = jnp.where(same, scores * HEAD ** (-0.5), -1e30)
                top = jnp.max(scores, axis=-1, keepdims=True)
                raised = jnp.exp(scores - top)
                weights = raised / jnp.sum(raised, axis=-1, keepdims=True)
                both.append(
                    jnp.dot(weights.astype(jnp.bfloat16), value, preferred_element_type=jnp.float32)
                )
            mixed = jnp.where(lane < HEAD, both[0], both[1]).astype(jnp.bfloat16)
            attended[:, spot, lanes] = mixed.reshape(frames, some, 2 * HEAD)
    projected = jnp.dot(
        attended[...].reshape(rows, chans), dense[3], preferred_element_type=jnp.float32
    )
    out[...] = (mid[...] + projected).astype(jnp.bfloat16).reshape(frames, places, chans)


def specs(count):
    return [pl.BlockSpec(memory_space=pl.ANY)] * count


def shards(
    latents,
    norm_gain,
    norm_bias,
    conv_weight,
    time_weight,
    first_gain,
    tconv_weight,
    second_gain,
    qkv_weight,
    out_weight,
    timesteps,
):
    devices = lax.axis_size(SEQ)
    device = lax.axis_index(SEQ)
    x, y, core = (lax.axis_index(name) for name in SEQ)
    clips = timesteps.shape[0]
    images = clips * FRAMES
    rows, width, chans = latents.shape
    image = device % images
    clip = image // FRAMES
    lower = device // images
    bf16, f32 = jnp.bfloat16, jnp.float32

    where = jnp.stack([x, y, core, lower]).astype(jnp.int32)
    smem = pl.BlockSpec(memory_space=pltpu.SMEM)
    vmem = pl.BlockSpec(memory_space=pltpu.VMEM)
    params = pltpu.CompilerParams(vmem_limit_bytes=VMEM_LIMIT)

    conv_rows, tconv_rows = conv_weight.shape[0], tconv_weight.shape[0]
    few = qkv_weight.shape[0]

    def to_previous(px, py, pcore):
        spot = 2 * py + pcore - 1
        return None if spot < 0 else (px, spot // 2, spot % 2)

    some_rows = jax.ShapeDtypeStruct((2 * few, chans), bf16)
    both, query_key, crossed, value_out = pl.pallas_call(
        pack_kernel,
        out_shape=[
            jax.ShapeDtypeStruct((conv_rows + tconv_rows, chans), bf16),
            some_rows,
            some_rows,
            some_rows,
        ],
        in_specs=[smem] + [vmem] * 4,
        out_specs=[vmem] * 4,
        scratch_shapes=[pltpu.VMEM((64, chans), f32), pltpu.VMEM((24, chans), f32)],
        name="pack",
    )(where, conv_weight, tconv_weight, qkv_weight, out_weight)
    following = send(both, to_previous)
    same_core = send(query_key, lambda px, py, pcore: (py, px, 0) if pcore == 0 else None)
    crossed = send(crossed, lambda px, py, pcore: (px, py, 1) if pcore == 0 else (py, px, 0))

    pairs = [(i, (i + images) % devices) for i in range(devices)]
    edge = lax.dynamic_slice_in_dim(latents, jnp.where(lower == 1, 0, rows - 1), 1, 0)
    halo = lax.ppermute(edge, SEQ, pairs)
    values = latents.astype(f32).reshape(rows * width, chans)
    sums = jnp.stack([jnp.sum(values, axis=0), jnp.sum(values * values, axis=0)])
    other = lax.ppermute(sums, SEQ, pairs)
    temb = time_embed(lax.dynamic_index_in_dim(timesteps, clip, 0, False), time_weight)
    shifted = pl.pallas_call(
        norm_kernel,
        out_shape=jax.ShapeDtypeStruct((3, rows + 2, width, chans), bf16),
        in_specs=[smem] + [vmem] * 6,
        out_specs=vmem,
        compiler_params=params,
        name="norm",
    )(where, latents, halo, sums, other, norm_gain[None], norm_bias[None])

    block = pl.pallas_call(
        cut_kernel,
        out_shape=jax.ShapeDtypeStruct((CONV_BLOCK + TCONV_BLOCK + 4 * few, chans), bf16),
        in_specs=[smem] + [vmem] * 5,
        out_specs=vmem,
        scratch_shapes=[
            pltpu.VMEM((112, chans), f32),
            pltpu.VMEM((32, chans), f32),
            pltpu.VMEM((24, chans), f32),
        ],
        name="cut",
    )(where, both, following, same_core, crossed, value_out)

    line = ring(block, inner)
    whole_line = pl.pallas_call(
        line_kernel,
        out_shape=jax.ShapeDtypeStruct((SIDE * line[0].shape[0], chans), bf16),
        in_specs=[smem] + [vmem] * SIDE,
        out_specs=vmem,
        scratch_shapes=[
            pltpu.VMEM((SIDE * 4 * few, chans), f32),
            pltpu.VMEM((SIDE, 4 * few, chans), f32),
        ],
        name="line",
    )(where, *line)
    pieces, shifted = outer_ring(whole_line, shifted)

    spatial = pl.pallas_call(
        conv_kernel,
        out_shape=jax.ShapeDtypeStruct((rows * width, chans), bf16),
        in_specs=[smem] + [vmem] * 3 + specs(2 * SIDE),
        out_specs=vmem,
        scratch_shapes=[
            pltpu.VMEM((9 * chans, chans), bf16),
            pltpu.VMEM((rows * width, chans), f32),
            pltpu.SemaphoreType.DMA((SIDE,)),
        ],
        compiler_params=params,
        name="conv",
    )(where, latents, temb, shifted, *pieces)
    moved = lax.all_to_all(spatial, SEQ[1:], split_axis=0, concat_axis=0, tiled=True)
    places = rows * width // FRAMES
    result = pl.pallas_call(
        temporal_kernel,
        out_shape=jax.ShapeDtypeStruct((FRAMES, places, chans), bf16),
        in_specs=[smem, vmem, vmem] + specs(2 * SIDE),
        out_specs=vmem,
        scratch_shapes=[
            pltpu.VMEM((3 * chans, chans), bf16),
            pltpu.VMEM((4, chans, chans), bf16),
            pltpu.VMEM((FRAMES * places, chans), f32),
            pltpu.VMEM((3, FRAMES, places, chans), bf16),
            pltpu.VMEM((FRAMES, places, chans), bf16),
            pltpu.SemaphoreType.DMA((SIDE,)),
            pltpu.SemaphoreType.DMA,
        ],
        compiler_params=params,
        name="temporal",
    )(
        where,
        moved.reshape(FRAMES, places, chans),
        jnp.stack([first_gain, second_gain]),
        *pieces,
    )
    returned = lax.all_to_all(
        result.reshape(rows * width, chans), SEQ[1:], split_axis=0, concat_axis=0, tiled=True
    )
    return returned.reshape(rows, width, chans)


def solution(mesh):
    torus = Mesh(
        mesh.devices.reshape(mesh.shape["groups"], SIDE, SIDE, 2),
        ("groups", "seq_0", "seq_1", "seq_2"),
    )
    return jax.shard_map(
        shards,
        mesh=torus,
        in_specs=(
            P(GROUPS_SEQ, None, None),
            P(),
            P(),
            P(SEQ, None),
            P(),
            P(),
            P(SEQ, None),
            P(),
            P(SEQ, None),
            P(SEQ, None),
            P("groups"),
        ),
        out_specs=P(GROUPS_SEQ, None, None),
        check_vma=False,
    )
```

```python
import jax
import jax.numpy as jnp
from jax import lax
from jax.experimental import pallas as pl
from jax.experimental.pallas import tpu as pltpu
from jax.sharding import Mesh
from jax.sharding import PartitionSpec as P

HEAD = 64
GROUPS = 32
TFEAT = 320
FRAMES = 16
SEQ = ("seq_0", "seq_1", "seq_2")
GROUPS_SEQ = ("groups", "seq_0", "seq_1", "seq_2")
SIDE = 8
CONV_BLOCK = 48
TCONV_BLOCK = 16
VMEM_LIMIT = 56 * 2**20
OFFSETS = (0, -1, -2, -3, -4, 1, 2, 3)


def route(target):
    pairs = []
    for x in range(SIDE):
        for y in range(SIDE):
            for core in range(2):
                there = target(x, y, core)
                if there is not None:
                    tx, ty, tcore = there
                    to = (tx % SIDE * SIDE + ty % SIDE) * 2 + tcore
                    pairs.append(((x * SIDE + y) * 2 + core, to))
    return pairs


def send(block, target):
    return lax.ppermute(block, SEQ, route(target))


def inner(step):
    return lambda x, y, core: (x + step, y, core) if core == 0 else (x, y + step, core)


def outer(step):
    return lambda x, y, core: (x, y + step, core) if core == 0 else (x + step, y, core)


def swap(x, y, core):
    return x, y, 1 - core


def direct(block):
    return [block] + [send(block, inner(-offset)) for offset in OFFSETS[1:]]


def two_rings(first, second):
    chains = {}
    for sign, steps in ((1, SIDE // 2), (-1, SIDE // 2 - 1)):
        chains[sign] = ([first], [second])
    for step in range(SIDE // 2):
        for sign, steps in ((1, SIDE // 2), (-1, SIDE // 2 - 1)):
            if step >= steps:
                continue
            one, two = chains[sign]
            if step > 1:
                one[-1], two[-2] = lax.optimization_barrier((one[-1], two[-2]))
            if step > 0:
                two[-1], one[-1] = lax.optimization_barrier((two[-1], one[-1]))
            one.append(send(one[-1], outer(sign)))
            two.append(send(two[-1], outer(sign)))
    own = [chains[1][i] + chains[-1][i][1:] for i in range(2)]
    return own[0] + [send(piece, swap) for piece in own[0]], own[1]


def time_embed(timestep, time_weight):
    half = TFEAT // 2
    freqs = jnp.exp(-jnp.log(10000.0) * jnp.arange(half, dtype=jnp.float32) / half)
    angles = timestep.astype(jnp.float32)[None, None] * freqs[None, :]
    feats = jnp.concatenate([jnp.cos(angles), jnp.sin(angles)], axis=-1)
    return jnp.dot(feats, time_weight.astype(jnp.float32), precision=lax.Precision.HIGHEST)


def wrap(value):
    return lax.rem(value + 2 * SIDE, SIDE)


def offset_of(slot):
    return jnp.where(slot <= SIDE // 2, -slot, slot - SIDE // 2)


def holder_of(core, slot):
    return core if slot < SIDE else 1 - core


def fetch_blocks(where, pieces, weight, size, sems):
    x, y, core = where[0], where[1], where[2]
    for slot, ref in enumerate(pieces):
        holder = holder_of(core, slot)
        across = OFFSETS[slot % SIDE]

        def one(b, carry, ref=ref, holder=holder, across=across):
            along = offset_of(b)
            px = wrap(x + jnp.where(holder == 0, along, across))
            py = wrap(y + jnp.where(holder == 0, across, along))
            inside = 2 * py + holder

            @pl.when(inside < 2 * SIDE - 1)
            def _():
                at = pl.multiple_of((px * (2 * SIDE - 1) + inside) * size, size)
                source = ref.at[pl.ds(pl.multiple_of(b * size, size), size)]
                target = weight.at[pl.ds(at, size)]
                pltpu.make_async_copy(source, target, sems.at[px]).start()

            return carry

        lax.fori_loop(0, SIDE, one, 0)


def await_line(weight, sems, px):
    size = weight.shape[0] // SIDE
    part = weight.at[pl.ds(px * size, size)]
    pltpu.make_async_copy(part, part, sems.at[px]).wait()


def pack_kernel(where, latents, conv, tconv, qkv, last, *refs):
    both, query_key, crossed, value_out, edge, sums, rows, few = refs
    conv_rows, chans = conv.shape
    count = qkv.shape[0]
    f32, bf16 = jnp.float32, jnp.bfloat16
    rows[pl.ds(0, conv_rows), :] = conv[...].astype(f32)
    rows[pl.ds(conv_rows, tconv.shape[0]), :] = tconv[...].astype(f32)
    both[...] = rows[pl.ds(0, both.shape[0]), :].astype(bf16)
    for m in range(3):
        few[pl.ds(m * count, count), :] = qkv[:, m * chans : (m + 1) * chans].astype(f32)
    few[pl.ds(3 * count, count), :] = last[...].astype(f32)
    head = few[pl.ds(0, 2 * count), :].astype(bf16)
    tail = few[pl.ds(2 * count, 2 * count), :].astype(bf16)
    query_key[...] = head
    value_out[...] = tail
    crossed[...] = jnp.where(where[2] == 0, tail.astype(f32), head.astype(f32)).astype(bf16)
    edge[0] = latents[jnp.where(where[3] == 1, 0, latents.shape[0] - 1)]
    values = latents[0].astype(f32)
    first, second = values, values * values
    for r in range(1, latents.shape[0]):
        values = latents[r].astype(f32)
        first, second = first + values, second + values * values
    sums[...] = jnp.zeros(sums.shape, f32)
    sums[0:1, :] = jnp.sum(first, axis=0, keepdims=True)
    sums[1:2, :] = jnp.sum(second, axis=0, keepdims=True)


def cut_kernel(where, both, following, same_core, crossed, value_out, block, conv, tconv, few):
    f32, bf16 = jnp.float32, jnp.bfloat16
    count = same_core.shape[0] // 2
    tconv_rows = TCONV_BLOCK - 1
    conv_rows = both.shape[0] - tconv_rows
    inside = 2 * where[1] + where[2]
    own, next_rows = both[...].astype(f32), following[...].astype(f32)
    conv[pl.ds(0, both.shape[0]), :] = own
    tconv[pl.ds(0, tconv_rows), :] = conv[pl.ds(conv_rows, tconv_rows), :]
    conv[pl.ds(conv_rows, both.shape[0]), :] = next_rows
    tconv[pl.ds(tconv_rows, tconv_rows), :] = conv[pl.ds(2 * conv_rows, tconv_rows), :]
    conv_at = jnp.minimum((CONV_BLOCK - conv_rows) * inside, 2 * conv_rows - CONV_BLOCK)
    tconv_at = jnp.minimum(inside, 2 * tconv_rows - TCONV_BLOCK)
    turned = pltpu.roll(conv[...], lax.rem(conv.shape[0] - conv_at, conv.shape[0]), 0)
    block[pl.ds(0, CONV_BLOCK), :] = turned[:CONV_BLOCK].astype(bf16)
    turned = pltpu.roll(tconv[...], lax.rem(tconv.shape[0] - tconv_at, tconv.shape[0]), 0)
    block[pl.ds(CONV_BLOCK, TCONV_BLOCK), :] = turned[:TCONV_BLOCK].astype(bf16)
    near, far, kept = same_core[...].astype(f32), crossed[...].astype(f32), value_out[...].astype(f32)
    even = jnp.where(where[2] == 0, near, far)
    odd = jnp.where(where[2] == 0, far, kept)
    conv[pl.ds(0, 2 * count), :] = even
    conv[pl.ds(2 * count, 2 * count), :] = odd
    for m in range(2):
        for parity in range(2):
            source = conv[pl.ds((2 * parity + m) * count, count), :]
            few[pl.ds((2 * m + parity) * count, count), :] = source
    dense = few[pl.ds(0, 4 * count), :].astype(bf16)
    block[pl.ds(CONV_BLOCK + TCONV_BLOCK, 4 * count), :] = dense


def line_kernel(where, *refs):
    pieces, (conv, rest, dense, few) = refs[:SIDE], refs[SIDE:]
    along = jnp.where(where[2] == 0, where[0], where[1])
    start = CONV_BLOCK + TCONV_BLOCK
    share = pieces[0].shape[0] - start
    half = share // 2
    for slot, piece in enumerate(pieces):
        conv[pl.ds(slot * CONV_BLOCK, CONV_BLOCK), :] = piece[pl.ds(0, CONV_BLOCK), :]
        rest[pl.ds(slot * TCONV_BLOCK, TCONV_BLOCK), :] = piece[pl.ds(CONV_BLOCK, TCONV_BLOCK), :]
        few[slot] = piece[pl.ds(start, share), :].astype(jnp.float32)
    for b in range(SIDE):
        ahead = wrap(b - along)
        slot = jnp.where(ahead < SIDE // 2, jnp.where(ahead == 0, 0, SIDE // 2 + ahead), SIDE - ahead)
        rows = few[slot]
        for m in range(2):
            target = pl.ds((m * SIDE + b) * half, half)
            dense[target, :] = rows[m * half : (m + 1) * half]
    rest[pl.ds(SIDE * TCONV_BLOCK, share * SIDE), :] = dense[...].astype(jnp.bfloat16)


def conv_kernel(where, latents, halo, sums, other, gain, offset, temb, *refs):
    pieces, (out, weight, shifted, total, sems) = refs[: 2 * SIDE], refs[2 * SIDE :]
    fetch_blocks(where, pieces, weight, CONV_BLOCK, sems)
    rows, width, chans = latents.shape
    size = chans // GROUPS
    group = lax.broadcasted_iota(jnp.int32, (chans, chans), 0) // size
    same = group == lax.broadcasted_iota(jnp.int32, (chans, chans), 1) // size
    frame = jnp.dot(
        sums[...] + other[...],
        same.astype(jnp.float32),
        precision=lax.Precision.HIGHEST,
        preferred_element_type=jnp.float32,
    )
    entries = 2 * rows * width * size
    mean = frame[0:1] / entries
    var = frame[1:2] / entries - mean * mean
    scale = lax.rsqrt(var + 1e-05) * gain[...]
    bias = offset[...]
    column = lax.broadcasted_iota(jnp.int32, (width, 1), 0)
    lower = where[3]

    def fill(at, raw):
        values = (raw.astype(jnp.float32) - mean) * scale + bias
        values = values / (1.0 + jnp.exp(-values))
        left = jnp.where(column == 0, 0.0, pltpu.roll(values, 1, 0))
        right = jnp.where(column == width - 1, 0.0, pltpu.roll(values, width - 1, 0))
        shifted[0, at] = left.astype(jnp.bfloat16)
        shifted[1, at] = values.astype(jnp.bfloat16)
        shifted[2, at] = right.astype(jnp.bfloat16)

    def one_row(r, carry):
        fill(r + 1, latents[r])
        return carry

    lax.fori_loop(0, rows, one_row, 0)
    fill(jnp.where(lower == 1, 0, rows + 1), halo[0])
    empty = jnp.where(lower == 1, rows + 1, 0)
    for dx in range(3):
        shifted[dx, empty] = jnp.zeros((width, chans), jnp.bfloat16)
    for px in range(SIDE):
        await_line(weight, sems, px)
    base = latents[...].astype(jnp.float32).reshape(rows * width, chans)
    total[...] = base + temb[...]

    def one_row_of_taps(dy, carry):
        for dx in range(3):
            taken = shifted[dx, pl.ds(dy, rows)].reshape(rows * width, chans)
            at = pl.multiple_of((3 * dy + dx) * chans, 128)
            total[...] += jnp.dot(
                taken, weight[pl.ds(at, chans), :], preferred_element_type=jnp.float32
            )
        return carry

    lax.fori_loop(0, 3, one_row_of_taps, 0)
    out[...] = total[...].astype(jnp.bfloat16)


def layer_norm(values):
    mean = jnp.mean(values, axis=-1, keepdims=True)
    centered = values - mean
    var = jnp.mean(centered * centered, axis=-1, keepdims=True)
    return centered * lax.rsqrt(var + 1e-05)


def temporal_kernel(where, moved, gains, *refs):
    halves = refs[SIDE : SIDE + 2]
    pieces = [*refs[:SIDE]] + [halves[i // 4].at[i % 4] for i in range(SIDE)]
    out, tconv, dense, mid, qkv, attended, sems, dense_sem = refs[SIDE + 2 :]
    x, y, core = where[0], where[1], where[2]
    frames, places, chans = moved.shape
    fetch_blocks(where, pieces, tconv, TCONV_BLOCK, sems)
    share = chans // SIDE
    for slot, ref in enumerate(pieces):
        holder = holder_of(core, slot)
        at = wrap(jnp.where(holder == 0, y, x) + OFFSETS[slot % SIDE])
        for m in range(2):
            source = ref.at[pl.ds(SIDE * TCONV_BLOCK + m * share, share)]
            target = dense.at[2 * holder + m, pl.ds(pl.multiple_of(at * share, 16), share)]
            pltpu.make_async_copy(source, target, dense_sem).start()
    rows = frames * places
    values = moved[...].astype(jnp.float32).reshape(rows, chans)
    first = (layer_norm(values) * gains[0:1, :]).astype(jnp.bfloat16)
    zero = jnp.zeros((places, chans), jnp.bfloat16)
    before = jnp.concatenate([zero, first[:-places]], axis=0)
    after = jnp.concatenate([first[places:], zero], axis=0)
    for px in range(SIDE):
        await_line(tconv, sems, px)
    mid[...] = values + jnp.dot(
        before, tconv[:chans, :], preferred_element_type=jnp.float32
    )
    mid[...] += jnp.dot(first, tconv[chans : 2 * chans, :], preferred_element_type=jnp.float32)
    mid[...] += jnp.dot(after, tconv[2 * chans :, :], preferred_element_type=jnp.float32)
    second = (layer_norm(mid[...]) * gains[1:2, :]).astype(jnp.bfloat16)
    pltpu.make_async_copy(dense, dense, dense_sem).wait()
    for m in range(3):
        part = jnp.dot(second, dense[m], preferred_element_type=jnp.float32)
        qkv[m] = part.astype(jnp.bfloat16).reshape(frames, places, chans)
    some = 16
    many = frames * some
    row_place = lax.broadcasted_iota(jnp.int32, (many, many), 0) % some
    col_place = lax.broadcasted_iota(jnp.int32, (many, many), 1) % some
    same = row_place == col_place
    lane = lax.broadcasted_iota(jnp.int32, (1, 2 * HEAD), 1)

    def one_group(group, carry):
        spot = pl.ds(pl.multiple_of(group * some, some), some)
        for pair in range(chans // (2 * HEAD)):
            lanes = slice(pair * 2 * HEAD, (pair + 1) * 2 * HEAD)
            query = qkv[0, :, spot, lanes].reshape(many, 2 * HEAD)
            key = qkv[1, :, spot, lanes].reshape(many, 2 * HEAD)
            value = qkv[2, :, spot, lanes].reshape(many, 2 * HEAD)
            both = []
            for side in range(2):
                own = (lane < HEAD) if side == 0 else (lane >= HEAD)
                only = jnp.where(own, query, jnp.zeros_like(query))
                scores = lax.dot_general(
                    only, key, (((1,), (1,)), ((), ())), preferred_element_type=jnp.float32
                )
                scores = jnp.where(same, scores * HEAD ** (-0.5), -1e30)
                top = jnp.max(scores, axis=-1, keepdims=True)
                raised = jnp.exp(scores - top)
                weights = raised / jnp.sum(raised, axis=-1, keepdims=True)
                both.append(
                    jnp.dot(weights.astype(jnp.bfloat16), value, preferred_element_type=jnp.float32)
                )
            mixed = jnp.where(lane < HEAD, both[0], both[1]).astype(jnp.bfloat16)
            attended[:, spot, lanes] = mixed.reshape(frames, some, 2 * HEAD)
        return carry

    lax.fori_loop(0, places // some, one_group, 0)
    projected = jnp.dot(
        attended[...].reshape(rows, chans), dense[3], preferred_element_type=jnp.float32
    )
    out[...] = (mid[...] + projected).astype(jnp.bfloat16).reshape(frames, places, chans)


def specs(count):
    return [pl.BlockSpec(memory_space=pl.ANY)] * count


def shards(
    latents,
    norm_gain,
    norm_bias,
    conv_weight,
    time_weight,
    first_gain,
    tconv_weight,
    second_gain,
    qkv_weight,
    out_weight,
    timesteps,
):
    devices = lax.axis_size(SEQ)
    device = lax.axis_index(SEQ)
    x, y, core = (lax.axis_index(name) for name in SEQ)
    clips = timesteps.shape[0]
    images = clips * FRAMES
    rows, width, chans = latents.shape
    image = device % images
    clip = image // FRAMES
    lower = device // images
    bf16, f32 = jnp.bfloat16, jnp.float32

    where = jnp.stack([x, y, core, lower]).astype(jnp.int32)
    smem = pl.BlockSpec(memory_space=pltpu.SMEM)
    vmem = pl.BlockSpec(memory_space=pltpu.VMEM)
    params = pltpu.CompilerParams(vmem_limit_bytes=VMEM_LIMIT)

    conv_rows, tconv_rows = conv_weight.shape[0], tconv_weight.shape[0]
    few = qkv_weight.shape[0]

    def to_previous(px, py, pcore):
        spot = 2 * py + pcore - 1
        return None if spot < 0 else (px, spot // 2, spot % 2)

    some_rows = jax.ShapeDtypeStruct((2 * few, chans), bf16)
    both, query_key, crossed, value_out, edge, sums = pl.pallas_call(
        pack_kernel,
        out_shape=[
            jax.ShapeDtypeStruct((conv_rows + tconv_rows, chans), bf16),
            some_rows,
            some_rows,
            some_rows,
            jax.ShapeDtypeStruct((1, width, chans), bf16),
            jax.ShapeDtypeStruct((8, chans), f32),
        ],
        in_specs=[smem] + [vmem] * 5,
        out_specs=[vmem] * 6,
        scratch_shapes=[pltpu.VMEM((64, chans), f32), pltpu.VMEM((24, chans), f32)],
        name="pack",
    )(where, latents, conv_weight, tconv_weight, qkv_weight, out_weight)
    following = send(both, to_previous)
    same_core = send(query_key, lambda px, py, pcore: (py, px, 0) if pcore == 0 else None)
    crossed = send(crossed, lambda px, py, pcore: (px, py, 1) if pcore == 0 else (py, px, 0))

    pairs = [(i, (i + images) % devices) for i in range(devices)]
    halo = lax.ppermute(edge, SEQ, pairs)
    other = lax.ppermute(sums, SEQ, pairs)
    temb = time_embed(lax.dynamic_index_in_dim(timesteps, clip, 0, False), time_weight)
    following, halo, other = lax.optimization_barrier((following, halo, other))
    block = pl.pallas_call(
        cut_kernel,
        out_shape=jax.ShapeDtypeStruct((CONV_BLOCK + TCONV_BLOCK + 4 * few, chans), bf16),
        in_specs=[smem] + [vmem] * 5,
        out_specs=vmem,
        scratch_shapes=[
            pltpu.VMEM((112, chans), f32),
            pltpu.VMEM((32, chans), f32),
            pltpu.VMEM((24, chans), f32),
        ],
        name="cut",
    )(where, both, following, same_core, crossed, value_out)

    line = direct(block)
    conv_line, rest_line = pl.pallas_call(
        line_kernel,
        out_shape=[
            jax.ShapeDtypeStruct((SIDE * CONV_BLOCK, chans), bf16),
            jax.ShapeDtypeStruct((SIDE * (TCONV_BLOCK + 4 * few), chans), bf16),
        ],
        in_specs=[smem] + [vmem] * SIDE,
        out_specs=[vmem] * 2,
        scratch_shapes=[
            pltpu.VMEM((SIDE * 4 * few, chans), f32),
            pltpu.VMEM((SIDE, 4 * few, chans), f32),
        ],
        name="line",
    )(where, *line)
    conv_pieces, rest_pieces = two_rings(conv_line, rest_line)

    spatial = pl.pallas_call(
        conv_kernel,
        out_shape=jax.ShapeDtypeStruct((rows * width, chans), bf16),
        in_specs=[smem] + [vmem] * 7 + specs(2 * SIDE),
        out_specs=vmem,
        scratch_shapes=[
            pltpu.VMEM((9 * chans, chans), bf16),
            pltpu.VMEM((3, rows + 2, width, chans), bf16),
            pltpu.VMEM((rows * width, chans), f32),
            pltpu.SemaphoreType.DMA((SIDE,)),
        ],
        compiler_params=params,
        name="conv",
    )(where, latents, halo, sums, other, norm_gain[None], norm_bias[None], temb, *conv_pieces)
    spatial, rest_pieces = lax.optimization_barrier((spatial, rest_pieces))
    half = SIDE // 2
    halves = [send(jnp.stack(rest_pieces[at : at + half]), swap) for at in (0, half)]
    moved = lax.all_to_all(spatial, SEQ[1:], split_axis=0, concat_axis=0, tiled=True)
    places = rows * width // FRAMES
    result = pl.pallas_call(
        temporal_kernel,
        out_shape=jax.ShapeDtypeStruct((FRAMES, places, chans), bf16),
        in_specs=[smem, vmem, vmem] + specs(SIDE + 2),
        out_specs=vmem,
        scratch_shapes=[
            pltpu.VMEM((3 * chans, chans), bf16),
            pltpu.VMEM((4, chans, chans), bf16),
            pltpu.VMEM((FRAMES * places, chans), f32),
            pltpu.VMEM((3, FRAMES, places, chans), bf16),
            pltpu.VMEM((FRAMES, places, chans), bf16),
            pltpu.SemaphoreType.DMA((SIDE,)),
            pltpu.SemaphoreType.DMA,
        ],
        compiler_params=params,
        name="temporal",
    )(
        where,
        moved.reshape(FRAMES, places, chans),
        jnp.stack([first_gain, second_gain]),
        *rest_pieces,
        *halves,
    )
    returned = lax.all_to_all(
        result.reshape(rows * width, chans), SEQ[1:], split_axis=0, concat_axis=0, tiled=True
    )
    return returned.reshape(rows, width, chans)


def solution(mesh):
    torus = Mesh(
        mesh.devices.reshape(mesh.shape["groups"], SIDE, SIDE, 2),
        ("groups", "seq_0", "seq_1", "seq_2"),
    )
    return jax.shard_map(
        shards,
        mesh=torus,
        in_specs=(
            P(GROUPS_SEQ, None, None),
            P(),
            P(),
            P(SEQ, None),
            P(),
            P(),
            P(SEQ, None),
            P(),
            P(SEQ, None),
            P(SEQ, None),
            P("groups"),
        ),
        out_specs=P(GROUPS_SEQ, None, None),
        check_vma=False,
    )
```

```python
import jax
import jax.numpy as jnp
from jax import lax
from jax.experimental import pallas as pl
from jax.experimental.pallas import tpu as pltpu
from jax.sharding import Mesh
from jax.sharding import PartitionSpec as P

HEAD = 64
GROUPS = 32
TFEAT = 320
FRAMES = 16
SEQ = ("seq_0", "seq_1", "seq_2")
GROUPS_SEQ = ("groups", "seq_0", "seq_1", "seq_2")
SIDE = 8
CONV_BLOCK = 48
TCONV_BLOCK = 16
SUM_ROWS = 16
VMEM_LIMIT = 56 * 2**20
OFFSETS = (0, -1, -2, -3, -4, 1, 2, 3)


def route(target):
    pairs = []
    for x in range(SIDE):
        for y in range(SIDE):
            for core in range(2):
                there = target(x, y, core)
                if there is not None:
                    tx, ty, tcore = there
                    to = (tx % SIDE * SIDE + ty % SIDE) * 2 + tcore
                    pairs.append(((x * SIDE + y) * 2 + core, to))
    return pairs


def send(block, target):
    return lax.ppermute(block, SEQ, route(target))


def inner(step):
    return lambda x, y, core: (x + step, y, core) if core == 0 else (x, y + step, core)


def outer(step):
    return lambda x, y, core: (x, y + step, core) if core == 0 else (x + step, y, core)


def swap(x, y, core):
    return x, y, 1 - core


def lines():
    device = lambda x, y, core: (x * SIDE + y) * 2 + core
    even = [[device(x, y, 0) for x in range(SIDE)] for y in range(SIDE)]
    return even + [[device(x, y, 1) for y in range(SIDE)] for x in range(SIDE)]


def two_rings(first, second, early):
    chains = {}
    for sign in (1, -1):
        chains[sign] = ([first], [second])
    for step in range(SIDE // 2):
        for sign, steps in ((1, SIDE // 2), (-1, SIDE // 2 - 1)):
            if step >= steps:
                continue
            one, two = chains[sign]
            if step == 2 and sign == 1:
                one[-1], early = lax.optimization_barrier((one[-1], early))
            if step > 1:
                one[-1], two[-2] = lax.optimization_barrier((one[-1], two[-2]))
            if step > 0:
                two[-1], one[-1] = lax.optimization_barrier((two[-1], one[-1]))
            one.append(send(one[-1], outer(sign)))
            two.append(send(two[-1], outer(sign)))
    own = [chains[1][i] + chains[-1][i][1:] for i in range(2)]
    return own[0] + [send(piece, swap) for piece in own[0]], own[1], early


def time_embed(timestep, time_weight):
    half = TFEAT // 2
    freqs = jnp.exp(-jnp.log(10000.0) * jnp.arange(half, dtype=jnp.float32) / half)
    angles = timestep.astype(jnp.float32)[None, None] * freqs[None, :]
    feats = jnp.concatenate([jnp.cos(angles), jnp.sin(angles)], axis=-1)
    return jnp.dot(feats, time_weight.astype(jnp.float32), precision=lax.Precision.HIGHEST)


def wrap(value):
    return lax.rem(value + 2 * SIDE, SIDE)


def holder_of(core, slot):
    return core if slot < SIDE else 1 - core


def fetch_blocks(where, pieces, weight, size, sems):
    x, y, core = where[0], where[1], where[2]
    for slot, ref in enumerate(pieces):
        holder = holder_of(core, slot)
        across = OFFSETS[slot % SIDE]

        def one(b, carry, ref=ref, holder=holder, across=across):
            px = jnp.where(holder == 0, b, wrap(x + across))
            py = jnp.where(holder == 0, wrap(y + across), b)
            inside = 2 * py + holder

            @pl.when(inside < 2 * SIDE - 1)
            def _():
                at = pl.multiple_of((px * (2 * SIDE - 1) + inside) * size, size)
                source = ref.at[pl.ds(pl.multiple_of(b * size, size), size)]
                target = weight.at[pl.ds(at, size)]
                pltpu.make_async_copy(source, target, sems.at[px]).start()

            return carry

        lax.fori_loop(0, SIDE, one, 0)


def await_line(weight, sems, px):
    size = weight.shape[0] // SIDE
    part = weight.at[pl.ds(px * size, size)]
    pltpu.make_async_copy(part, part, sems.at[px]).wait()


def pack_kernel(where, latents, conv, tconv, qkv, last, *refs):
    both, query_key, crossed, value_out, edge, rows, few = refs
    conv_rows, chans = conv.shape
    count = qkv.shape[0]
    f32, bf16 = jnp.float32, jnp.bfloat16
    rows[pl.ds(0, conv_rows), :] = conv[...].astype(f32)
    rows[pl.ds(conv_rows, tconv.shape[0]), :] = tconv[...].astype(f32)
    both[...] = rows[pl.ds(0, both.shape[0]), :].astype(bf16)
    for m in range(3):
        few[pl.ds(m * count, count), :] = qkv[:, m * chans : (m + 1) * chans].astype(f32)
    few[pl.ds(3 * count, count), :] = last[...].astype(f32)
    head = few[pl.ds(0, 2 * count), :].astype(bf16)
    tail = few[pl.ds(2 * count, 2 * count), :].astype(bf16)
    query_key[...] = head
    value_out[...] = tail
    crossed[...] = jnp.where(where[2] == 0, tail.astype(f32), head.astype(f32)).astype(bf16)
    width = latents.shape[1]
    edge[pl.ds(0, width), :] = latents[jnp.where(where[3] == 1, 0, latents.shape[0] - 1)]
    values = latents[0].astype(f32)
    first, second = values, values * values
    for r in range(1, latents.shape[0]):
        values = latents[r].astype(f32)
        first, second = first + values, second + values * values
    left = jnp.concatenate([jnp.sum(v, axis=0, keepdims=True) for v in (first, second)], axis=0)
    few[...] = jnp.zeros(few.shape, f32)
    for part in range(3):
        high = left.astype(bf16).astype(f32)
        few[pl.ds(2 * part, 2), :] = high
        left = left - high
    edge[pl.ds(width, SUM_ROWS), :] = few[pl.ds(0, SUM_ROWS), :].astype(bf16)


def cut_kernel(where, both, following, same_core, crossed, value_out, block, conv, tconv, few):
    f32, bf16 = jnp.float32, jnp.bfloat16
    count = same_core.shape[0] // 2
    tconv_rows = TCONV_BLOCK - 1
    conv_rows = both.shape[0] - tconv_rows
    inside = 2 * where[1] + where[2]
    own, next_rows = both[...].astype(f32), following[...].astype(f32)
    conv[pl.ds(0, both.shape[0]), :] = own
    tconv[pl.ds(0, tconv_rows), :] = conv[pl.ds(conv_rows, tconv_rows), :]
    conv[pl.ds(conv_rows, both.shape[0]), :] = next_rows
    tconv[pl.ds(tconv_rows, tconv_rows), :] = conv[pl.ds(2 * conv_rows, tconv_rows), :]
    conv_at = jnp.minimum((CONV_BLOCK - conv_rows) * inside, 2 * conv_rows - CONV_BLOCK)
    tconv_at = jnp.minimum(inside, 2 * tconv_rows - TCONV_BLOCK)
    turned = pltpu.roll(conv[...], lax.rem(conv.shape[0] - conv_at, conv.shape[0]), 0)
    block[pl.ds(0, CONV_BLOCK), :] = turned[:CONV_BLOCK].astype(bf16)
    turned = pltpu.roll(tconv[...], lax.rem(tconv.shape[0] - tconv_at, tconv.shape[0]), 0)
    block[pl.ds(CONV_BLOCK, TCONV_BLOCK), :] = turned[:TCONV_BLOCK].astype(bf16)
    near, far, kept = same_core[...].astype(f32), crossed[...].astype(f32), value_out[...].astype(f32)
    even = jnp.where(where[2] == 0, near, far)
    odd = jnp.where(where[2] == 0, far, kept)
    conv[pl.ds(0, 2 * count), :] = even
    conv[pl.ds(2 * count, 2 * count), :] = odd
    for m in range(2):
        for parity in range(2):
            source = conv[pl.ds((2 * parity + m) * count, count), :]
            few[pl.ds((2 * m + parity) * count, count), :] = source
    dense = few[pl.ds(0, 4 * count), :].astype(bf16)
    block[pl.ds(CONV_BLOCK + TCONV_BLOCK, 4 * count), :] = dense


def line_kernel(blocks, conv, rest, dense):
    start = CONV_BLOCK + TCONV_BLOCK
    share = blocks.shape[1] - start
    half = share // 2
    for b in range(SIDE):
        conv[pl.ds(b * CONV_BLOCK, CONV_BLOCK), :] = blocks[b, pl.ds(0, CONV_BLOCK), :]
        taken = blocks[b, pl.ds(CONV_BLOCK, TCONV_BLOCK), :]
        rest[pl.ds(b * TCONV_BLOCK, TCONV_BLOCK), :] = taken
        rows = blocks[b, pl.ds(start, share), :].astype(jnp.float32)
        for m in range(2):
            target = pl.ds((m * SIDE + b) * half, half)
            dense[target, :] = rows[m * half : (m + 1) * half]
    rest[pl.ds(SIDE * TCONV_BLOCK, share * SIDE), :] = dense[...].astype(jnp.bfloat16)


def conv_kernel(where, latents, edge, halo, gain, offset, temb, *refs):
    pieces, (out, weight, shifted, total, sems) = refs[: 2 * SIDE], refs[2 * SIDE :]
    fetch_blocks(where, pieces, weight, CONV_BLOCK, sems)
    rows, width, chans = latents.shape
    size = chans // GROUPS
    group = lax.broadcasted_iota(jnp.int32, (chans, chans), 0) // size
    same = group == lax.broadcasted_iota(jnp.int32, (chans, chans), 1) // size
    parts = edge[pl.ds(width, SUM_ROWS), :].astype(jnp.float32)
    parts = parts + halo[pl.ds(width, SUM_ROWS), :].astype(jnp.float32)
    sums = parts[0:2] + parts[2:4] + parts[4:6]
    frame = jnp.dot(
        jnp.concatenate([sums] * 4, axis=0),
        same.astype(jnp.float32),
        precision=lax.Precision.HIGHEST,
        preferred_element_type=jnp.float32,
    )
    entries = 2 * rows * width * size
    mean = frame[0:1] / entries
    var = frame[1:2] / entries - mean * mean
    scale = lax.rsqrt(var + 1e-05) * gain[...]
    bias = offset[...]
    column = lax.broadcasted_iota(jnp.int32, (width, 1), 0)
    lower = where[3]

    def fill(at, raw):
        values = (raw.astype(jnp.float32) - mean) * scale + bias
        values = values / (1.0 + jnp.exp(-values))
        left = jnp.where(column == 0, 0.0, pltpu.roll(values, 1, 0))
        right = jnp.where(column == width - 1, 0.0, pltpu.roll(values, width - 1, 0))
        shifted[0, at] = left.astype(jnp.bfloat16)
        shifted[1, at] = values.astype(jnp.bfloat16)
        shifted[2, at] = right.astype(jnp.bfloat16)

    def one_row(r, carry):
        fill(r + 1, latents[r])
        return carry

    lax.fori_loop(0, rows, one_row, 0)
    fill(jnp.where(lower == 1, 0, rows + 1), halo[pl.ds(0, width), :])
    empty = jnp.where(lower == 1, rows + 1, 0)
    for dx in range(3):
        shifted[dx, empty] = jnp.zeros((width, chans), jnp.bfloat16)
    for px in range(SIDE):
        await_line(weight, sems, px)
    base = latents[...].astype(jnp.float32).reshape(rows * width, chans)
    total[...] = base + temb[...]

    def one_row_of_taps(dy, carry):
        for dx in range(3):
            taken = shifted[dx, pl.ds(dy, rows)].reshape(rows * width, chans)
            at = pl.multiple_of((3 * dy + dx) * chans, 128)
            total[...] += jnp.dot(
                taken, weight[pl.ds(at, chans), :], preferred_element_type=jnp.float32
            )
        return carry

    lax.fori_loop(0, 3, one_row_of_taps, 0)
    out[...] = total[...].astype(jnp.bfloat16)


def layer_norm(values):
    mean = jnp.mean(values, axis=-1, keepdims=True)
    centered = values - mean
    var = jnp.mean(centered * centered, axis=-1, keepdims=True)
    return centered * lax.rsqrt(var + 1e-05)


def temporal_kernel(where, moved, gains, *refs):
    halves = refs[SIDE : SIDE + 2]
    pieces = [*refs[:SIDE]] + [halves[i // 4].at[i % 4] for i in range(SIDE)]
    out, tconv, dense, mid, qkv, attended, sems, dense_sem = refs[SIDE + 2 :]
    x, y, core = where[0], where[1], where[2]
    frames, places, chans = moved.shape
    fetch_blocks(where, pieces, tconv, TCONV_BLOCK, sems)
    share = chans // SIDE
    for slot, ref in enumerate(pieces):
        holder = holder_of(core, slot)
        at = wrap(jnp.where(holder == 0, y, x) + OFFSETS[slot % SIDE])
        for m in range(2):
            source = ref.at[pl.ds(SIDE * TCONV_BLOCK + m * share, share)]
            target = dense.at[2 * holder + m, pl.ds(pl.multiple_of(at * share, 16), share)]
            pltpu.make_async_copy(source, target, dense_sem).start()
    rows = frames * places
    values = moved[...].astype(jnp.float32).reshape(rows, chans)
    first = (layer_norm(values) * gains[0:1, :]).astype(jnp.bfloat16)
    zero = jnp.zeros((places, chans), jnp.bfloat16)
    before = jnp.concatenate([zero, first[:-places]], axis=0)
    after = jnp.concatenate([first[places:], zero], axis=0)
    for px in range(SIDE):
        await_line(tconv, sems, px)
    mid[...] = values + jnp.dot(
        before, tconv[:chans, :], preferred_element_type=jnp.float32
    )
    mid[...] += jnp.dot(first, tconv[chans : 2 * chans, :], preferred_element_type=jnp.float32)
    mid[...] += jnp.dot(after, tconv[2 * chans :, :], preferred_element_type=jnp.float32)
    second = (layer_norm(mid[...]) * gains[1:2, :]).astype(jnp.bfloat16)
    pltpu.make_async_copy(dense, dense, dense_sem).wait()
    for m in range(3):
        part = jnp.dot(second, dense[m], preferred_element_type=jnp.float32)
        qkv[m] = part.astype(jnp.bfloat16).reshape(frames, places, chans)
    some = 16
    many = frames * some
    row_place = lax.broadcasted_iota(jnp.int32, (many, many), 0) % some
    col_place = lax.broadcasted_iota(jnp.int32, (many, many), 1) % some
    same = row_place == col_place
    lane = lax.broadcasted_iota(jnp.int32, (1, 2 * HEAD), 1)
    for group in range(places // some):
        spot = slice(group * some, (group + 1) * some)
        for pair in range(chans // (2 * HEAD)):
            lanes = slice(pair * 2 * HEAD, (pair + 1) * 2 * HEAD)
            query = qkv[0, :, spot, lanes].reshape(many, 2 * HEAD)
            key = qkv[1, :, spot, lanes].reshape(many, 2 * HEAD)
            value = qkv[2, :, spot, lanes].reshape(many, 2 * HEAD)
            both = []
            for side in range(2):
                own = (lane < HEAD) if side == 0 else (lane >= HEAD)
                only = jnp.where(own, query, jnp.zeros_like(query))
                scores = lax.dot_general(
                    only, key, (((1,), (1,)), ((), ())), preferred_element_type=jnp.float32
                )
                scores = jnp.where(same, scores * HEAD ** (-0.5), -1e30)
                top = jnp.max(scores, axis=-1, keepdims=True)
                raised = jnp.exp(scores - top)
                weights = raised / jnp.sum(raised, axis=-1, keepdims=True)
                both.append(
                    jnp.dot(weights.astype(jnp.bfloat16), value, preferred_element_type=jnp.float32)
                )
            mixed = jnp.where(lane < HEAD, both[0], both[1]).astype(jnp.bfloat16)
            attended[:, spot, lanes] = mixed.reshape(frames, some, 2 * HEAD)
    projected = jnp.dot(
        attended[...].reshape(rows, chans), dense[3], preferred_element_type=jnp.float32
    )
    out[...] = (mid[...] + projected).astype(jnp.bfloat16).reshape(frames, places, chans)


def specs(count):
    return [pl.BlockSpec(memory_space=pl.ANY)] * count


def shards(
    latents,
    norm_gain,
    norm_bias,
    conv_weight,
    time_weight,
    first_gain,
    tconv_weight,
    second_gain,
    qkv_weight,
    out_weight,
    timesteps,
):
    devices = lax.axis_size(SEQ)
    device = lax.axis_index(SEQ)
    x, y, core = (lax.axis_index(name) for name in SEQ)
    clips = timesteps.shape[0]
    images = clips * FRAMES
    rows, width, chans = latents.shape
    image = device % images
    clip = image // FRAMES
    lower = device // images
    bf16, f32 = jnp.bfloat16, jnp.float32

    where = jnp.stack([x, y, core, lower]).astype(jnp.int32)
    smem = pl.BlockSpec(memory_space=pltpu.SMEM)
    vmem = pl.BlockSpec(memory_space=pltpu.VMEM)
    params = pltpu.CompilerParams(vmem_limit_bytes=VMEM_LIMIT)

    conv_rows, tconv_rows = conv_weight.shape[0], tconv_weight.shape[0]
    few = qkv_weight.shape[0]

    def to_previous(px, py, pcore):
        spot = 2 * py + pcore - 1
        return None if spot < 0 else (px, spot // 2, spot % 2)

    some_rows = jax.ShapeDtypeStruct((2 * few, chans), bf16)
    both, query_key, crossed, value_out, edge = pl.pallas_call(
        pack_kernel,
        out_shape=[
            jax.ShapeDtypeStruct((conv_rows + tconv_rows, chans), bf16),
            some_rows,
            some_rows,
            some_rows,
            jax.ShapeDtypeStruct((width + SUM_ROWS, chans), bf16),
        ],
        in_specs=[smem] + [vmem] * 5,
        out_specs=[vmem] * 5,
        scratch_shapes=[pltpu.VMEM((64, chans), f32), pltpu.VMEM((24, chans), f32)],
        name="pack",
    )(where, latents, conv_weight, tconv_weight, qkv_weight, out_weight)
    following = send(both, to_previous)
    same_core = send(query_key, lambda px, py, pcore: (py, px, 0) if pcore == 0 else None)
    crossed = send(crossed, lambda px, py, pcore: (px, py, 1) if pcore == 0 else (py, px, 0))

    pairs = [(i, (i + images) % devices) for i in range(devices)]
    halo = lax.ppermute(edge, SEQ, pairs)
    temb = time_embed(lax.dynamic_index_in_dim(timesteps, clip, 0, False), time_weight)
    following, halo = lax.optimization_barrier((following, halo))
    block = pl.pallas_call(
        cut_kernel,
        out_shape=jax.ShapeDtypeStruct((CONV_BLOCK + TCONV_BLOCK + 4 * few, chans), bf16),
        in_specs=[smem] + [vmem] * 5,
        out_specs=vmem,
        scratch_shapes=[
            pltpu.VMEM((112, chans), f32),
            pltpu.VMEM((32, chans), f32),
            pltpu.VMEM((24, chans), f32),
        ],
        name="cut",
    )(where, both, following, same_core, crossed, value_out)

    line = lax.all_to_all(
        jnp.broadcast_to(block[None], (SIDE, *block.shape)),
        SEQ,
        split_axis=0,
        concat_axis=0,
        axis_index_groups=lines(),
        tiled=True,
    )
    conv_line, rest_line = pl.pallas_call(
        line_kernel,
        out_shape=[
            jax.ShapeDtypeStruct((SIDE * CONV_BLOCK, chans), bf16),
            jax.ShapeDtypeStruct((SIDE * (TCONV_BLOCK + 4 * few), chans), bf16),
        ],
        in_specs=[vmem],
        out_specs=[vmem] * 2,
        scratch_shapes=[pltpu.VMEM((SIDE * 4 * few, chans), f32)],
        name="line",
    )(line)
    early = (norm_gain[None], norm_bias[None], temb, jnp.stack([first_gain, second_gain]))
    conv_pieces, rest_pieces, early = two_rings(conv_line, rest_line, early)
    gain, bias, temb, gains = early

    spatial = pl.pallas_call(
        conv_kernel,
        out_shape=jax.ShapeDtypeStruct((rows * width, chans), bf16),
        in_specs=[smem] + [vmem] * 6 + specs(2 * SIDE),
        out_specs=vmem,
        scratch_shapes=[
            pltpu.VMEM((9 * chans, chans), bf16),
            pltpu.VMEM((3, rows + 2, width, chans), bf16),
            pltpu.VMEM((rows * width, chans), f32),
            pltpu.SemaphoreType.DMA((SIDE,)),
        ],
        compiler_params=params,
        name="conv",
    )(where, latents, edge, halo, gain, bias, temb, *conv_pieces)
    spatial, rest_pieces = lax.optimization_barrier((spatial, rest_pieces))
    half = SIDE // 2
    halves = [send(jnp.stack(rest_pieces[at : at + half]), swap) for at in (0, half)]
    moved = lax.all_to_all(spatial, SEQ[1:], split_axis=0, concat_axis=0, tiled=True)
    places = rows * width // FRAMES
    result = pl.pallas_call(
        temporal_kernel,
        out_shape=jax.ShapeDtypeStruct((FRAMES, places, chans), bf16),
        in_specs=[smem, vmem, vmem] + specs(SIDE + 2),
        out_specs=vmem,
        scratch_shapes=[
            pltpu.VMEM((3 * chans, chans), bf16),
            pltpu.VMEM((4, chans, chans), bf16),
            pltpu.VMEM((FRAMES * places, chans), f32),
            pltpu.VMEM((3, FRAMES, places, chans), bf16),
            pltpu.VMEM((FRAMES, places, chans), bf16),
            pltpu.SemaphoreType.DMA((SIDE,)),
            pltpu.SemaphoreType.DMA,
        ],
        compiler_params=params,
        name="temporal",
    )(
        where,
        moved.reshape(FRAMES, places, chans),
        gains,
        *rest_pieces,
        *halves,
    )
    returned = lax.all_to_all(
        result.reshape(rows * width, chans), SEQ[1:], split_axis=0, concat_axis=0, tiled=True
    )
    return returned.reshape(rows, width, chans)


def solution(mesh):
    torus = Mesh(
        mesh.devices.reshape(mesh.shape["groups"], SIDE, SIDE, 2),
        ("groups", "seq_0", "seq_1", "seq_2"),
    )
    return jax.shard_map(
        shards,
        mesh=torus,
        in_specs=(
            P(GROUPS_SEQ, None, None),
            P(),
            P(),
            P(SEQ, None),
            P(),
            P(),
            P(SEQ, None),
            P(),
            P(SEQ, None),
            P(SEQ, None),
            P("groups"),
        ),
        out_specs=P(GROUPS_SEQ, None, None),
        check_vma=False,
    )
```

```python
import jax
import jax.numpy as jnp
from jax import lax
from jax.experimental import pallas as pl
from jax.experimental.pallas import tpu as pltpu
from jax.sharding import Mesh
from jax.sharding import PartitionSpec as P

HEAD = 64
GROUPS = 32
TFEAT = 320
FRAMES = 16
SEQ = ("seq_0", "seq_1", "seq_2")
GROUPS_SEQ = ("groups", "seq_0", "seq_1", "seq_2")
SIDE = 8
CONV_BLOCK = 48
TCONV_BLOCK = 16
SUM_ROWS = 16
VMEM_LIMIT = 56 * 2**20
OFFSETS = (0, -1, -2, -3, -4, 1, 2, 3)


def route(target):
    pairs = []
    for x in range(SIDE):
        for y in range(SIDE):
            for core in range(2):
                there = target(x, y, core)
                if there is not None:
                    tx, ty, tcore = there
                    to = (tx % SIDE * SIDE + ty % SIDE) * 2 + tcore
                    pairs.append(((x * SIDE + y) * 2 + core, to))
    return pairs


def send(block, target):
    return lax.ppermute(block, SEQ, route(target))


def inner(step):
    return lambda x, y, core: (x + step, y, core) if core == 0 else (x, y + step, core)


def outer(step):
    return lambda x, y, core: (x, y + step, core) if core == 0 else (x + step, y, core)


def swap(x, y, core):
    return x, y, 1 - core


def lines():
    device = lambda x, y, core: (x * SIDE + y) * 2 + core
    even = [[device(x, y, 0) for x in range(SIDE)] for y in range(SIDE)]
    return even + [[device(x, y, 1) for y in range(SIDE)] for x in range(SIDE)]


def two_rings(first, second, early):
    chains = {}
    for sign in (1, -1):
        chains[sign] = ([first], [second])
    for step in range(SIDE // 2):
        for sign, steps in ((1, SIDE // 2), (-1, SIDE // 2 - 1)):
            if step >= steps:
                continue
            one, two = chains[sign]
            if step == 2 and sign == 1:
                one[-1], early = lax.optimization_barrier((one[-1], early))
            if step > 1:
                one[-1], two[-2] = lax.optimization_barrier((one[-1], two[-2]))
            if step > 0:
                two[-1], one[-1] = lax.optimization_barrier((two[-1], one[-1]))
            one.append(send(one[-1], outer(sign)))
            two.append(send(two[-1], outer(sign)))
    own = [chains[1][i] + chains[-1][i][1:] for i in range(2)]
    return own[0] + [send(piece, swap) for piece in own[0]], own[1], early


def time_embed(timestep, time_weight):
    half = TFEAT // 2
    freqs = jnp.exp(-jnp.log(10000.0) * jnp.arange(half, dtype=jnp.float32) / half)
    angles = timestep.astype(jnp.float32)[None, None] * freqs[None, :]
    feats = jnp.concatenate([jnp.cos(angles), jnp.sin(angles)], axis=-1)
    return jnp.dot(feats, time_weight.astype(jnp.float32), precision=lax.Precision.HIGHEST)


def wrap(value):
    return lax.rem(value + 2 * SIDE, SIDE)


def holder_of(core, slot):
    return core if slot < SIDE else 1 - core


def fetch_blocks(where, pieces, weight, size, sems):
    x, y, core = where[0], where[1], where[2]
    for slot, ref in enumerate(pieces):
        holder = holder_of(core, slot)
        across = OFFSETS[slot % SIDE]

        def one(b, carry, ref=ref, holder=holder, across=across):
            px = jnp.where(holder == 0, b, wrap(x + across))
            py = jnp.where(holder == 0, wrap(y + across), b)
            inside = 2 * py + holder

            @pl.when(inside < 2 * SIDE - 1)
            def _():
                at = pl.multiple_of((px * (2 * SIDE - 1) + inside) * size, size)
                source = ref.at[pl.ds(pl.multiple_of(b * size, size), size)]
                target = weight.at[pl.ds(at, size)]
                pltpu.make_async_copy(source, target, sems.at[px]).start()

            return carry

        lax.fori_loop(0, SIDE, one, 0)


def await_line(weight, sems, px):
    size = weight.shape[0] // SIDE
    part = weight.at[pl.ds(px * size, size)]
    pltpu.make_async_copy(part, part, sems.at[px]).wait()


def pack_kernel(where, latents, conv, tconv, qkv, last, *refs):
    both, query_key, crossed, value_out, edge, rows, few = refs
    conv_rows, chans = conv.shape
    count = qkv.shape[0]
    f32, bf16 = jnp.float32, jnp.bfloat16
    rows[pl.ds(0, conv_rows), :] = conv[...].astype(f32)
    rows[pl.ds(conv_rows, tconv.shape[0]), :] = tconv[...].astype(f32)
    both[...] = rows[pl.ds(0, both.shape[0]), :].astype(bf16)
    for m in range(3):
        few[pl.ds(m * count, count), :] = qkv[:, m * chans : (m + 1) * chans].astype(f32)
    few[pl.ds(3 * count, count), :] = last[...].astype(f32)
    head = few[pl.ds(0, 2 * count), :].astype(bf16)
    tail = few[pl.ds(2 * count, 2 * count), :].astype(bf16)
    query_key[...] = head
    value_out[...] = tail
    crossed[...] = jnp.where(where[2] == 0, tail.astype(f32), head.astype(f32)).astype(bf16)
    width = latents.shape[1]
    edge[pl.ds(0, width), :] = latents[jnp.where(where[3] == 1, 0, latents.shape[0] - 1)]
    values = latents[0].astype(f32)
    first, second = values, values * values
    for r in range(1, latents.shape[0]):
        values = latents[r].astype(f32)
        first, second = first + values, second + values * values
    left = jnp.concatenate([jnp.sum(v, axis=0, keepdims=True) for v in (first, second)], axis=0)
    few[...] = jnp.zeros(few.shape, f32)
    for part in range(3):
        high = left.astype(bf16).astype(f32)
        few[pl.ds(2 * part, 2), :] = high
        left = left - high
    edge[pl.ds(width, SUM_ROWS), :] = few[pl.ds(0, SUM_ROWS), :].astype(bf16)


def cut_kernel(where, both, following, same_core, crossed, value_out, copies, *scratch):
    block, conv, tconv, few = scratch
    f32, bf16 = jnp.float32, jnp.bfloat16
    count = same_core.shape[0] // 2
    tconv_rows = TCONV_BLOCK - 1
    conv_rows = both.shape[0] - tconv_rows
    inside = 2 * where[1] + where[2]
    own, next_rows = both[...].astype(f32), following[...].astype(f32)
    conv[pl.ds(0, both.shape[0]), :] = own
    tconv[pl.ds(0, tconv_rows), :] = conv[pl.ds(conv_rows, tconv_rows), :]
    conv[pl.ds(conv_rows, both.shape[0]), :] = next_rows
    tconv[pl.ds(tconv_rows, tconv_rows), :] = conv[pl.ds(2 * conv_rows, tconv_rows), :]
    conv_at = jnp.minimum((CONV_BLOCK - conv_rows) * inside, 2 * conv_rows - CONV_BLOCK)
    tconv_at = jnp.minimum(inside, 2 * tconv_rows - TCONV_BLOCK)
    turned = pltpu.roll(conv[...], lax.rem(conv.shape[0] - conv_at, conv.shape[0]), 0)
    block[pl.ds(0, CONV_BLOCK), :] = turned[:CONV_BLOCK].astype(bf16)
    turned = pltpu.roll(tconv[...], lax.rem(tconv.shape[0] - tconv_at, tconv.shape[0]), 0)
    block[pl.ds(CONV_BLOCK, TCONV_BLOCK), :] = turned[:TCONV_BLOCK].astype(bf16)
    near, far, kept = same_core[...].astype(f32), crossed[...].astype(f32), value_out[...].astype(f32)
    even = jnp.where(where[2] == 0, near, far)
    odd = jnp.where(where[2] == 0, far, kept)
    conv[pl.ds(0, 2 * count), :] = even
    conv[pl.ds(2 * count, 2 * count), :] = odd
    for m in range(2):
        for parity in range(2):
            source = conv[pl.ds((2 * parity + m) * count, count), :]
            few[pl.ds((2 * m + parity) * count, count), :] = source
    dense = few[pl.ds(0, 4 * count), :].astype(bf16)
    block[pl.ds(CONV_BLOCK + TCONV_BLOCK, 4 * count), :] = dense
    for b in range(SIDE):
        copies[b] = block[...]


def line_kernel(blocks, conv, rest, dense):
    start = CONV_BLOCK + TCONV_BLOCK
    share = blocks.shape[1] - start
    half = share // 2
    for b in range(SIDE):
        conv[pl.ds(b * CONV_BLOCK, CONV_BLOCK), :] = blocks[b, pl.ds(0, CONV_BLOCK), :]
        taken = blocks[b, pl.ds(CONV_BLOCK, TCONV_BLOCK), :]
        rest[pl.ds(b * TCONV_BLOCK, TCONV_BLOCK), :] = taken
        rows = blocks[b, pl.ds(start, share), :].astype(jnp.float32)
        for m in range(2):
            target = pl.ds((m * SIDE + b) * half, half)
            dense[target, :] = rows[m * half : (m + 1) * half]
    rest[pl.ds(SIDE * TCONV_BLOCK, share * SIDE), :] = dense[...].astype(jnp.bfloat16)


def conv_kernel(where, latents, edge, halo, gain, offset, temb, *refs):
    pieces, (out, weight, shifted, total, sems) = refs[: 2 * SIDE], refs[2 * SIDE :]
    fetch_blocks(where, pieces, weight, CONV_BLOCK, sems)
    rows, width, chans = latents.shape
    size = chans // GROUPS
    group = lax.broadcasted_iota(jnp.int32, (chans, chans), 0) // size
    same = group == lax.broadcasted_iota(jnp.int32, (chans, chans), 1) // size
    parts = edge[pl.ds(width, SUM_ROWS), :].astype(jnp.float32)
    parts = parts + halo[pl.ds(width, SUM_ROWS), :].astype(jnp.float32)
    sums = parts[0:2] + parts[2:4] + parts[4:6]
    frame = jnp.dot(
        jnp.concatenate([sums] * 4, axis=0),
        same.astype(jnp.float32),
        precision=lax.Precision.HIGHEST,
        preferred_element_type=jnp.float32,
    )
    entries = 2 * rows * width * size
    mean = frame[0:1] / entries
    var = frame[1:2] / entries - mean * mean
    scale = lax.rsqrt(var + 1e-05) * gain[...][None, :]
    bias = offset[...][None, :]
    column = lax.broadcasted_iota(jnp.int32, (width, 1), 0)
    lower = where[3]

    def fill(at, raw):
        values = (raw.astype(jnp.float32) - mean) * scale + bias
        values = values / (1.0 + jnp.exp(-values))
        left = jnp.where(column == 0, 0.0, pltpu.roll(values, 1, 0))
        right = jnp.where(column == width - 1, 0.0, pltpu.roll(values, width - 1, 0))
        shifted[0, at] = left.astype(jnp.bfloat16)
        shifted[1, at] = values.astype(jnp.bfloat16)
        shifted[2, at] = right.astype(jnp.bfloat16)

    def one_row(r, carry):
        fill(r + 1, latents[r])
        return carry

    lax.fori_loop(0, rows, one_row, 0)
    fill(jnp.where(lower == 1, 0, rows + 1), halo[pl.ds(0, width), :])
    empty = jnp.where(lower == 1, rows + 1, 0)
    for dx in range(3):
        shifted[dx, empty] = jnp.zeros((width, chans), jnp.bfloat16)
    for px in range(SIDE):
        await_line(weight, sems, px)
    base = latents[...].astype(jnp.float32).reshape(rows * width, chans)
    total[...] = base + temb[...]

    def one_row_of_taps(dy, carry):
        for dx in range(3):
            taken = shifted[dx, pl.ds(dy, rows)].reshape(rows * width, chans)
            at = pl.multiple_of((3 * dy + dx) * chans, 128)
            total[...] += jnp.dot(
                taken, weight[pl.ds(at, chans), :], preferred_element_type=jnp.float32
            )
        return carry

    lax.fori_loop(0, 3, one_row_of_taps, 0)
    out[...] = total[...].astype(jnp.bfloat16)


def layer_norm(values):
    mean = jnp.mean(values, axis=-1, keepdims=True)
    centered = values - mean
    var = jnp.mean(centered * centered, axis=-1, keepdims=True)
    return centered * lax.rsqrt(var + 1e-05)


def temporal_kernel(where, moved, first_gain, second_gain, *refs):
    halves = refs[SIDE : SIDE + 2]
    pieces = [*refs[:SIDE]] + [halves[i // 4].at[i % 4] for i in range(SIDE)]
    out, tconv, dense, mid, qkv, attended, sems, dense_sem = refs[SIDE + 2 :]
    x, y, core = where[0], where[1], where[2]
    frames, places, chans = moved.shape
    fetch_blocks(where, pieces, tconv, TCONV_BLOCK, sems)
    share = chans // SIDE
    for slot, ref in enumerate(pieces):
        holder = holder_of(core, slot)
        at = wrap(jnp.where(holder == 0, y, x) + OFFSETS[slot % SIDE])
        for m in range(2):
            source = ref.at[pl.ds(SIDE * TCONV_BLOCK + m * share, share)]
            target = dense.at[2 * holder + m, pl.ds(pl.multiple_of(at * share, 16), share)]
            pltpu.make_async_copy(source, target, dense_sem).start()
    rows = frames * places
    values = moved[...].astype(jnp.float32).reshape(rows, chans)
    first = (layer_norm(values) * first_gain[...][None, :]).astype(jnp.bfloat16)
    zero = jnp.zeros((places, chans), jnp.bfloat16)
    before = jnp.concatenate([zero, first[:-places]], axis=0)
    after = jnp.concatenate([first[places:], zero], axis=0)
    for px in range(SIDE):
        await_line(tconv, sems, px)
    mid[...] = values + jnp.dot(
        before, tconv[:chans, :], preferred_element_type=jnp.float32
    )
    mid[...] += jnp.dot(first, tconv[chans : 2 * chans, :], preferred_element_type=jnp.float32)
    mid[...] += jnp.dot(after, tconv[2 * chans :, :], preferred_element_type=jnp.float32)
    second = (layer_norm(mid[...]) * second_gain[...][None, :]).astype(jnp.bfloat16)
    pltpu.make_async_copy(dense, dense, dense_sem).wait()
    for m in range(3):
        part = jnp.dot(second, dense[m], preferred_element_type=jnp.float32)
        qkv[m] = part.astype(jnp.bfloat16).reshape(frames, places, chans)
    some = 16
    many = frames * some
    row_place = lax.broadcasted_iota(jnp.int32, (many, many), 0) % some
    col_place = lax.broadcasted_iota(jnp.int32, (many, many), 1) % some
    same = row_place == col_place
    lane = lax.broadcasted_iota(jnp.int32, (1, 2 * HEAD), 1)
    for group in range(places // some):
        spot = slice(group * some, (group + 1) * some)
        for pair in range(chans // (2 * HEAD)):
            lanes = slice(pair * 2 * HEAD, (pair + 1) * 2 * HEAD)
            query = qkv[0, :, spot, lanes].reshape(many, 2 * HEAD)
            key = qkv[1, :, spot, lanes].reshape(many, 2 * HEAD)
            value = qkv[2, :, spot, lanes].reshape(many, 2 * HEAD)
            both = []
            for side in range(2):
                own = (lane < HEAD) if side == 0 else (lane >= HEAD)
                only = jnp.where(own, query, jnp.zeros_like(query))
                scores = lax.dot_general(
                    only, key, (((1,), (1,)), ((), ())), preferred_element_type=jnp.float32
                )
                scores = jnp.where(same, scores * HEAD ** (-0.5), -1e30)
                top = jnp.max(scores, axis=-1, keepdims=True)
                raised = jnp.exp(scores - top)
                weights = raised / jnp.sum(raised, axis=-1, keepdims=True)
                both.append(
                    jnp.dot(weights.astype(jnp.bfloat16), value, preferred_element_type=jnp.float32)
                )
            mixed = jnp.where(lane < HEAD, both[0], both[1]).astype(jnp.bfloat16)
            attended[:, spot, lanes] = mixed.reshape(frames, some, 2 * HEAD)
    projected = jnp.dot(
        attended[...].reshape(rows, chans), dense[3], preferred_element_type=jnp.float32
    )
    out[...] = (mid[...] + projected).astype(jnp.bfloat16).reshape(frames, places, chans)


def specs(count):
    return [pl.BlockSpec(memory_space=pl.ANY)] * count


def shards(
    latents,
    norm_gain,
    norm_bias,
    conv_weight,
    time_weight,
    first_gain,
    tconv_weight,
    second_gain,
    qkv_weight,
    out_weight,
    timesteps,
):
    devices = lax.axis_size(SEQ)
    device = lax.axis_index(SEQ)
    x, y, core = (lax.axis_index(name) for name in SEQ)
    clips = timesteps.shape[0]
    images = clips * FRAMES
    rows, width, chans = latents.shape
    image = device % images
    clip = image // FRAMES
    lower = device // images
    bf16, f32 = jnp.bfloat16, jnp.float32

    where = jnp.stack([x, y, core, lower]).astype(jnp.int32)
    smem = pl.BlockSpec(memory_space=pltpu.SMEM)
    vmem = pl.BlockSpec(memory_space=pltpu.VMEM)
    params = pltpu.CompilerParams(vmem_limit_bytes=VMEM_LIMIT)

    conv_rows, tconv_rows = conv_weight.shape[0], tconv_weight.shape[0]
    few = qkv_weight.shape[0]

    def to_previous(px, py, pcore):
        spot = 2 * py + pcore - 1
        return None if spot < 0 else (px, spot // 2, spot % 2)

    some_rows = jax.ShapeDtypeStruct((2 * few, chans), bf16)
    both, query_key, crossed, value_out, edge = pl.pallas_call(
        pack_kernel,
        out_shape=[
            jax.ShapeDtypeStruct((conv_rows + tconv_rows, chans), bf16),
            some_rows,
            some_rows,
            some_rows,
            jax.ShapeDtypeStruct((width + SUM_ROWS, chans), bf16),
        ],
        in_specs=[smem] + [vmem] * 5,
        out_specs=[vmem] * 5,
        scratch_shapes=[pltpu.VMEM((64, chans), f32), pltpu.VMEM((24, chans), f32)],
        name="pack",
    )(where, latents, conv_weight, tconv_weight, qkv_weight, out_weight)
    following = send(both, to_previous)
    same_core = send(query_key, lambda px, py, pcore: (py, px, 0) if pcore == 0 else None)
    crossed = send(crossed, lambda px, py, pcore: (px, py, 1) if pcore == 0 else (py, px, 0))

    temb = time_embed(lax.dynamic_index_in_dim(timesteps, clip, 0, False), time_weight)
    own_rows = CONV_BLOCK + TCONV_BLOCK + 4 * few
    copies = pl.pallas_call(
        cut_kernel,
        out_shape=jax.ShapeDtypeStruct((SIDE, own_rows, chans), bf16),
        in_specs=[smem] + [vmem] * 5,
        out_specs=vmem,
        scratch_shapes=[
            pltpu.VMEM((own_rows, chans), bf16),
            pltpu.VMEM((112, chans), f32),
            pltpu.VMEM((32, chans), f32),
            pltpu.VMEM((24, chans), f32),
        ],
        name="cut",
    )(where, both, following, same_core, crossed, value_out)

    line = lax.all_to_all(
        copies,
        SEQ,
        split_axis=0,
        concat_axis=0,
        axis_index_groups=lines(),
        tiled=True,
    )
    conv_line, rest_line = pl.pallas_call(
        line_kernel,
        out_shape=[
            jax.ShapeDtypeStruct((SIDE * CONV_BLOCK, chans), bf16),
            jax.ShapeDtypeStruct((SIDE * (TCONV_BLOCK + 4 * few), chans), bf16),
        ],
        in_specs=[vmem],
        out_specs=[vmem] * 2,
        scratch_shapes=[pltpu.VMEM((SIDE * 4 * few, chans), f32)],
        name="line",
    )(line)
    pairs = [(i, (i + images) % devices) for i in range(devices)]
    conv_line, edge = lax.optimization_barrier((conv_line, edge))
    halo = lax.ppermute(edge, SEQ, pairs)
    conv_pieces, rest_pieces, (halo, temb) = two_rings(conv_line, rest_line, (halo, temb))

    spatial = pl.pallas_call(
        conv_kernel,
        out_shape=jax.ShapeDtypeStruct((rows * width, chans), bf16),
        in_specs=[smem] + [vmem] * 6 + specs(2 * SIDE),
        out_specs=vmem,
        scratch_shapes=[
            pltpu.VMEM((9 * chans, chans), bf16),
            pltpu.VMEM((3, rows + 2, width, chans), bf16),
            pltpu.VMEM((rows * width, chans), f32),
            pltpu.SemaphoreType.DMA((SIDE,)),
        ],
        compiler_params=params,
        name="conv",
    )(where, latents, edge, halo, norm_gain, norm_bias, temb, *conv_pieces)
    spatial, rest_pieces = lax.optimization_barrier((spatial, rest_pieces))
    half = SIDE // 2
    halves = [send(jnp.stack(rest_pieces[at : at + half]), swap) for at in (0, half)]
    moved = lax.all_to_all(spatial, SEQ[1:], split_axis=0, concat_axis=0, tiled=True)
    places = rows * width // FRAMES
    result = pl.pallas_call(
        temporal_kernel,
        out_shape=jax.ShapeDtypeStruct((FRAMES, places, chans), bf16),
        in_specs=[smem, vmem, vmem, vmem] + specs(SIDE + 2),
        out_specs=vmem,
        scratch_shapes=[
            pltpu.VMEM((3 * chans, chans), bf16),
            pltpu.VMEM((4, chans, chans), bf16),
            pltpu.VMEM((FRAMES * places, chans), f32),
            pltpu.VMEM((3, FRAMES, places, chans), bf16),
            pltpu.VMEM((FRAMES, places, chans), bf16),
            pltpu.SemaphoreType.DMA((SIDE,)),
            pltpu.SemaphoreType.DMA,
        ],
        compiler_params=params,
        name="temporal",
    )(
        where,
        moved.reshape(FRAMES, places, chans),
        first_gain,
        second_gain,
        *rest_pieces,
        *halves,
    )
    returned = lax.all_to_all(
        result.reshape(rows * width, chans), SEQ[1:], split_axis=0, concat_axis=0, tiled=True
    )
    return returned.reshape(rows, width, chans)


def solution(mesh):
    torus = Mesh(
        mesh.devices.reshape(mesh.shape["groups"], SIDE, SIDE, 2),
        ("groups", "seq_0", "seq_1", "seq_2"),
    )
    return jax.shard_map(
        shards,
        mesh=torus,
        in_specs=(
            P(GROUPS_SEQ, None, None),
            P(),
            P(),
            P(SEQ, None),
            P(),
            P(),
            P(SEQ, None),
            P(),
            P(SEQ, None),
            P(SEQ, None),
            P("groups"),
        ),
        out_specs=P(GROUPS_SEQ, None, None),
        check_vma=False,
    )
```

```python
import jax
import jax.numpy as jnp
from jax import lax
from jax.experimental import pallas as pl
from jax.experimental.pallas import tpu as pltpu
from jax.sharding import Mesh
from jax.sharding import PartitionSpec as P

HEAD = 64
GROUPS = 32
TFEAT = 320
FRAMES = 16
SEQ = ("seq_0", "seq_1", "seq_2")
GROUPS_SEQ = ("groups", "seq_0", "seq_1", "seq_2")
SIDE = 8
CONV_BLOCK = 48
TCONV_BLOCK = 16
SUM_ROWS = 16
VMEM_LIMIT = 56 * 2**20
OFFSETS = (0, -1, -2, -3, -4, 1, 2, 3)


def route(target):
    pairs = []
    for x in range(SIDE):
        for y in range(SIDE):
            for core in range(2):
                there = target(x, y, core)
                if there is not None:
                    tx, ty, tcore = there
                    to = (tx % SIDE * SIDE + ty % SIDE) * 2 + tcore
                    pairs.append(((x * SIDE + y) * 2 + core, to))
    return pairs


def send(block, target):
    return lax.ppermute(block, SEQ, route(target))


def inner(step):
    return lambda x, y, core: (x + step, y, core) if core == 0 else (x, y + step, core)


def outer(step):
    return lambda x, y, core: (x, y + step, core) if core == 0 else (x + step, y, core)


def swap(x, y, core):
    return x, y, 1 - core


def lines():
    device = lambda x, y, core: (x * SIDE + y) * 2 + core
    even = [[device(x, y, 0) for x in range(SIDE)] for y in range(SIDE)]
    return even + [[device(x, y, 1) for y in range(SIDE)] for x in range(SIDE)]


def two_rings(first, second, early):
    chains = {}
    for sign in (1, -1):
        chains[sign] = ([first], [second])
    for step in range(SIDE // 2):
        for sign, steps in ((1, SIDE // 2), (-1, SIDE // 2 - 1)):
            if step >= steps:
                continue
            one, two = chains[sign]
            if step == SIDE // 2 - 1 and sign == 1:
                one[-1], early = lax.optimization_barrier((one[-1], early))
            if step > 1:
                one[-1], two[-2] = lax.optimization_barrier((one[-1], two[-2]))
            if step > 0:
                two[-1], one[-1] = lax.optimization_barrier((two[-1], one[-1]))
            one.append(send(one[-1], outer(sign)))
            two.append(send(two[-1], outer(sign)))
    own = [chains[1][i] + chains[-1][i][1:] for i in range(2)]
    return own[0] + [send(piece, swap) for piece in own[0]], own[1], early


def time_embed(timestep, time_weight):
    half = TFEAT // 2
    freqs = jnp.exp(-jnp.log(10000.0) * jnp.arange(half, dtype=jnp.float32) / half)
    angles = timestep.astype(jnp.float32)[None, None] * freqs[None, :]
    feats = jnp.concatenate([jnp.cos(angles), jnp.sin(angles)], axis=-1)
    return jnp.dot(feats, time_weight.astype(jnp.float32), precision=lax.Precision.HIGHEST)


def wrap(value):
    return lax.rem(value + 2 * SIDE, SIDE)


def holder_of(core, slot):
    return core if slot < SIDE else 1 - core


def fetch_blocks(where, pieces, weight, size, sems):
    x, y, core = where[0], where[1], where[2]
    for slot, ref in enumerate(pieces):
        holder = holder_of(core, slot)
        across = OFFSETS[slot % SIDE]

        def one(b, carry, ref=ref, holder=holder, across=across):
            px = jnp.where(holder == 0, b, wrap(x + across))
            py = jnp.where(holder == 0, wrap(y + across), b)
            inside = 2 * py + holder

            @pl.when(inside < 2 * SIDE - 1)
            def _():
                at = pl.multiple_of((px * (2 * SIDE - 1) + inside) * size, size)
                source = ref.at[pl.ds(pl.multiple_of(b * size, size), size)]
                target = weight.at[pl.ds(at, size)]
                pltpu.make_async_copy(source, target, sems.at[px]).start()

            return carry

        lax.fori_loop(0, SIDE, one, 0)


def await_line(weight, sems, px):
    size = weight.shape[0] // SIDE
    part = weight.at[pl.ds(px * size, size)]
    pltpu.make_async_copy(part, part, sems.at[px]).wait()


def pack_kernel(where, latents, conv, tconv, qkv, last, *refs):
    both, query_key, crossed, value_out, edge, rows, few = refs
    conv_rows, chans = conv.shape
    count = qkv.shape[0]
    f32, bf16 = jnp.float32, jnp.bfloat16
    rows[pl.ds(0, conv_rows), :] = conv[...].astype(f32)
    rows[pl.ds(conv_rows, tconv.shape[0]), :] = tconv[...].astype(f32)
    both[...] = rows[pl.ds(0, both.shape[0]), :].astype(bf16)
    for m in range(3):
        few[pl.ds(m * count, count), :] = qkv[:, m * chans : (m + 1) * chans].astype(f32)
    few[pl.ds(3 * count, count), :] = last[...].astype(f32)
    head = few[pl.ds(0, 2 * count), :].astype(bf16)
    tail = few[pl.ds(2 * count, 2 * count), :].astype(bf16)
    query_key[...] = head
    value_out[...] = tail
    crossed[...] = jnp.where(where[2] == 0, tail.astype(f32), head.astype(f32)).astype(bf16)
    width = latents.shape[1]
    edge[pl.ds(0, width), :] = latents[jnp.where(where[3] == 1, 0, latents.shape[0] - 1)]
    values = latents[0].astype(f32)
    first, second = values, values * values
    for r in range(1, latents.shape[0]):
        values = latents[r].astype(f32)
        first, second = first + values, second + values * values
    left = jnp.concatenate([jnp.sum(v, axis=0, keepdims=True) for v in (first, second)], axis=0)
    few[...] = jnp.zeros(few.shape, f32)
    for part in range(3):
        high = left.astype(bf16).astype(f32)
        few[pl.ds(2 * part, 2), :] = high
        left = left - high
    edge[pl.ds(width, SUM_ROWS), :] = few[pl.ds(0, SUM_ROWS), :].astype(bf16)


def cut_kernel(where, both, following, same_core, crossed, value_out, copies, *scratch):
    block, conv, tconv, few = scratch
    f32, bf16 = jnp.float32, jnp.bfloat16
    count = same_core.shape[0] // 2
    tconv_rows = TCONV_BLOCK - 1
    conv_rows = both.shape[0] - tconv_rows
    inside = 2 * where[1] + where[2]
    own, next_rows = both[...].astype(f32), following[...].astype(f32)
    conv[pl.ds(0, both.shape[0]), :] = own
    tconv[pl.ds(0, tconv_rows), :] = conv[pl.ds(conv_rows, tconv_rows), :]
    conv[pl.ds(conv_rows, both.shape[0]), :] = next_rows
    tconv[pl.ds(tconv_rows, tconv_rows), :] = conv[pl.ds(2 * conv_rows, tconv_rows), :]
    conv_at = jnp.minimum((CONV_BLOCK - conv_rows) * inside, 2 * conv_rows - CONV_BLOCK)
    tconv_at = jnp.minimum(inside, 2 * tconv_rows - TCONV_BLOCK)
    turned = pltpu.roll(conv[...], lax.rem(conv.shape[0] - conv_at, conv.shape[0]), 0)
    block[pl.ds(0, CONV_BLOCK), :] = turned[:CONV_BLOCK].astype(bf16)
    turned = pltpu.roll(tconv[...], lax.rem(tconv.shape[0] - tconv_at, tconv.shape[0]), 0)
    block[pl.ds(CONV_BLOCK, TCONV_BLOCK), :] = turned[:TCONV_BLOCK].astype(bf16)
    near, far, kept = same_core[...].astype(f32), crossed[...].astype(f32), value_out[...].astype(f32)
    even = jnp.where(where[2] == 0, near, far)
    odd = jnp.where(where[2] == 0, far, kept)
    conv[pl.ds(0, 2 * count), :] = even
    conv[pl.ds(2 * count, 2 * count), :] = odd
    for m in range(2):
        for parity in range(2):
            source = conv[pl.ds((2 * parity + m) * count, count), :]
            few[pl.ds((2 * m + parity) * count, count), :] = source
    dense = few[pl.ds(0, 4 * count), :].astype(bf16)
    block[pl.ds(CONV_BLOCK + TCONV_BLOCK, 4 * count), :] = dense
    for b in range(SIDE):
        copies[b] = block[...]


def line_kernel(blocks, conv, rest, dense):
    start = CONV_BLOCK + TCONV_BLOCK
    share = blocks.shape[1] - start
    half = share // 2
    for b in range(SIDE):
        conv[pl.ds(b * CONV_BLOCK, CONV_BLOCK), :] = blocks[b, pl.ds(0, CONV_BLOCK), :]
        taken = blocks[b, pl.ds(CONV_BLOCK, TCONV_BLOCK), :]
        rest[pl.ds(b * TCONV_BLOCK, TCONV_BLOCK), :] = taken
        rows = blocks[b, pl.ds(start, share), :].astype(jnp.float32)
        for m in range(2):
            target = pl.ds((m * SIDE + b) * half, half)
            dense[target, :] = rows[m * half : (m + 1) * half]
    rest[pl.ds(SIDE * TCONV_BLOCK, share * SIDE), :] = dense[...].astype(jnp.bfloat16)


def conv_kernel(where, latents, edge, halo, gain, offset, temb, *refs):
    pieces, (out, weight, shifted, total, sems) = refs[: 2 * SIDE], refs[2 * SIDE :]
    fetch_blocks(where, pieces, weight, CONV_BLOCK, sems)
    rows, width, chans = latents.shape
    size = chans // GROUPS
    group = lax.broadcasted_iota(jnp.int32, (chans, chans), 0) // size
    same = group == lax.broadcasted_iota(jnp.int32, (chans, chans), 1) // size
    parts = edge[pl.ds(width, SUM_ROWS), :].astype(jnp.float32)
    parts = parts + halo[pl.ds(width, SUM_ROWS), :].astype(jnp.float32)
    sums = parts[0:2] + parts[2:4] + parts[4:6]
    frame = jnp.dot(
        jnp.concatenate([sums] * 4, axis=0),
        same.astype(jnp.float32),
        precision=lax.Precision.HIGHEST,
        preferred_element_type=jnp.float32,
    )
    entries = 2 * rows * width * size
    mean = frame[0:1] / entries
    var = frame[1:2] / entries - mean * mean
    scale = lax.rsqrt(var + 1e-05) * gain[...][None, :]
    bias = offset[...][None, :]
    column = lax.broadcasted_iota(jnp.int32, (width, 1), 0)
    lower = where[3]

    def fill(at, raw):
        values = (raw.astype(jnp.float32) - mean) * scale + bias
        values = values / (1.0 + jnp.exp(-values))
        left = jnp.where(column == 0, 0.0, pltpu.roll(values, 1, 0))
        right = jnp.where(column == width - 1, 0.0, pltpu.roll(values, width - 1, 0))
        shifted[0, at] = left.astype(jnp.bfloat16)
        shifted[1, at] = values.astype(jnp.bfloat16)
        shifted[2, at] = right.astype(jnp.bfloat16)

    def one_row(r, carry):
        fill(r + 1, latents[r])
        return carry

    lax.fori_loop(0, rows, one_row, 0)
    fill(jnp.where(lower == 1, 0, rows + 1), halo[pl.ds(0, width), :])
    empty = jnp.where(lower == 1, rows + 1, 0)
    for dx in range(3):
        shifted[dx, empty] = jnp.zeros((width, chans), jnp.bfloat16)
    for px in range(SIDE):
        await_line(weight, sems, px)
    base = latents[...].astype(jnp.float32).reshape(rows * width, chans)
    total[...] = base + temb[...]

    def one_row_of_taps(dy, carry):
        for dx in range(3):
            taken = shifted[dx, pl.ds(dy, rows)].reshape(rows * width, chans)
            at = pl.multiple_of((3 * dy + dx) * chans, 128)
            total[...] += jnp.dot(
                taken, weight[pl.ds(at, chans), :], preferred_element_type=jnp.float32
            )
        return carry

    lax.fori_loop(0, 3, one_row_of_taps, 0)
    out[...] = total[...].astype(jnp.bfloat16)


def layer_norm(values):
    mean = jnp.mean(values, axis=-1, keepdims=True)
    centered = values - mean
    var = jnp.mean(centered * centered, axis=-1, keepdims=True)
    return centered * lax.rsqrt(var + 1e-05)


def temporal_kernel(where, moved, first_gain, second_gain, *refs):
    halves = refs[SIDE : SIDE + 2]
    pieces = [*refs[:SIDE]] + [halves[i // 4].at[i % 4] for i in range(SIDE)]
    out, tconv, dense, mid, qkv, attended, sems, dense_sem = refs[SIDE + 2 :]
    x, y, core = where[0], where[1], where[2]
    frames, places, chans = moved.shape
    fetch_blocks(where, pieces, tconv, TCONV_BLOCK, sems)
    share = chans // SIDE
    for slot, ref in enumerate(pieces):
        holder = holder_of(core, slot)
        at = wrap(jnp.where(holder == 0, y, x) + OFFSETS[slot % SIDE])
        for m in range(2):
            source = ref.at[pl.ds(SIDE * TCONV_BLOCK + m * share, share)]
            target = dense.at[2 * holder + m, pl.ds(pl.multiple_of(at * share, 16), share)]
            pltpu.make_async_copy(source, target, dense_sem).start()
    rows = frames * places
    values = moved[...].astype(jnp.float32).reshape(rows, chans)
    first = (layer_norm(values) * first_gain[...][None, :]).astype(jnp.bfloat16)
    zero = jnp.zeros((places, chans), jnp.bfloat16)
    before = jnp.concatenate([zero, first[:-places]], axis=0)
    after = jnp.concatenate([first[places:], zero], axis=0)
    for px in range(SIDE):
        await_line(tconv, sems, px)
    stacked = jnp.concatenate([before, first, after], axis=1)
    mid[...] = values + jnp.dot(stacked, tconv[...], preferred_element_type=jnp.float32)
    second = (layer_norm(mid[...]) * second_gain[...][None, :]).astype(jnp.bfloat16)
    pltpu.make_async_copy(dense, dense, dense_sem).wait()
    for m in range(3):
        part = jnp.dot(second, dense[m], preferred_element_type=jnp.float32)
        qkv[m] = part.astype(jnp.bfloat16).reshape(frames, places, chans)
    some = 16
    many = frames * some
    row_place = lax.broadcasted_iota(jnp.int32, (many, many), 0) % some
    col_place = lax.broadcasted_iota(jnp.int32, (many, many), 1) % some
    same = row_place == col_place
    lane = lax.broadcasted_iota(jnp.int32, (1, 2 * HEAD), 1)
    for group in range(places // some):
        spot = slice(group * some, (group + 1) * some)
        for pair in range(chans // (2 * HEAD)):
            lanes = slice(pair * 2 * HEAD, (pair + 1) * 2 * HEAD)
            query = qkv[0, :, spot, lanes].reshape(many, 2 * HEAD)
            key = qkv[1, :, spot, lanes].reshape(many, 2 * HEAD)
            value = qkv[2, :, spot, lanes].reshape(many, 2 * HEAD)
            both = []
            for side in range(2):
                own = (lane < HEAD) if side == 0 else (lane >= HEAD)
                only = jnp.where(own, query, jnp.zeros_like(query))
                scores = lax.dot_general(
                    only, key, (((1,), (1,)), ((), ())), preferred_element_type=jnp.float32
                )
                scores = jnp.where(same, scores * HEAD ** (-0.5), -1e30)
                top = jnp.max(scores, axis=-1, keepdims=True)
                raised = jnp.exp(scores - top)
                weights = raised / jnp.sum(raised, axis=-1, keepdims=True)
                both.append(
                    jnp.dot(weights.astype(jnp.bfloat16), value, preferred_element_type=jnp.float32)
                )
            mixed = jnp.where(lane < HEAD, both[0], both[1]).astype(jnp.bfloat16)
            attended[:, spot, lanes] = mixed.reshape(frames, some, 2 * HEAD)
    projected = jnp.dot(
        attended[...].reshape(rows, chans), dense[3], preferred_element_type=jnp.float32
    )
    out[...] = (mid[...] + projected).astype(jnp.bfloat16).reshape(frames, places, chans)


def specs(count):
    return [pl.BlockSpec(memory_space=pl.ANY)] * count


def shards(
    latents,
    norm_gain,
    norm_bias,
    conv_weight,
    time_weight,
    first_gain,
    tconv_weight,
    second_gain,
    qkv_weight,
    out_weight,
    timesteps,
):
    devices = lax.axis_size(SEQ)
    device = lax.axis_index(SEQ)
    x, y, core = (lax.axis_index(name) for name in SEQ)
    clips = timesteps.shape[0]
    images = clips * FRAMES
    rows, width, chans = latents.shape
    image = device % images
    clip = image // FRAMES
    lower = device // images
    bf16, f32 = jnp.bfloat16, jnp.float32

    where = jnp.stack([x, y, core, lower]).astype(jnp.int32)
    smem = pl.BlockSpec(memory_space=pltpu.SMEM)
    vmem = pl.BlockSpec(memory_space=pltpu.VMEM)
    params = pltpu.CompilerParams(vmem_limit_bytes=VMEM_LIMIT)

    conv_rows, tconv_rows = conv_weight.shape[0], tconv_weight.shape[0]
    few = qkv_weight.shape[0]

    def to_previous(px, py, pcore):
        spot = 2 * py + pcore - 1
        return None if spot < 0 else (px, spot // 2, spot % 2)

    some_rows = jax.ShapeDtypeStruct((2 * few, chans), bf16)
    both, query_key, crossed, value_out, edge = pl.pallas_call(
        pack_kernel,
        out_shape=[
            jax.ShapeDtypeStruct((conv_rows + tconv_rows, chans), bf16),
            some_rows,
            some_rows,
            some_rows,
            jax.ShapeDtypeStruct((width + SUM_ROWS, chans), bf16),
        ],
        in_specs=[smem] + [vmem] * 5,
        out_specs=[vmem] * 5,
        scratch_shapes=[pltpu.VMEM((64, chans), f32), pltpu.VMEM((24, chans), f32)],
        name="pack",
    )(where, latents, conv_weight, tconv_weight, qkv_weight, out_weight)
    following = send(both, to_previous)
    same_core = send(query_key, lambda px, py, pcore: (py, px, 0) if pcore == 0 else None)
    crossed = send(crossed, lambda px, py, pcore: (px, py, 1) if pcore == 0 else (py, px, 0))

    temb = time_embed(lax.dynamic_index_in_dim(timesteps, clip, 0, False), time_weight)
    own_rows = CONV_BLOCK + TCONV_BLOCK + 4 * few
    copies = pl.pallas_call(
        cut_kernel,
        out_shape=jax.ShapeDtypeStruct((SIDE, own_rows, chans), bf16),
        in_specs=[smem] + [vmem] * 5,
        out_specs=vmem,
        scratch_shapes=[
            pltpu.VMEM((own_rows, chans), bf16),
            pltpu.VMEM((112, chans), f32),
            pltpu.VMEM((32, chans), f32),
            pltpu.VMEM((24, chans), f32),
        ],
        name="cut",
    )(where, both, following, same_core, crossed, value_out)

    line = lax.all_to_all(
        copies,
        SEQ,
        split_axis=0,
        concat_axis=0,
        axis_index_groups=lines(),
        tiled=True,
    )
    conv_line, rest_line = pl.pallas_call(
        line_kernel,
        out_shape=[
            jax.ShapeDtypeStruct((SIDE * CONV_BLOCK, chans), bf16),
            jax.ShapeDtypeStruct((SIDE * (TCONV_BLOCK + 4 * few), chans), bf16),
        ],
        in_specs=[vmem],
        out_specs=[vmem] * 2,
        scratch_shapes=[pltpu.VMEM((SIDE * 4 * few, chans), f32)],
        name="line",
    )(line)
    pairs = [(i, (i + images) % devices) for i in range(devices)]
    conv_line, edge = lax.optimization_barrier((conv_line, edge))
    halo = lax.ppermute(edge, SEQ, pairs)
    conv_pieces, rest_pieces, (halo, temb) = two_rings(conv_line, rest_line, (halo, temb))

    spatial = pl.pallas_call(
        conv_kernel,
        out_shape=jax.ShapeDtypeStruct((rows * width, chans), bf16),
        in_specs=[smem] + [vmem] * 6 + specs(2 * SIDE),
        out_specs=vmem,
        scratch_shapes=[
            pltpu.VMEM((9 * chans, chans), bf16),
            pltpu.VMEM((3, rows + 2, width, chans), bf16),
            pltpu.VMEM((rows * width, chans), f32),
            pltpu.SemaphoreType.DMA((SIDE,)),
        ],
        compiler_params=params,
        name="conv",
    )(where, latents, edge, halo, norm_gain, norm_bias, temb, *conv_pieces)
    spatial, rest_pieces = lax.optimization_barrier((spatial, rest_pieces))
    half = SIDE // 2
    halves = [send(jnp.stack(rest_pieces[at : at + half]), swap) for at in (0, half)]
    moved = lax.all_to_all(spatial, SEQ[1:], split_axis=0, concat_axis=0, tiled=True)
    places = rows * width // FRAMES
    result = pl.pallas_call(
        temporal_kernel,
        out_shape=jax.ShapeDtypeStruct((FRAMES, places, chans), bf16),
        in_specs=[smem, vmem, vmem, vmem] + specs(SIDE + 2),
        out_specs=vmem,
        scratch_shapes=[
            pltpu.VMEM((3 * chans, chans), bf16),
            pltpu.VMEM((4, chans, chans), bf16),
            pltpu.VMEM((FRAMES * places, chans), f32),
            pltpu.VMEM((3, FRAMES, places, chans), bf16),
            pltpu.VMEM((FRAMES, places, chans), bf16),
            pltpu.SemaphoreType.DMA((SIDE,)),
            pltpu.SemaphoreType.DMA,
        ],
        compiler_params=params,
        name="temporal",
    )(
        where,
        moved.reshape(FRAMES, places, chans),
        first_gain,
        second_gain,
        *rest_pieces,
        *halves,
    )
    returned = lax.all_to_all(
        result.reshape(rows * width, chans), SEQ[1:], split_axis=0, concat_axis=0, tiled=True
    )
    return returned.reshape(rows, width, chans)


def solution(mesh):
    torus = Mesh(
        mesh.devices.reshape(mesh.shape["groups"], SIDE, SIDE, 2),
        ("groups", "seq_0", "seq_1", "seq_2"),
    )
    return jax.shard_map(
        shards,
        mesh=torus,
        in_specs=(
            P(GROUPS_SEQ, None, None),
            P(),
            P(),
            P(SEQ, None),
            P(),
            P(),
            P(SEQ, None),
            P(),
            P(SEQ, None),
            P(SEQ, None),
            P("groups"),
        ),
        out_specs=P(GROUPS_SEQ, None, None),
        check_vma=False,
    )
```

```python
import jax
import jax.numpy as jnp
from jax import lax
from jax.experimental import pallas as pl
from jax.experimental.pallas import tpu as pltpu
from jax.sharding import Mesh
from jax.sharding import PartitionSpec as P

HEAD = 64
GROUPS = 32
TFEAT = 320
FRAMES = 16
SEQ = ("seq_0", "seq_1", "seq_2")
GROUPS_SEQ = ("groups", "seq_0", "seq_1", "seq_2")
SIDE = 8
CONV_BLOCK = 48
TCONV_BLOCK = 16
SUM_ROWS = 16
VMEM_LIMIT = 56 * 2**20
OFFSETS = (0, -1, -2, -3, -4, 1, 2, 3)


def route(target):
    pairs = []
    for x in range(SIDE):
        for y in range(SIDE):
            for core in range(2):
                there = target(x, y, core)
                if there is not None:
                    tx, ty, tcore = there
                    to = (tx % SIDE * SIDE + ty % SIDE) * 2 + tcore
                    pairs.append(((x * SIDE + y) * 2 + core, to))
    return pairs


def send(block, target):
    return lax.ppermute(block, SEQ, route(target))


def inner(step):
    return lambda x, y, core: (x + step, y, core) if core == 0 else (x, y + step, core)


def outer(step):
    return lambda x, y, core: (x, y + step, core) if core == 0 else (x + step, y, core)


def swap(x, y, core):
    return x, y, 1 - core


def lines():
    device = lambda x, y, core: (x * SIDE + y) * 2 + core
    even = [[device(x, y, 0) for x in range(SIDE)] for y in range(SIDE)]
    return even + [[device(x, y, 1) for y in range(SIDE)] for x in range(SIDE)]


def two_rings(first, second, early):
    chains = {}
    for sign in (1, -1):
        chains[sign] = ([first], [second])
    for step in range(SIDE // 2):
        for sign, steps in ((1, SIDE // 2), (-1, SIDE // 2 - 1)):
            if step >= steps:
                continue
            one, two = chains[sign]
            if step == SIDE // 2 - 1 and sign == 1:
                one[-1], early = lax.optimization_barrier((one[-1], early))
            if step > 1:
                one[-1], two[-2] = lax.optimization_barrier((one[-1], two[-2]))
            if step > 0:
                two[-1], one[-1] = lax.optimization_barrier((two[-1], one[-1]))
            one.append(send(one[-1], outer(sign)))
            two.append(send(two[-1], outer(sign)))
    own = [chains[1][i] + chains[-1][i][1:] for i in range(2)]
    return own[0] + [send(piece, swap) for piece in own[0]], own[1], early


def time_embed(timestep, time_weight):
    half = TFEAT // 2
    freqs = jnp.exp(-jnp.log(10000.0) * jnp.arange(half, dtype=jnp.float32) / half)
    angles = timestep.astype(jnp.float32)[None, None] * freqs[None, :]
    feats = jnp.concatenate([jnp.cos(angles), jnp.sin(angles)], axis=-1)
    return jnp.dot(feats, time_weight.astype(jnp.float32), precision=lax.Precision.HIGHEST)


def wrap(value):
    return lax.rem(value + 2 * SIDE, SIDE)


def holder_of(core, slot):
    return core if slot < SIDE else 1 - core


def fetch_blocks(where, pieces, weight, size, sems):
    x, y, core = where[0], where[1], where[2]
    for slot, ref in enumerate(pieces):
        holder = holder_of(core, slot)
        across = OFFSETS[slot % SIDE]

        def one(b, carry, ref=ref, holder=holder, across=across):
            px = jnp.where(holder == 0, b, wrap(x + across))
            py = jnp.where(holder == 0, wrap(y + across), b)
            inside = 2 * py + holder

            @pl.when(inside < 2 * SIDE - 1)
            def _():
                at = pl.multiple_of((px * (2 * SIDE - 1) + inside) * size, size)
                source = ref.at[pl.ds(pl.multiple_of(b * size, size), size)]
                target = weight.at[pl.ds(at, size)]
                pltpu.make_async_copy(source, target, sems.at[px]).start()

            return carry

        lax.fori_loop(0, SIDE, one, 0)


def await_line(weight, sems, px):
    size = weight.shape[0] // SIDE
    part = weight.at[pl.ds(px * size, size)]
    pltpu.make_async_copy(part, part, sems.at[px]).wait()


def pack_kernel(where, conv, tconv, qkv, last, *refs):
    both, query_key, crossed, value_out, rows, few = refs
    conv_rows, chans = conv.shape
    count = qkv.shape[0]
    f32, bf16 = jnp.float32, jnp.bfloat16
    rows[pl.ds(0, conv_rows), :] = conv[...].astype(f32)
    rows[pl.ds(conv_rows, tconv.shape[0]), :] = tconv[...].astype(f32)
    both[...] = rows[pl.ds(0, both.shape[0]), :].astype(bf16)
    for m in range(3):
        few[pl.ds(m * count, count), :] = qkv[:, m * chans : (m + 1) * chans].astype(f32)
    few[pl.ds(3 * count, count), :] = last[...].astype(f32)
    head = few[pl.ds(0, 2 * count), :].astype(bf16)
    tail = few[pl.ds(2 * count, 2 * count), :].astype(bf16)
    query_key[...] = head
    value_out[...] = tail
    crossed[...] = jnp.where(where[2] == 0, tail.astype(f32), head.astype(f32)).astype(bf16)


def sums_kernel(where, latents, edge, few):
    f32, bf16 = jnp.float32, jnp.bfloat16
    width = latents.shape[1]
    edge[pl.ds(0, width), :] = latents[jnp.where(where[3] == 1, 0, latents.shape[0] - 1)]
    values = latents[0].astype(f32)
    first, second = values, values * values
    for r in range(1, latents.shape[0]):
        values = latents[r].astype(f32)
        first, second = first + values, second + values * values
    left = jnp.concatenate([jnp.sum(v, axis=0, keepdims=True) for v in (first, second)], axis=0)
    few[...] = jnp.zeros(few.shape, f32)
    for part in range(3):
        high = left.astype(bf16).astype(f32)
        few[pl.ds(2 * part, 2), :] = high
        left = left - high
    edge[pl.ds(width, SUM_ROWS), :] = few[pl.ds(0, SUM_ROWS), :].astype(bf16)


def cut_kernel(where, both, following, same_core, crossed, value_out, copies, *scratch):
    block, conv, tconv, few = scratch
    f32, bf16 = jnp.float32, jnp.bfloat16
    count = same_core.shape[0] // 2
    tconv_rows = TCONV_BLOCK - 1
    conv_rows = both.shape[0] - tconv_rows
    inside = 2 * where[1] + where[2]
    own, next_rows = both[...].astype(f32), following[...].astype(f32)
    conv[pl.ds(0, both.shape[0]), :] = own
    tconv[pl.ds(0, tconv_rows), :] = conv[pl.ds(conv_rows, tconv_rows), :]
    conv[pl.ds(conv_rows, both.shape[0]), :] = next_rows
    tconv[pl.ds(tconv_rows, tconv_rows), :] = conv[pl.ds(2 * conv_rows, tconv_rows), :]
    conv_at = jnp.minimum((CONV_BLOCK - conv_rows) * inside, 2 * conv_rows - CONV_BLOCK)
    tconv_at = jnp.minimum(inside, 2 * tconv_rows - TCONV_BLOCK)
    turned = pltpu.roll(conv[...], lax.rem(conv.shape[0] - conv_at, conv.shape[0]), 0)
    block[pl.ds(0, CONV_BLOCK), :] = turned[:CONV_BLOCK].astype(bf16)
    turned = pltpu.roll(tconv[...], lax.rem(tconv.shape[0] - tconv_at, tconv.shape[0]), 0)
    block[pl.ds(CONV_BLOCK, TCONV_BLOCK), :] = turned[:TCONV_BLOCK].astype(bf16)
    near, far, kept = same_core[...].astype(f32), crossed[...].astype(f32), value_out[...].astype(f32)
    even = jnp.where(where[2] == 0, near, far)
    odd = jnp.where(where[2] == 0, far, kept)
    conv[pl.ds(0, 2 * count), :] = even
    conv[pl.ds(2 * count, 2 * count), :] = odd
    for m in range(2):
        for parity in range(2):
            source = conv[pl.ds((2 * parity + m) * count, count), :]
            few[pl.ds((2 * m + parity) * count, count), :] = source
    dense = few[pl.ds(0, 4 * count), :].astype(bf16)
    block[pl.ds(CONV_BLOCK + TCONV_BLOCK, 4 * count), :] = dense
    for b in range(SIDE):
        copies[b] = block[...]


def line_kernel(blocks, conv, rest, dense):
    start = CONV_BLOCK + TCONV_BLOCK
    share = blocks.shape[1] - start
    half = share // 2
    for b in range(SIDE):
        conv[pl.ds(b * CONV_BLOCK, CONV_BLOCK), :] = blocks[b, pl.ds(0, CONV_BLOCK), :]
        taken = blocks[b, pl.ds(CONV_BLOCK, TCONV_BLOCK), :]
        rest[pl.ds(b * TCONV_BLOCK, TCONV_BLOCK), :] = taken
        rows = blocks[b, pl.ds(start, share), :].astype(jnp.float32)
        for m in range(2):
            target = pl.ds((m * SIDE + b) * half, half)
            dense[target, :] = rows[m * half : (m + 1) * half]
    rest[pl.ds(SIDE * TCONV_BLOCK, share * SIDE), :] = dense[...].astype(jnp.bfloat16)


def conv_kernel(where, latents, edge, halo, gain, offset, temb, *refs):
    pieces, (out, weight, shifted, total, sems) = refs[: 2 * SIDE], refs[2 * SIDE :]
    fetch_blocks(where, pieces, weight, CONV_BLOCK, sems)
    rows, width, chans = latents.shape
    size = chans // GROUPS
    group = lax.broadcasted_iota(jnp.int32, (chans, chans), 0) // size
    same = group == lax.broadcasted_iota(jnp.int32, (chans, chans), 1) // size
    parts = edge[pl.ds(width, SUM_ROWS), :].astype(jnp.float32)
    parts = parts + halo[pl.ds(width, SUM_ROWS), :].astype(jnp.float32)
    sums = parts[0:2] + parts[2:4] + parts[4:6]
    frame = jnp.dot(
        jnp.concatenate([sums] * 4, axis=0),
        same.astype(jnp.float32),
        precision=lax.Precision.HIGHEST,
        preferred_element_type=jnp.float32,
    )
    entries = 2 * rows * width * size
    mean = frame[0:1] / entries
    var = frame[1:2] / entries - mean * mean
    scale = lax.rsqrt(var + 1e-05) * gain[...][None, :]
    bias = offset[...][None, :]
    column = lax.broadcasted_iota(jnp.int32, (width, 1), 0)
    lower = where[3]

    def fill(at, raw):
        values = (raw.astype(jnp.float32) - mean) * scale + bias
        values = values / (1.0 + jnp.exp(-values))
        left = jnp.where(column == 0, 0.0, pltpu.roll(values, 1, 0))
        right = jnp.where(column == width - 1, 0.0, pltpu.roll(values, width - 1, 0))
        shifted[0, at] = left.astype(jnp.bfloat16)
        shifted[1, at] = values.astype(jnp.bfloat16)
        shifted[2, at] = right.astype(jnp.bfloat16)

    def one_row(r, carry):
        fill(r + 1, latents[r])
        return carry

    lax.fori_loop(0, rows, one_row, 0)
    fill(jnp.where(lower == 1, 0, rows + 1), halo[pl.ds(0, width), :])
    empty = jnp.where(lower == 1, rows + 1, 0)
    for dx in range(3):
        shifted[dx, empty] = jnp.zeros((width, chans), jnp.bfloat16)
    for px in range(SIDE):
        await_line(weight, sems, px)
    base = latents[...].astype(jnp.float32).reshape(rows * width, chans)
    total[...] = base + temb[...]

    def one_row_of_taps(dy, carry):
        for dx in range(3):
            taken = shifted[dx, pl.ds(dy, rows)].reshape(rows * width, chans)
            at = pl.multiple_of((3 * dy + dx) * chans, 128)
            total[...] += jnp.dot(
                taken, weight[pl.ds(at, chans), :], preferred_element_type=jnp.float32
            )
        return carry

    lax.fori_loop(0, 3, one_row_of_taps, 0)
    out[...] = total[...].astype(jnp.bfloat16)


def layer_norm(values):
    mean = jnp.mean(values, axis=-1, keepdims=True)
    centered = values - mean
    var = jnp.mean(centered * centered, axis=-1, keepdims=True)
    return centered * lax.rsqrt(var + 1e-05)


def temporal_kernel(where, moved, first_gain, second_gain, *refs):
    halves = refs[SIDE : SIDE + 2]
    pieces = [*refs[:SIDE]] + [halves[i // 4].at[i % 4] for i in range(SIDE)]
    out, tconv, dense, mid, qkv, attended, sems, dense_sem = refs[SIDE + 2 :]
    x, y, core = where[0], where[1], where[2]
    frames, places, chans = moved.shape
    fetch_blocks(where, pieces, tconv, TCONV_BLOCK, sems)
    share = chans // SIDE
    for slot, ref in enumerate(pieces):
        holder = holder_of(core, slot)
        at = wrap(jnp.where(holder == 0, y, x) + OFFSETS[slot % SIDE])
        for m in range(2):
            source = ref.at[pl.ds(SIDE * TCONV_BLOCK + m * share, share)]
            target = dense.at[2 * holder + m, pl.ds(pl.multiple_of(at * share, 16), share)]
            pltpu.make_async_copy(source, target, dense_sem).start()
    rows = frames * places
    values = moved[...].astype(jnp.float32).reshape(rows, chans)
    first = (layer_norm(values) * first_gain[...][None, :]).astype(jnp.bfloat16)
    zero = jnp.zeros((places, chans), jnp.bfloat16)
    before = jnp.concatenate([zero, first[:-places]], axis=0)
    after = jnp.concatenate([first[places:], zero], axis=0)
    for px in range(SIDE):
        await_line(tconv, sems, px)
    mid[...] = values + jnp.dot(
        before, tconv[:chans, :], preferred_element_type=jnp.float32
    )
    mid[...] += jnp.dot(first, tconv[chans : 2 * chans, :], preferred_element_type=jnp.float32)
    mid[...] += jnp.dot(after, tconv[2 * chans :, :], preferred_element_type=jnp.float32)
    second = (layer_norm(mid[...]) * second_gain[...][None, :]).astype(jnp.bfloat16)
    pltpu.make_async_copy(dense, dense, dense_sem).wait()
    for m in range(3):
        part = jnp.dot(second, dense[m], preferred_element_type=jnp.float32)
        qkv[m] = part.astype(jnp.bfloat16).reshape(frames, places, chans)
    some = 16
    many = frames * some
    row_place = lax.broadcasted_iota(jnp.int32, (many, many), 0) % some
    col_place = lax.broadcasted_iota(jnp.int32, (many, many), 1) % some
    same = row_place == col_place
    lane = lax.broadcasted_iota(jnp.int32, (1, 2 * HEAD), 1)
    for group in range(places // some):
        spot = slice(group * some, (group + 1) * some)
        for pair in range(chans // (2 * HEAD)):
            lanes = slice(pair * 2 * HEAD, (pair + 1) * 2 * HEAD)
            query = qkv[0, :, spot, lanes].reshape(many, 2 * HEAD)
            key = qkv[1, :, spot, lanes].reshape(many, 2 * HEAD)
            value = qkv[2, :, spot, lanes].reshape(many, 2 * HEAD)
            both = []
            for side in range(2):
                own = (lane < HEAD) if side == 0 else (lane >= HEAD)
                only = jnp.where(own, query, jnp.zeros_like(query))
                scores = lax.dot_general(
                    only, key, (((1,), (1,)), ((), ())), preferred_element_type=jnp.float32
                )
                scores = jnp.where(same, scores * HEAD ** (-0.5), -1e30)
                top = jnp.max(scores, axis=-1, keepdims=True)
                raised = jnp.exp(scores - top)
                weights = raised / jnp.sum(raised, axis=-1, keepdims=True)
                both.append(
                    jnp.dot(weights.astype(jnp.bfloat16), value, preferred_element_type=jnp.float32)
                )
            mixed = jnp.where(lane < HEAD, both[0], both[1]).astype(jnp.bfloat16)
            attended[:, spot, lanes] = mixed.reshape(frames, some, 2 * HEAD)
    projected = jnp.dot(
        attended[...].reshape(rows, chans), dense[3], preferred_element_type=jnp.float32
    )
    out[...] = (mid[...] + projected).astype(jnp.bfloat16).reshape(frames, places, chans)


def specs(count):
    return [pl.BlockSpec(memory_space=pl.ANY)] * count


def shards(
    latents,
    norm_gain,
    norm_bias,
    conv_weight,
    time_weight,
    first_gain,
    tconv_weight,
    second_gain,
    qkv_weight,
    out_weight,
    timesteps,
):
    devices = lax.axis_size(SEQ)
    device = lax.axis_index(SEQ)
    x, y, core = (lax.axis_index(name) for name in SEQ)
    clips = timesteps.shape[0]
    images = clips * FRAMES
    rows, width, chans = latents.shape
    image = device % images
    clip = image // FRAMES
    lower = device // images
    bf16, f32 = jnp.bfloat16, jnp.float32

    where = jnp.stack([x, y, core, lower]).astype(jnp.int32)
    smem = pl.BlockSpec(memory_space=pltpu.SMEM)
    vmem = pl.BlockSpec(memory_space=pltpu.VMEM)
    params = pltpu.CompilerParams(vmem_limit_bytes=VMEM_LIMIT)

    conv_rows, tconv_rows = conv_weight.shape[0], tconv_weight.shape[0]
    few = qkv_weight.shape[0]

    def to_previous(px, py, pcore):
        spot = 2 * py + pcore - 1
        return None if spot < 0 else (px, spot // 2, spot % 2)

    some_rows = jax.ShapeDtypeStruct((2 * few, chans), bf16)
    both, query_key, crossed, value_out = pl.pallas_call(
        pack_kernel,
        out_shape=[
            jax.ShapeDtypeStruct((conv_rows + tconv_rows, chans), bf16),
            some_rows,
            some_rows,
            some_rows,
        ],
        in_specs=[smem] + [vmem] * 4,
        out_specs=[vmem] * 4,
        scratch_shapes=[pltpu.VMEM((64, chans), f32), pltpu.VMEM((24, chans), f32)],
        name="pack",
    )(where, conv_weight, tconv_weight, qkv_weight, out_weight)
    following = send(both, to_previous)
    same_core = send(query_key, lambda px, py, pcore: (py, px, 0) if pcore == 0 else None)
    crossed = send(crossed, lambda px, py, pcore: (px, py, 1) if pcore == 0 else (py, px, 0))

    edge = pl.pallas_call(
        sums_kernel,
        out_shape=jax.ShapeDtypeStruct((width + SUM_ROWS, chans), bf16),
        in_specs=[smem, vmem],
        out_specs=vmem,
        scratch_shapes=[pltpu.VMEM((24, chans), f32)],
        name="sums",
    )(where, latents)
    halo = lax.ppermute(edge, SEQ, [(i, (i + images) % devices) for i in range(devices)])
    temb = time_embed(lax.dynamic_index_in_dim(timesteps, clip, 0, False), time_weight)
    own_rows = CONV_BLOCK + TCONV_BLOCK + 4 * few
    copies = pl.pallas_call(
        cut_kernel,
        out_shape=jax.ShapeDtypeStruct((SIDE, own_rows, chans), bf16),
        in_specs=[smem] + [vmem] * 5,
        out_specs=vmem,
        scratch_shapes=[
            pltpu.VMEM((own_rows, chans), bf16),
            pltpu.VMEM((112, chans), f32),
            pltpu.VMEM((32, chans), f32),
            pltpu.VMEM((24, chans), f32),
        ],
        name="cut",
    )(where, both, following, same_core, crossed, value_out)

    line = lax.all_to_all(
        copies,
        SEQ,
        split_axis=0,
        concat_axis=0,
        axis_index_groups=lines(),
        tiled=True,
    )
    conv_line, rest_line = pl.pallas_call(
        line_kernel,
        out_shape=[
            jax.ShapeDtypeStruct((SIDE * CONV_BLOCK, chans), bf16),
            jax.ShapeDtypeStruct((SIDE * (TCONV_BLOCK + 4 * few), chans), bf16),
        ],
        in_specs=[vmem],
        out_specs=[vmem] * 2,
        scratch_shapes=[pltpu.VMEM((SIDE * 4 * few, chans), f32)],
        name="line",
    )(line)
    conv_line, halo = lax.optimization_barrier((conv_line, halo))
    conv_pieces, rest_pieces, temb = two_rings(conv_line, rest_line, temb)

    spatial = pl.pallas_call(
        conv_kernel,
        out_shape=jax.ShapeDtypeStruct((rows * width, chans), bf16),
        in_specs=[smem] + [vmem] * 6 + specs(2 * SIDE),
        out_specs=vmem,
        scratch_shapes=[
            pltpu.VMEM((9 * chans, chans), bf16),
            pltpu.VMEM((3, rows + 2, width, chans), bf16),
            pltpu.VMEM((rows * width, chans), f32),
            pltpu.SemaphoreType.DMA((SIDE,)),
        ],
        compiler_params=params,
        name="conv",
    )(where, latents, edge, halo, norm_gain, norm_bias, temb, *conv_pieces)
    spatial, rest_pieces = lax.optimization_barrier((spatial, rest_pieces))
    half = SIDE // 2
    halves = [send(jnp.stack(rest_pieces[at : at + half]), swap) for at in (0, half)]
    moved = lax.all_to_all(spatial, SEQ[1:], split_axis=0, concat_axis=0, tiled=True)
    places = rows * width // FRAMES
    result = pl.pallas_call(
        temporal_kernel,
        out_shape=jax.ShapeDtypeStruct((FRAMES, places, chans), bf16),
        in_specs=[smem, vmem, vmem, vmem] + specs(SIDE + 2),
        out_specs=vmem,
        scratch_shapes=[
            pltpu.VMEM((3 * chans, chans), bf16),
            pltpu.VMEM((4, chans, chans), bf16),
            pltpu.VMEM((FRAMES * places, chans), f32),
            pltpu.VMEM((3, FRAMES, places, chans), bf16),
            pltpu.VMEM((FRAMES, places, chans), bf16),
            pltpu.SemaphoreType.DMA((SIDE,)),
            pltpu.SemaphoreType.DMA,
        ],
        compiler_params=params,
        name="temporal",
    )(
        where,
        moved.reshape(FRAMES, places, chans),
        first_gain,
        second_gain,
        *rest_pieces,
        *halves,
    )
    returned = lax.all_to_all(
        result.reshape(rows * width, chans), SEQ[1:], split_axis=0, concat_axis=0, tiled=True
    )
    return returned.reshape(rows, width, chans)


def solution(mesh):
    torus = Mesh(
        mesh.devices.reshape(mesh.shape["groups"], SIDE, SIDE, 2),
        ("groups", "seq_0", "seq_1", "seq_2"),
    )
    return jax.shard_map(
        shards,
        mesh=torus,
        in_specs=(
            P(GROUPS_SEQ, None, None),
            P(),
            P(),
            P(SEQ, None),
            P(),
            P(),
            P(SEQ, None),
            P(),
            P(SEQ, None),
            P(SEQ, None),
            P("groups"),
        ),
        out_specs=P(GROUPS_SEQ, None, None),
        check_vma=False,
    )
```

```python
import jax
import jax.numpy as jnp
from jax import lax
from jax.experimental import pallas as pl
from jax.experimental.pallas import tpu as pltpu
from jax.sharding import Mesh
from jax.sharding import PartitionSpec as P

HEAD = 64
GROUPS = 32
TFEAT = 320
FRAMES = 16
SEQ = ("seq_0", "seq_1", "seq_2")
GROUPS_SEQ = ("groups", "seq_0", "seq_1", "seq_2")
SIDE = 8
CONV_BLOCK = 48
TCONV_BLOCK = 16
SUM_ROWS = 16
VMEM_LIMIT = 56 * 2**20
OFFSETS = (0, -1, -2, -3, -4, 1, 2, 3)
HALVES = ((0, 1, 2, 5), (3, 4, 6, 7))


def route(target):
    pairs = []
    for x in range(SIDE):
        for y in range(SIDE):
            for core in range(2):
                there = target(x, y, core)
                if there is not None:
                    tx, ty, tcore = there
                    to = (tx % SIDE * SIDE + ty % SIDE) * 2 + tcore
                    pairs.append(((x * SIDE + y) * 2 + core, to))
    return pairs


def send(block, target):
    return lax.ppermute(block, SEQ, route(target))


def inner(step):
    return lambda x, y, core: (x + step, y, core) if core == 0 else (x, y + step, core)


def outer(step):
    return lambda x, y, core: (x, y + step, core) if core == 0 else (x + step, y, core)


def swap(x, y, core):
    return x, y, 1 - core


def lines():
    device = lambda x, y, core: (x * SIDE + y) * 2 + core
    even = [[device(x, y, 0) for x in range(SIDE)] for y in range(SIDE)]
    return even + [[device(x, y, 1) for y in range(SIDE)] for x in range(SIDE)]


def two_rings(first, second, early):
    chains = {}
    for sign in (1, -1):
        chains[sign] = ([first], [second])
    for step in range(SIDE // 2):
        for sign, steps in ((1, SIDE // 2), (-1, SIDE // 2 - 1)):
            if step >= steps:
                continue
            one, two = chains[sign]
            if step == SIDE // 2 - 1 and sign == 1:
                one[-1], early = lax.optimization_barrier((one[-1], early))
            if step > 1:
                one[-1], two[-2] = lax.optimization_barrier((one[-1], two[-2]))
            if step > 0:
                two[-1], one[-1] = lax.optimization_barrier((two[-1], one[-1]))
            one.append(send(one[-1], outer(sign)))
            two.append(send(two[-1], outer(sign)))
    own = [chains[1][i] + chains[-1][i][1:] for i in range(2)]
    return own[0] + [send(piece, swap) for piece in own[0]], own[1], early


def time_embed(timestep, time_weight):
    half = TFEAT // 2
    freqs = jnp.exp(-jnp.log(10000.0) * jnp.arange(half, dtype=jnp.float32) / half)
    angles = timestep.astype(jnp.float32)[None, None] * freqs[None, :]
    feats = jnp.concatenate([jnp.cos(angles), jnp.sin(angles)], axis=-1)
    return jnp.dot(feats, time_weight.astype(jnp.float32), precision=lax.Precision.HIGHEST)


def wrap(value):
    return lax.rem(value + 2 * SIDE, SIDE)


def holder_of(core, slot):
    return core if slot < SIDE else 1 - core


def fetch_blocks(where, pieces, weight, size, sems):
    x, y, core = where[0], where[1], where[2]
    for slot, ref in enumerate(pieces):
        holder = holder_of(core, slot)
        across = OFFSETS[slot % SIDE]

        def one(b, carry, ref=ref, holder=holder, across=across):
            px = jnp.where(holder == 0, b, wrap(x + across))
            py = jnp.where(holder == 0, wrap(y + across), b)
            inside = 2 * py + holder

            @pl.when(inside < 2 * SIDE - 1)
            def _():
                at = pl.multiple_of((px * (2 * SIDE - 1) + inside) * size, size)
                source = ref.at[pl.ds(pl.multiple_of(b * size, size), size)]
                target = weight.at[pl.ds(at, size)]
                pltpu.make_async_copy(source, target, sems.at[px]).start()

            return carry

        lax.fori_loop(0, SIDE, one, 0)


def await_line(weight, sems, px):
    size = weight.shape[0] // SIDE
    part = weight.at[pl.ds(px * size, size)]
    pltpu.make_async_copy(part, part, sems.at[px]).wait()


def pack_kernel(where, conv, tconv, qkv, last, *refs):
    both, query_key, crossed, value_out, rows, few = refs
    conv_rows, chans = conv.shape
    count = qkv.shape[0]
    f32, bf16 = jnp.float32, jnp.bfloat16
    rows[pl.ds(0, conv_rows), :] = conv[...].astype(f32)
    rows[pl.ds(conv_rows, tconv.shape[0]), :] = tconv[...].astype(f32)
    both[...] = rows[pl.ds(0, both.shape[0]), :].astype(bf16)
    for m in range(3):
        few[pl.ds(m * count, count), :] = qkv[:, m * chans : (m + 1) * chans].astype(f32)
    few[pl.ds(3 * count, count), :] = last[...].astype(f32)
    head = few[pl.ds(0, 2 * count), :].astype(bf16)
    tail = few[pl.ds(2 * count, 2 * count), :].astype(bf16)
    query_key[...] = head
    value_out[...] = tail
    crossed[...] = jnp.where(where[2] == 0, tail.astype(f32), head.astype(f32)).astype(bf16)


def sums_kernel(where, latents, edge, few):
    f32, bf16 = jnp.float32, jnp.bfloat16
    width = latents.shape[1]
    edge[pl.ds(0, width), :] = latents[jnp.where(where[3] == 1, 0, latents.shape[0] - 1)]
    values = latents[0].astype(f32)
    first, second = values, values * values
    for r in range(1, latents.shape[0]):
        values = latents[r].astype(f32)
        first, second = first + values, second + values * values
    left = jnp.concatenate([jnp.sum(v, axis=0, keepdims=True) for v in (first, second)], axis=0)
    few[...] = jnp.zeros(few.shape, f32)
    for part in range(3):
        high = left.astype(bf16).astype(f32)
        few[pl.ds(2 * part, 2), :] = high
        left = left - high
    edge[pl.ds(width, SUM_ROWS), :] = few[pl.ds(0, SUM_ROWS), :].astype(bf16)


def cut_kernel(where, both, following, query_key, crossed, value_out, copies, *scratch):
    block, conv, tconv, few = scratch
    f32, bf16 = jnp.float32, jnp.bfloat16
    count = query_key.shape[0] // 2
    tconv_rows = TCONV_BLOCK - 1
    conv_rows = both.shape[0] - tconv_rows
    inside = 2 * where[1] + where[2]
    own, next_rows = both[...].astype(f32), following[...].astype(f32)
    conv[pl.ds(0, both.shape[0]), :] = own
    tconv[pl.ds(0, tconv_rows), :] = conv[pl.ds(conv_rows, tconv_rows), :]
    conv[pl.ds(conv_rows, both.shape[0]), :] = next_rows
    tconv[pl.ds(tconv_rows, tconv_rows), :] = conv[pl.ds(2 * conv_rows, tconv_rows), :]
    conv_at = jnp.minimum((CONV_BLOCK - conv_rows) * inside, 2 * conv_rows - CONV_BLOCK)
    tconv_at = jnp.minimum(inside, 2 * tconv_rows - TCONV_BLOCK)
    turned = pltpu.roll(conv[...], lax.rem(conv.shape[0] - conv_at, conv.shape[0]), 0)
    block[pl.ds(0, CONV_BLOCK), :] = turned[:CONV_BLOCK].astype(bf16)
    turned = pltpu.roll(tconv[...], lax.rem(tconv.shape[0] - tconv_at, tconv.shape[0]), 0)
    block[pl.ds(CONV_BLOCK, TCONV_BLOCK), :] = turned[:TCONV_BLOCK].astype(bf16)
    near, far, kept = query_key[...].astype(f32), crossed[...].astype(f32), value_out[...].astype(f32)
    even = jnp.where(where[2] == 0, near, far)
    odd = jnp.where(where[2] == 0, far, kept)
    conv[pl.ds(0, 2 * count), :] = even
    conv[pl.ds(2 * count, 2 * count), :] = odd
    for m in range(2):
        for parity in range(2):
            source = conv[pl.ds((2 * parity + m) * count, count), :]
            few[pl.ds((2 * m + parity) * count, count), :] = source
    dense = few[pl.ds(0, 4 * count), :].astype(bf16)
    block[pl.ds(CONV_BLOCK + TCONV_BLOCK, 4 * count), :] = dense
    for b in range(SIDE):
        copies[b] = block[...]


def line_kernel(blocks, conv, rest, dense):
    start = CONV_BLOCK + TCONV_BLOCK
    share = blocks.shape[1] - start
    half = share // 2
    for b in range(SIDE):
        conv[pl.ds(b * CONV_BLOCK, CONV_BLOCK), :] = blocks[b, pl.ds(0, CONV_BLOCK), :]
        taken = blocks[b, pl.ds(CONV_BLOCK, TCONV_BLOCK), :]
        rest[pl.ds(b * TCONV_BLOCK, TCONV_BLOCK), :] = taken
        rows = blocks[b, pl.ds(start, share), :].astype(jnp.float32)
        for m in range(2):
            target = pl.ds((m * SIDE + b) * half, half)
            dense[target, :] = rows[m * half : (m + 1) * half]
    rest[pl.ds(SIDE * TCONV_BLOCK, share * SIDE), :] = dense[...].astype(jnp.bfloat16)


def conv_kernel(where, latents, edge, halo, gain, offset, temb, *refs):
    pieces, (out, weight, shifted, total, sems) = refs[: 2 * SIDE], refs[2 * SIDE :]
    fetch_blocks(where, pieces, weight, CONV_BLOCK, sems)
    rows, width, chans = latents.shape
    size = chans // GROUPS
    group = lax.broadcasted_iota(jnp.int32, (chans, chans), 0) // size
    same = group == lax.broadcasted_iota(jnp.int32, (chans, chans), 1) // size
    parts = edge[pl.ds(width, SUM_ROWS), :].astype(jnp.float32)
    parts = parts + halo[pl.ds(width, SUM_ROWS), :].astype(jnp.float32)
    sums = parts[0:2] + parts[2:4] + parts[4:6]
    frame = jnp.dot(
        jnp.concatenate([sums] * 4, axis=0),
        same.astype(jnp.float32),
        precision=lax.Precision.HIGHEST,
        preferred_element_type=jnp.float32,
    )
    entries = 2 * rows * width * size
    mean = frame[0:1] / entries
    var = frame[1:2] / entries - mean * mean
    scale = lax.rsqrt(var + 1e-05) * gain[...][None, :]
    bias = offset[...][None, :]
    column = lax.broadcasted_iota(jnp.int32, (width, 1), 0)
    lower = where[3]

    def fill(at, raw):
        values = (raw.astype(jnp.float32) - mean) * scale + bias
        values = values / (1.0 + jnp.exp(-values))
        left = jnp.where(column == 0, 0.0, pltpu.roll(values, 1, 0))
        right = jnp.where(column == width - 1, 0.0, pltpu.roll(values, width - 1, 0))
        shifted[0, at] = left.astype(jnp.bfloat16)
        shifted[1, at] = values.astype(jnp.bfloat16)
        shifted[2, at] = right.astype(jnp.bfloat16)

    def one_row(r, carry):
        fill(r + 1, latents[r])
        return carry

    lax.fori_loop(0, rows, one_row, 0)
    fill(jnp.where(lower == 1, 0, rows + 1), halo[pl.ds(0, width), :])
    empty = jnp.where(lower == 1, rows + 1, 0)
    for dx in range(3):
        shifted[dx, empty] = jnp.zeros((width, chans), jnp.bfloat16)
    for px in range(SIDE):
        await_line(weight, sems, px)
    base = latents[...].astype(jnp.float32).reshape(rows * width, chans)
    total[...] = base + temb[...]

    def one_row_of_taps(dy, carry):
        for dx in range(3):
            taken = shifted[dx, pl.ds(dy, rows)].reshape(rows * width, chans)
            at = pl.multiple_of((3 * dy + dx) * chans, 128)
            total[...] += jnp.dot(
                taken, weight[pl.ds(at, chans), :], preferred_element_type=jnp.float32
            )
        return carry

    lax.fori_loop(0, 3, one_row_of_taps, 0)
    out[...] = total[...].astype(jnp.bfloat16)


def layer_norm(values):
    mean = jnp.mean(values, axis=-1, keepdims=True)
    centered = values - mean
    var = jnp.mean(centered * centered, axis=-1, keepdims=True)
    return centered * lax.rsqrt(var + 1e-05)


def temporal_kernel(where, moved, first_gain, second_gain, *refs):
    halves = refs[SIDE : SIDE + 2]
    swapped = {at: halves[h].at[i] for h in range(2) for i, at in enumerate(HALVES[h])}
    pieces = [*refs[:SIDE]] + [swapped[i] for i in range(SIDE)]
    out, tconv, dense, mid, qkv, attended, sems, dense_sem = refs[SIDE + 2 :]
    x, y, core = where[0], where[1], where[2]
    frames, places, chans = moved.shape
    fetch_blocks(where, pieces, tconv, TCONV_BLOCK, sems)
    share = chans // SIDE
    for slot, ref in enumerate(pieces):
        holder = holder_of(core, slot)
        at = wrap(jnp.where(holder == 0, y, x) + OFFSETS[slot % SIDE])
        for m in range(2):
            source = ref.at[pl.ds(SIDE * TCONV_BLOCK + m * share, share)]
            target = dense.at[2 * holder + m, pl.ds(pl.multiple_of(at * share, 16), share)]
            pltpu.make_async_copy(source, target, dense_sem).start()
    rows = frames * places
    values = moved[...].astype(jnp.float32).reshape(rows, chans)
    first = (layer_norm(values) * first_gain[...][None, :]).astype(jnp.bfloat16)
    zero = jnp.zeros((places, chans), jnp.bfloat16)
    before = jnp.concatenate([zero, first[:-places]], axis=0)
    after = jnp.concatenate([first[places:], zero], axis=0)
    for px in range(SIDE):
        await_line(tconv, sems, px)
    mid[...] = values + jnp.dot(
        before, tconv[:chans, :], preferred_element_type=jnp.float32
    )
    mid[...] += jnp.dot(first, tconv[chans : 2 * chans, :], preferred_element_type=jnp.float32)
    mid[...] += jnp.dot(after, tconv[2 * chans :, :], preferred_element_type=jnp.float32)
    second = (layer_norm(mid[...]) * second_gain[...][None, :]).astype(jnp.bfloat16)
    pltpu.make_async_copy(dense, dense, dense_sem).wait()
    tenth = chans // SIDE // SIDE
    there = lax.broadcasted_iota(jnp.int32, (chans, chans), 1)
    ty, tx = lax.div(there, share), lax.div(lax.rem(there, share), tenth)
    origin = tx * share + ty * tenth + lax.rem(there, tenth)
    pick = lax.broadcasted_iota(jnp.int32, (chans, chans), 0) == origin
    pick = jnp.where(pick, 1.0, 0.0).astype(jnp.bfloat16)
    turned = jnp.dot(second, pick, preferred_element_type=jnp.float32).astype(jnp.bfloat16)
    for m in range(3):
        taken = second if m == 2 else turned
        part = jnp.dot(taken, dense[m], preferred_element_type=jnp.float32)
        qkv[m] = part.astype(jnp.bfloat16).reshape(frames, places, chans)
    some = 16
    many = frames * some
    row_place = lax.broadcasted_iota(jnp.int32, (many, many), 0) % some
    col_place = lax.broadcasted_iota(jnp.int32, (many, many), 1) % some
    same = row_place == col_place
    lane = lax.broadcasted_iota(jnp.int32, (1, 2 * HEAD), 1)
    for group in range(places // some):
        spot = slice(group * some, (group + 1) * some)
        for pair in range(chans // (2 * HEAD)):
            lanes = slice(pair * 2 * HEAD, (pair + 1) * 2 * HEAD)
            query = qkv[0, :, spot, lanes].reshape(many, 2 * HEAD)
            key = qkv[1, :, spot, lanes].reshape(many, 2 * HEAD)
            value = qkv[2, :, spot, lanes].reshape(many, 2 * HEAD)
            both = []
            for side in range(2):
                own = (lane < HEAD) if side == 0 else (lane >= HEAD)
                only = jnp.where(own, query, jnp.zeros_like(query))
                scores = lax.dot_general(
                    only, key, (((1,), (1,)), ((), ())), preferred_element_type=jnp.float32
                )
                scores = jnp.where(same, scores * HEAD ** (-0.5), -1e30)
                top = jnp.max(scores, axis=-1, keepdims=True)
                raised = jnp.exp(scores - top)
                weights = raised / jnp.sum(raised, axis=-1, keepdims=True)
                both.append(
                    jnp.dot(weights.astype(jnp.bfloat16), value, preferred_element_type=jnp.float32)
                )
            mixed = jnp.where(lane < HEAD, both[0], both[1]).astype(jnp.bfloat16)
            attended[:, spot, lanes] = mixed.reshape(frames, some, 2 * HEAD)
    projected = jnp.dot(
        attended[...].reshape(rows, chans), dense[3], preferred_element_type=jnp.float32
    )
    out[...] = (mid[...] + projected).astype(jnp.bfloat16).reshape(frames, places, chans)


def specs(count):
    return [pl.BlockSpec(memory_space=pl.ANY)] * count


def shards(
    latents,
    norm_gain,
    norm_bias,
    conv_weight,
    time_weight,
    first_gain,
    tconv_weight,
    second_gain,
    qkv_weight,
    out_weight,
    timesteps,
):
    devices = lax.axis_size(SEQ)
    device = lax.axis_index(SEQ)
    x, y, core = (lax.axis_index(name) for name in SEQ)
    clips = timesteps.shape[0]
    images = clips * FRAMES
    rows, width, chans = latents.shape
    image = device % images
    clip = image // FRAMES
    lower = device // images
    bf16, f32 = jnp.bfloat16, jnp.float32

    where = jnp.stack([x, y, core, lower]).astype(jnp.int32)
    smem = pl.BlockSpec(memory_space=pltpu.SMEM)
    vmem = pl.BlockSpec(memory_space=pltpu.VMEM)
    params = pltpu.CompilerParams(vmem_limit_bytes=VMEM_LIMIT)

    conv_rows, tconv_rows = conv_weight.shape[0], tconv_weight.shape[0]
    few = qkv_weight.shape[0]

    def to_previous(px, py, pcore):
        spot = 2 * py + pcore - 1
        return None if spot < 0 else (px, spot // 2, spot % 2)

    some_rows = jax.ShapeDtypeStruct((2 * few, chans), bf16)
    both, query_key, crossed, value_out = pl.pallas_call(
        pack_kernel,
        out_shape=[
            jax.ShapeDtypeStruct((conv_rows + tconv_rows, chans), bf16),
            some_rows,
            some_rows,
            some_rows,
        ],
        in_specs=[smem] + [vmem] * 4,
        out_specs=[vmem] * 4,
        scratch_shapes=[pltpu.VMEM((64, chans), f32), pltpu.VMEM((24, chans), f32)],
        name="pack",
    )(where, conv_weight, tconv_weight, qkv_weight, out_weight)
    following = send(both, to_previous)
    crossed = send(crossed, swap)

    edge = pl.pallas_call(
        sums_kernel,
        out_shape=jax.ShapeDtypeStruct((width + SUM_ROWS, chans), bf16),
        in_specs=[smem, vmem],
        out_specs=vmem,
        scratch_shapes=[pltpu.VMEM((24, chans), f32)],
        name="sums",
    )(where, latents)
    halo = lax.ppermute(edge, SEQ, [(i, (i + images) % devices) for i in range(devices)])
    temb = time_embed(lax.dynamic_index_in_dim(timesteps, clip, 0, False), time_weight)
    own_rows = CONV_BLOCK + TCONV_BLOCK + 4 * few
    copies = pl.pallas_call(
        cut_kernel,
        out_shape=jax.ShapeDtypeStruct((SIDE, own_rows, chans), bf16),
        in_specs=[smem] + [vmem] * 5,
        out_specs=vmem,
        scratch_shapes=[
            pltpu.VMEM((own_rows, chans), bf16),
            pltpu.VMEM((112, chans), f32),
            pltpu.VMEM((32, chans), f32),
            pltpu.VMEM((24, chans), f32),
        ],
        name="cut",
    )(where, both, following, query_key, crossed, value_out)

    line = lax.all_to_all(
        copies,
        SEQ,
        split_axis=0,
        concat_axis=0,
        axis_index_groups=lines(),
        tiled=True,
    )
    conv_line, rest_line = pl.pallas_call(
        line_kernel,
        out_shape=[
            jax.ShapeDtypeStruct((SIDE * CONV_BLOCK, chans), bf16),
            jax.ShapeDtypeStruct((SIDE * (TCONV_BLOCK + 4 * few), chans), bf16),
        ],
        in_specs=[vmem],
        out_specs=[vmem] * 2,
        scratch_shapes=[pltpu.VMEM((SIDE * 4 * few, chans), f32)],
        name="line",
    )(line)
    conv_line, halo = lax.optimization_barrier((conv_line, halo))
    conv_pieces, rest_pieces, temb = two_rings(conv_line, rest_line, temb)

    swapped = send(jnp.stack([rest_pieces[i] for i in HALVES[0]]), swap)
    spatial = pl.pallas_call(
        conv_kernel,
        out_shape=jax.ShapeDtypeStruct((rows * width, chans), bf16),
        in_specs=[smem] + [vmem] * 6 + specs(2 * SIDE),
        out_specs=vmem,
        scratch_shapes=[
            pltpu.VMEM((9 * chans, chans), bf16),
            pltpu.VMEM((3, rows + 2, width, chans), bf16),
            pltpu.VMEM((rows * width, chans), f32),
            pltpu.SemaphoreType.DMA((SIDE,)),
        ],
        compiler_params=params,
        name="conv",
    )(where, latents, edge, halo, norm_gain, norm_bias, temb, *conv_pieces)
    spatial, late = lax.optimization_barrier((spatial, [rest_pieces[i] for i in HALVES[1]]))
    halves = [swapped, send(jnp.stack(late), swap)]
    moved = lax.all_to_all(spatial, SEQ[1:], split_axis=0, concat_axis=0, tiled=True)
    places = rows * width // FRAMES
    result = pl.pallas_call(
        temporal_kernel,
        out_shape=jax.ShapeDtypeStruct((FRAMES, places, chans), bf16),
        in_specs=[smem, vmem, vmem, vmem] + specs(SIDE + 2),
        out_specs=vmem,
        scratch_shapes=[
            pltpu.VMEM((3 * chans, chans), bf16),
            pltpu.VMEM((4, chans, chans), bf16),
            pltpu.VMEM((FRAMES * places, chans), f32),
            pltpu.VMEM((3, FRAMES, places, chans), bf16),
            pltpu.VMEM((FRAMES, places, chans), bf16),
            pltpu.SemaphoreType.DMA((SIDE,)),
            pltpu.SemaphoreType.DMA,
        ],
        compiler_params=params,
        name="temporal",
    )(
        where,
        moved.reshape(FRAMES, places, chans),
        first_gain,
        second_gain,
        *rest_pieces,
        *halves,
    )
    returned = lax.all_to_all(
        result.reshape(rows * width, chans), SEQ[1:], split_axis=0, concat_axis=0, tiled=True
    )
    return returned.reshape(rows, width, chans)


def solution(mesh):
    torus = Mesh(
        mesh.devices.reshape(mesh.shape["groups"], SIDE, SIDE, 2),
        ("groups", "seq_0", "seq_1", "seq_2"),
    )
    return jax.shard_map(
        shards,
        mesh=torus,
        in_specs=(
            P(GROUPS_SEQ, None, None),
            P(),
            P(),
            P(SEQ, None),
            P(),
            P(),
            P(SEQ, None),
            P(),
            P(SEQ, None),
            P(SEQ, None),
            P("groups"),
        ),
        out_specs=P(GROUPS_SEQ, None, None),
        check_vma=False,
    )
```

```python
import jax
import jax.numpy as jnp
from jax import lax
from jax.experimental import pallas as pl
from jax.experimental.pallas import tpu as pltpu
from jax.sharding import Mesh
from jax.sharding import PartitionSpec as P

HEAD = 64
GROUPS = 32
TFEAT = 320
FRAMES = 16
SEQ = ("seq_0", "seq_1", "seq_2")
GROUPS_SEQ = ("groups", "seq_0", "seq_1", "seq_2")
SIDE = 8
CONV_BLOCK = 48
TCONV_BLOCK = 16
SUM_ROWS = 16
VMEM_LIMIT = 56 * 2**20
OFFSETS = (0, -1, -2, -3, -4, 1, 2, 3)
HALVES = ((0, 1, 2, 5), (3, 4, 6, 7))


def route(target):
    pairs = []
    for x in range(SIDE):
        for y in range(SIDE):
            for core in range(2):
                there = target(x, y, core)
                if there is not None:
                    tx, ty, tcore = there
                    to = (tx % SIDE * SIDE + ty % SIDE) * 2 + tcore
                    pairs.append(((x * SIDE + y) * 2 + core, to))
    return pairs


def send(block, target):
    return lax.ppermute(block, SEQ, route(target))


def inner(step):
    return lambda x, y, core: (x + step, y, core) if core == 0 else (x, y + step, core)


def outer(step):
    return lambda x, y, core: (x, y + step, core) if core == 0 else (x + step, y, core)


def swap(x, y, core):
    return x, y, 1 - core


def lines():
    device = lambda x, y, core: (x * SIDE + y) * 2 + core
    even = [[device(x, y, 0) for x in range(SIDE)] for y in range(SIDE)]
    return even + [[device(x, y, 1) for y in range(SIDE)] for x in range(SIDE)]


def two_rings(first, second, early):
    chains = {}
    for sign in (1, -1):
        chains[sign] = ([first], [second])
    for step in range(SIDE // 2):
        for sign, steps in ((1, SIDE // 2), (-1, SIDE // 2 - 1)):
            if step >= steps:
                continue
            one, two = chains[sign]
            if step == SIDE // 2 - 1 and sign == 1:
                one[-1], early = lax.optimization_barrier((one[-1], early))
            if step > 1:
                one[-1], two[-2] = lax.optimization_barrier((one[-1], two[-2]))
            if step > 0:
                two[-1], one[-1] = lax.optimization_barrier((two[-1], one[-1]))
            one.append(send(one[-1], outer(sign)))
            two.append(send(two[-1], outer(sign)))
    own = [chains[1][i] + chains[-1][i][1:] for i in range(2)]
    return own[0] + [send(piece, swap) for piece in own[0]], own[1], early


def time_embed(timestep, time_weight):
    half = TFEAT // 2
    freqs = jnp.exp(-jnp.log(10000.0) * jnp.arange(half, dtype=jnp.float32) / half)
    angles = timestep.astype(jnp.float32)[None, None] * freqs[None, :]
    feats = jnp.concatenate([jnp.cos(angles), jnp.sin(angles)], axis=-1)
    return jnp.dot(feats, time_weight.astype(jnp.float32), precision=lax.Precision.HIGHEST)


def wrap(value):
    return lax.rem(value + 2 * SIDE, SIDE)


def holder_of(core, slot):
    return core if slot < SIDE else 1 - core


def fetch_blocks(where, pieces, weight, size, sems):
    x, y, core = where[0], where[1], where[2]
    for slot, ref in enumerate(pieces):
        holder = holder_of(core, slot)
        across = OFFSETS[slot % SIDE]

        def one(b, carry, ref=ref, holder=holder, across=across):
            px = jnp.where(holder == 0, b, wrap(x + across))
            py = jnp.where(holder == 0, wrap(y + across), b)
            inside = 2 * py + holder

            @pl.when(inside < 2 * SIDE - 1)
            def _():
                at = pl.multiple_of((px * (2 * SIDE - 1) + inside) * size, size)
                source = ref.at[pl.ds(pl.multiple_of(b * size, size), size)]
                target = weight.at[pl.ds(at, size)]
                pltpu.make_async_copy(source, target, sems.at[px]).start()

            return carry

        lax.fori_loop(0, SIDE, one, 0)


def await_line(weight, sems, px):
    size = weight.shape[0] // SIDE
    part = weight.at[pl.ds(px * size, size)]
    pltpu.make_async_copy(part, part, sems.at[px]).wait()


def pack_kernel(where, conv, tconv, qkv, last, *refs):
    both, query_key, crossed, value_out, rows, few = refs
    conv_rows, chans = conv.shape
    count = qkv.shape[0]
    f32, bf16 = jnp.float32, jnp.bfloat16
    rows[pl.ds(0, conv_rows), :] = conv[...].astype(f32)
    rows[pl.ds(conv_rows, tconv.shape[0]), :] = tconv[...].astype(f32)
    both[...] = rows[pl.ds(0, both.shape[0]), :].astype(bf16)
    for m in range(3):
        few[pl.ds(m * count, count), :] = qkv[:, m * chans : (m + 1) * chans].astype(f32)
    few[pl.ds(3 * count, count), :] = last[...].astype(f32)
    head = few[pl.ds(0, 2 * count), :].astype(bf16)
    tail = few[pl.ds(2 * count, 2 * count), :].astype(bf16)
    query_key[...] = head
    value_out[...] = tail
    crossed[...] = jnp.where(where[2] == 0, tail.astype(f32), head.astype(f32)).astype(bf16)


def sums_kernel(where, latents, edge, few):
    f32, bf16 = jnp.float32, jnp.bfloat16
    width = latents.shape[1]
    edge[pl.ds(0, width), :] = latents[jnp.where(where[3] == 1, 0, latents.shape[0] - 1)]
    values = latents[0].astype(f32)
    first, second = values, values * values
    for r in range(1, latents.shape[0]):
        values = latents[r].astype(f32)
        first, second = first + values, second + values * values
    left = jnp.concatenate([jnp.sum(v, axis=0, keepdims=True) for v in (first, second)], axis=0)
    few[...] = jnp.zeros(few.shape, f32)
    for part in range(3):
        high = left.astype(bf16).astype(f32)
        few[pl.ds(2 * part, 2), :] = high
        left = left - high
    edge[pl.ds(width, SUM_ROWS), :] = few[pl.ds(0, SUM_ROWS), :].astype(bf16)


def cut_kernel(where, both, following, query_key, crossed, value_out, copies, *scratch):
    block, conv, tconv, few = scratch
    f32, bf16 = jnp.float32, jnp.bfloat16
    count = query_key.shape[0] // 2
    tconv_rows = TCONV_BLOCK - 1
    conv_rows = both.shape[0] - tconv_rows
    inside = 2 * where[1] + where[2]
    own, next_rows = both[...].astype(f32), following[...].astype(f32)
    conv[pl.ds(0, both.shape[0]), :] = own
    tconv[pl.ds(0, tconv_rows), :] = conv[pl.ds(conv_rows, tconv_rows), :]
    conv[pl.ds(conv_rows, both.shape[0]), :] = next_rows
    tconv[pl.ds(tconv_rows, tconv_rows), :] = conv[pl.ds(2 * conv_rows, tconv_rows), :]
    conv_at = jnp.minimum((CONV_BLOCK - conv_rows) * inside, 2 * conv_rows - CONV_BLOCK)
    tconv_at = jnp.minimum(inside, 2 * tconv_rows - TCONV_BLOCK)
    turned = pltpu.roll(conv[...], lax.rem(conv.shape[0] - conv_at, conv.shape[0]), 0)
    block[pl.ds(0, CONV_BLOCK), :] = turned[:CONV_BLOCK].astype(bf16)
    turned = pltpu.roll(tconv[...], lax.rem(tconv.shape[0] - tconv_at, tconv.shape[0]), 0)
    block[pl.ds(CONV_BLOCK, TCONV_BLOCK), :] = turned[:TCONV_BLOCK].astype(bf16)
    near, far, kept = query_key[...].astype(f32), crossed[...].astype(f32), value_out[...].astype(f32)
    even = jnp.where(where[2] == 0, near, far)
    odd = jnp.where(where[2] == 0, far, kept)
    conv[pl.ds(0, 2 * count), :] = even
    conv[pl.ds(2 * count, 2 * count), :] = odd
    for m in range(2):
        for parity in range(2):
            source = conv[pl.ds((2 * parity + m) * count, count), :]
            few[pl.ds((2 * m + parity) * count, count), :] = source
    dense = few[pl.ds(0, 4 * count), :].astype(bf16)
    block[pl.ds(CONV_BLOCK + TCONV_BLOCK, 4 * count), :] = dense
    for b in range(SIDE):
        copies[b] = block[...]


def line_kernel(blocks, conv, rest, dense):
    start = CONV_BLOCK + TCONV_BLOCK
    share = blocks.shape[1] - start
    half = share // 2
    for b in range(SIDE):
        conv[pl.ds(b * CONV_BLOCK, CONV_BLOCK), :] = blocks[b, pl.ds(0, CONV_BLOCK), :]
        taken = blocks[b, pl.ds(CONV_BLOCK, TCONV_BLOCK), :]
        rest[pl.ds(b * TCONV_BLOCK, TCONV_BLOCK), :] = taken
        rows = blocks[b, pl.ds(start, share), :].astype(jnp.float32)
        for m in range(2):
            target = pl.ds((m * SIDE + b) * half, half)
            dense[target, :] = rows[m * half : (m + 1) * half]
    rest[pl.ds(SIDE * TCONV_BLOCK, share * SIDE), :] = dense[...].astype(jnp.bfloat16)


def conv_kernel(where, latents, edge, halo, gain, offset, temb, *refs):
    pieces, (out, weight, shifted, total, sems) = refs[: 2 * SIDE], refs[2 * SIDE :]
    fetch_blocks(where, pieces, weight, CONV_BLOCK, sems)
    rows, width, chans = latents.shape
    size = chans // GROUPS
    group = lax.broadcasted_iota(jnp.int32, (chans, chans), 0) // size
    same = group == lax.broadcasted_iota(jnp.int32, (chans, chans), 1) // size
    parts = edge[pl.ds(width, SUM_ROWS), :].astype(jnp.float32)
    parts = parts + halo[pl.ds(width, SUM_ROWS), :].astype(jnp.float32)
    sums = parts[0:2] + parts[2:4] + parts[4:6]
    frame = jnp.dot(
        jnp.concatenate([sums] * 4, axis=0),
        same.astype(jnp.float32),
        precision=lax.Precision.HIGHEST,
        preferred_element_type=jnp.float32,
    )
    entries = 2 * rows * width * size
    mean = frame[0:1] / entries
    var = frame[1:2] / entries - mean * mean
    scale = lax.rsqrt(var + 1e-05) * gain[...][None, :]
    bias = offset[...][None, :]
    column = lax.broadcasted_iota(jnp.int32, (width, 1), 0)
    lower = where[3]

    def fill(at, raw):
        values = (raw.astype(jnp.float32) - mean) * scale + bias
        values = values / (1.0 + jnp.exp(-values))
        left = jnp.where(column == 0, 0.0, pltpu.roll(values, 1, 0))
        right = jnp.where(column == width - 1, 0.0, pltpu.roll(values, width - 1, 0))
        shifted[0, at] = left.astype(jnp.bfloat16)
        shifted[1, at] = values.astype(jnp.bfloat16)
        shifted[2, at] = right.astype(jnp.bfloat16)

    def one_row(r, carry):
        fill(r + 1, latents[r])
        return carry

    lax.fori_loop(0, rows, one_row, 0)
    fill(jnp.where(lower == 1, 0, rows + 1), halo[pl.ds(0, width), :])
    empty = jnp.where(lower == 1, rows + 1, 0)
    for dx in range(3):
        shifted[dx, empty] = jnp.zeros((width, chans), jnp.bfloat16)
    for px in range(SIDE):
        await_line(weight, sems, px)
    base = latents[...].astype(jnp.float32).reshape(rows * width, chans)
    total[...] = base + temb[...]

    def one_row_of_taps(dy, carry):
        for dx in range(3):
            taken = shifted[dx, pl.ds(dy, rows)].reshape(rows * width, chans)
            at = pl.multiple_of((3 * dy + dx) * chans, 128)
            total[...] += jnp.dot(
                taken, weight[pl.ds(at, chans), :], preferred_element_type=jnp.float32
            )
        return carry

    lax.fori_loop(0, 3, one_row_of_taps, 0)
    out[...] = total[...].astype(jnp.bfloat16)


def layer_norm(values):
    mean = jnp.mean(values, axis=-1, keepdims=True)
    centered = values - mean
    var = jnp.mean(centered * centered, axis=-1, keepdims=True)
    return centered * lax.rsqrt(var + 1e-05)


def temporal_kernel(where, moved, first_gain, second_gain, *refs):
    late = SIDE + 1 + len(HALVES[1])
    swapped = {at: refs[SIDE].at[i] for i, at in enumerate(HALVES[0])}
    swapped |= dict(zip(HALVES[1], refs[SIDE + 1 : late]))
    pieces = [*refs[:SIDE]] + [swapped[i] for i in range(SIDE)]
    out, tconv, dense, mid, qkv, attended, sems, dense_sem = refs[late:]
    x, y, core = where[0], where[1], where[2]
    frames, places, chans = moved.shape
    fetch_blocks(where, pieces, tconv, TCONV_BLOCK, sems)
    share = chans // SIDE
    for slot, ref in enumerate(pieces):
        holder = holder_of(core, slot)
        at = wrap(jnp.where(holder == 0, y, x) + OFFSETS[slot % SIDE])
        for m in range(2):
            source = ref.at[pl.ds(SIDE * TCONV_BLOCK + m * share, share)]
            target = dense.at[2 * holder + m, pl.ds(pl.multiple_of(at * share, 16), share)]
            pltpu.make_async_copy(source, target, dense_sem).start()
    rows = frames * places
    values = moved[...].astype(jnp.float32).reshape(rows, chans)
    first = (layer_norm(values) * first_gain[...][None, :]).astype(jnp.bfloat16)
    zero = jnp.zeros((places, chans), jnp.bfloat16)
    before = jnp.concatenate([zero, first[:-places]], axis=0)
    after = jnp.concatenate([first[places:], zero], axis=0)
    for px in range(SIDE):
        await_line(tconv, sems, px)
    mid[...] = values + jnp.dot(
        before, tconv[:chans, :], preferred_element_type=jnp.float32
    )
    mid[...] += jnp.dot(first, tconv[chans : 2 * chans, :], preferred_element_type=jnp.float32)
    mid[...] += jnp.dot(after, tconv[2 * chans :, :], preferred_element_type=jnp.float32)
    second = (layer_norm(mid[...]) * second_gain[...][None, :]).astype(jnp.bfloat16)
    pltpu.make_async_copy(dense, dense, dense_sem).wait()
    tenth = chans // SIDE // SIDE
    there = lax.broadcasted_iota(jnp.int32, (chans, chans), 1)
    ty, tx = lax.div(there, share), lax.div(lax.rem(there, share), tenth)
    origin = tx * share + ty * tenth + lax.rem(there, tenth)
    pick = lax.broadcasted_iota(jnp.int32, (chans, chans), 0) == origin
    pick = jnp.where(pick, 1.0, 0.0).astype(jnp.bfloat16)
    turned = jnp.dot(second, pick, preferred_element_type=jnp.float32).astype(jnp.bfloat16)
    for m in range(3):
        taken = second if m == 2 else turned
        part = jnp.dot(taken, dense[m], preferred_element_type=jnp.float32)
        qkv[m] = part.astype(jnp.bfloat16).reshape(frames, places, chans)
    some = 16
    many = frames * some
    row_place = lax.broadcasted_iota(jnp.int32, (many, many), 0) % some
    col_place = lax.broadcasted_iota(jnp.int32, (many, many), 1) % some
    same = row_place == col_place
    lane = lax.broadcasted_iota(jnp.int32, (1, 2 * HEAD), 1)
    for group in range(places // some):
        spot = slice(group * some, (group + 1) * some)
        for pair in range(chans // (2 * HEAD)):
            lanes = slice(pair * 2 * HEAD, (pair + 1) * 2 * HEAD)
            query = qkv[0, :, spot, lanes].reshape(many, 2 * HEAD)
            key = qkv[1, :, spot, lanes].reshape(many, 2 * HEAD)
            value = qkv[2, :, spot, lanes].reshape(many, 2 * HEAD)
            both = []
            for side in range(2):
                own = (lane < HEAD) if side == 0 else (lane >= HEAD)
                only = jnp.where(own, query, jnp.zeros_like(query))
                scores = lax.dot_general(
                    only, key, (((1,), (1,)), ((), ())), preferred_element_type=jnp.float32
                )
                scores = jnp.where(same, scores * HEAD ** (-0.5), -1e30)
                top = jnp.max(scores, axis=-1, keepdims=True)
                raised = jnp.exp(scores - top)
                weights = raised / jnp.sum(raised, axis=-1, keepdims=True)
                both.append(
                    jnp.dot(weights.astype(jnp.bfloat16), value, preferred_element_type=jnp.float32)
                )
            mixed = jnp.where(lane < HEAD, both[0], both[1]).astype(jnp.bfloat16)
            attended[:, spot, lanes] = mixed.reshape(frames, some, 2 * HEAD)
    projected = jnp.dot(
        attended[...].reshape(rows, chans), dense[3], preferred_element_type=jnp.float32
    )
    out[...] = (mid[...] + projected).astype(jnp.bfloat16).reshape(frames, places, chans)


def specs(count):
    return [pl.BlockSpec(memory_space=pl.ANY)] * count


def shards(
    latents,
    norm_gain,
    norm_bias,
    conv_weight,
    time_weight,
    first_gain,
    tconv_weight,
    second_gain,
    qkv_weight,
    out_weight,
    timesteps,
):
    devices = lax.axis_size(SEQ)
    device = lax.axis_index(SEQ)
    x, y, core = (lax.axis_index(name) for name in SEQ)
    clips = timesteps.shape[0]
    images = clips * FRAMES
    rows, width, chans = latents.shape
    image = device % images
    clip = image // FRAMES
    lower = device // images
    bf16, f32 = jnp.bfloat16, jnp.float32

    where = jnp.stack([x, y, core, lower]).astype(jnp.int32)
    smem = pl.BlockSpec(memory_space=pltpu.SMEM)
    vmem = pl.BlockSpec(memory_space=pltpu.VMEM)
    params = pltpu.CompilerParams(vmem_limit_bytes=VMEM_LIMIT)

    conv_rows, tconv_rows = conv_weight.shape[0], tconv_weight.shape[0]
    few = qkv_weight.shape[0]

    def to_previous(px, py, pcore):
        spot = 2 * py + pcore - 1
        return None if spot < 0 else (px, spot // 2, spot % 2)

    some_rows = jax.ShapeDtypeStruct((2 * few, chans), bf16)
    both, query_key, crossed, value_out = pl.pallas_call(
        pack_kernel,
        out_shape=[
            jax.ShapeDtypeStruct((conv_rows + tconv_rows, chans), bf16),
            some_rows,
            some_rows,
            some_rows,
        ],
        in_specs=[smem] + [vmem] * 4,
        out_specs=[vmem] * 4,
        scratch_shapes=[pltpu.VMEM((64, chans), f32), pltpu.VMEM((24, chans), f32)],
        name="pack",
    )(where, conv_weight, tconv_weight, qkv_weight, out_weight)
    following = send(both, to_previous)
    crossed = send(crossed, swap)

    edge = pl.pallas_call(
        sums_kernel,
        out_shape=jax.ShapeDtypeStruct((width + SUM_ROWS, chans), bf16),
        in_specs=[smem, vmem],
        out_specs=vmem,
        scratch_shapes=[pltpu.VMEM((24, chans), f32)],
        name="sums",
    )(where, latents)
    halo = lax.ppermute(edge, SEQ, [(i, (i + images) % devices) for i in range(devices)])
    temb = time_embed(lax.dynamic_index_in_dim(timesteps, clip, 0, False), time_weight)
    own_rows = CONV_BLOCK + TCONV_BLOCK + 4 * few
    copies = pl.pallas_call(
        cut_kernel,
        out_shape=jax.ShapeDtypeStruct((SIDE, own_rows, chans), bf16),
        in_specs=[smem] + [vmem] * 5,
        out_specs=vmem,
        scratch_shapes=[
            pltpu.VMEM((own_rows, chans), bf16),
            pltpu.VMEM((112, chans), f32),
            pltpu.VMEM((32, chans), f32),
            pltpu.VMEM((24, chans), f32),
        ],
        name="cut",
    )(where, both, following, query_key, crossed, value_out)

    line = lax.all_to_all(
        copies,
        SEQ,
        split_axis=0,
        concat_axis=0,
        axis_index_groups=lines(),
        tiled=True,
    )
    conv_line, rest_line = pl.pallas_call(
        line_kernel,
        out_shape=[
            jax.ShapeDtypeStruct((SIDE * CONV_BLOCK, chans), bf16),
            jax.ShapeDtypeStruct((SIDE * (TCONV_BLOCK + 4 * few), chans), bf16),
        ],
        in_specs=[vmem],
        out_specs=[vmem] * 2,
        scratch_shapes=[pltpu.VMEM((SIDE * 4 * few, chans), f32)],
        name="line",
    )(line)
    conv_line, halo = lax.optimization_barrier((conv_line, halo))
    conv_pieces, rest_pieces, temb = two_rings(conv_line, rest_line, temb)

    swapped = send(jnp.stack([rest_pieces[i] for i in HALVES[0]]), swap)
    spatial = pl.pallas_call(
        conv_kernel,
        out_shape=jax.ShapeDtypeStruct((rows * width, chans), bf16),
        in_specs=[smem] + [vmem] * 6 + specs(2 * SIDE),
        out_specs=vmem,
        scratch_shapes=[
            pltpu.VMEM((9 * chans, chans), bf16),
            pltpu.VMEM((3, rows + 2, width, chans), bf16),
            pltpu.VMEM((rows * width, chans), f32),
            pltpu.SemaphoreType.DMA((SIDE,)),
        ],
        compiler_params=params,
        name="conv",
    )(where, latents, edge, halo, norm_gain, norm_bias, temb, *conv_pieces)
    spatial, late = lax.optimization_barrier((spatial, [rest_pieces[i] for i in HALVES[1]]))
    halves = [swapped] + [send(piece, swap) for piece in late]
    moved = lax.all_to_all(spatial, SEQ[1:], split_axis=0, concat_axis=0, tiled=True)
    places = rows * width // FRAMES
    result = pl.pallas_call(
        temporal_kernel,
        out_shape=jax.ShapeDtypeStruct((FRAMES, places, chans), bf16),
        in_specs=[smem, vmem, vmem, vmem] + specs(SIDE + 1 + len(HALVES[1])),
        out_specs=vmem,
        scratch_shapes=[
            pltpu.VMEM((3 * chans, chans), bf16),
            pltpu.VMEM((4, chans, chans), bf16),
            pltpu.VMEM((FRAMES * places, chans), f32),
            pltpu.VMEM((3, FRAMES, places, chans), bf16),
            pltpu.VMEM((FRAMES, places, chans), bf16),
            pltpu.SemaphoreType.DMA((SIDE,)),
            pltpu.SemaphoreType.DMA,
        ],
        compiler_params=params,
        name="temporal",
    )(
        where,
        moved.reshape(FRAMES, places, chans),
        first_gain,
        second_gain,
        *rest_pieces,
        *halves,
    )
    returned = lax.all_to_all(
        result.reshape(rows * width, chans), SEQ[1:], split_axis=0, concat_axis=0, tiled=True
    )
    return returned.reshape(rows, width, chans)


def solution(mesh):
    torus = Mesh(
        mesh.devices.reshape(mesh.shape["groups"], SIDE, SIDE, 2),
        ("groups", "seq_0", "seq_1", "seq_2"),
    )
    return jax.shard_map(
        shards,
        mesh=torus,
        in_specs=(
            P(GROUPS_SEQ, None, None),
            P(),
            P(),
            P(SEQ, None),
            P(),
            P(),
            P(SEQ, None),
            P(),
            P(SEQ, None),
            P(SEQ, None),
            P("groups"),
        ),
        out_specs=P(GROUPS_SEQ, None, None),
        check_vma=False,
    )
```

```python
import jax
import jax.numpy as jnp
from jax import lax
from jax.experimental import pallas as pl
from jax.experimental.pallas import tpu as pltpu
from jax.sharding import Mesh
from jax.sharding import PartitionSpec as P

HEAD = 64
GROUPS = 32
TFEAT = 320
FRAMES = 16
SEQ = ("seq_0", "seq_1", "seq_2")
GROUPS_SEQ = ("groups", "seq_0", "seq_1", "seq_2")
SIDE = 8
CONV_BLOCK = 48
TCONV_BLOCK = 16
SUM_ROWS = 16
VMEM_LIMIT = 56 * 2**20
OFFSETS = (0, -1, -2, -3, -4, 1, 2, 3)


def route(target):
    pairs = []
    for x in range(SIDE):
        for y in range(SIDE):
            for core in range(2):
                there = target(x, y, core)
                if there is not None:
                    tx, ty, tcore = there
                    to = (tx % SIDE * SIDE + ty % SIDE) * 2 + tcore
                    pairs.append(((x * SIDE + y) * 2 + core, to))
    return pairs


def send(block, target):
    return lax.ppermute(block, SEQ, route(target))


def inner(step):
    return lambda x, y, core: (x + step, y, core) if core == 0 else (x, y + step, core)


def outer(step):
    return lambda x, y, core: (x, y + step, core) if core == 0 else (x + step, y, core)


def swap(x, y, core):
    return x, y, 1 - core


def lines():
    device = lambda x, y, core: (x * SIDE + y) * 2 + core
    even = [[device(x, y, 0) for x in range(SIDE)] for y in range(SIDE)]
    return even + [[device(x, y, 1) for y in range(SIDE)] for x in range(SIDE)]


def two_rings(first, second, early):
    chains = {}
    for sign in (1, -1):
        chains[sign] = ([first], [second])
    for step in range(SIDE // 2):
        for sign, steps in ((1, SIDE // 2), (-1, SIDE // 2 - 1)):
            if step >= steps:
                continue
            one, two = chains[sign]
            if step == SIDE // 2 - 1 and sign == 1:
                one[-1], early = lax.optimization_barrier((one[-1], early))
            if step > 1:
                one[-1], two[-2] = lax.optimization_barrier((one[-1], two[-2]))
            if step > 0:
                two[-1], one[-1] = lax.optimization_barrier((two[-1], one[-1]))
            one.append(send(one[-1], outer(sign)))
            two.append(send(two[-1], outer(sign)))
    own = [chains[1][i] + chains[-1][i][1:] for i in range(2)]
    return own[0] + [send(piece, swap) for piece in own[0]], own[1], early


def time_embed(timestep, time_weight):
    half = TFEAT // 2
    freqs = jnp.exp(-jnp.log(10000.0) * jnp.arange(half, dtype=jnp.float32) / half)
    angles = timestep.astype(jnp.float32)[None, None] * freqs[None, :]
    feats = jnp.concatenate([jnp.cos(angles), jnp.sin(angles)], axis=-1)
    return jnp.dot(feats, time_weight.astype(jnp.float32), precision=lax.Precision.HIGHEST)


def wrap(value):
    return lax.rem(value + 2 * SIDE, SIDE)


def holder_of(core, slot):
    return core if slot < SIDE else 1 - core


def fetch_blocks(where, pieces, weight, size, sems):
    x, y, core = where[0], where[1], where[2]
    for slot, ref in enumerate(pieces):
        holder = holder_of(core, slot)
        across = OFFSETS[slot % SIDE]

        def one(b, carry, ref=ref, holder=holder, across=across):
            px = jnp.where(holder == 0, b, wrap(x + across))
            py = jnp.where(holder == 0, wrap(y + across), b)
            inside = 2 * py + holder

            @pl.when(inside < 2 * SIDE - 1)
            def _():
                at = pl.multiple_of((px * (2 * SIDE - 1) + inside) * size, size)
                source = ref.at[pl.ds(pl.multiple_of(b * size, size), size)]
                target = weight.at[pl.ds(at, size)]
                pltpu.make_async_copy(source, target, sems.at[px]).start()

            return carry

        lax.fori_loop(0, SIDE, one, 0)


def await_line(weight, sems, px):
    size = weight.shape[0] // SIDE
    part = weight.at[pl.ds(px * size, size)]
    pltpu.make_async_copy(part, part, sems.at[px]).wait()


def pack_kernel(where, conv, tconv, qkv, last, *refs):
    both, query_key, crossed, value_out, rows, few = refs
    conv_rows, chans = conv.shape
    count = qkv.shape[0]
    f32, bf16 = jnp.float32, jnp.bfloat16
    rows[pl.ds(0, conv_rows), :] = conv[...].astype(f32)
    rows[pl.ds(conv_rows, tconv.shape[0]), :] = tconv[...].astype(f32)
    both[...] = rows[pl.ds(0, both.shape[0]), :].astype(bf16)
    for m in range(3):
        few[pl.ds(m * count, count), :] = qkv[:, m * chans : (m + 1) * chans].astype(f32)
    few[pl.ds(3 * count, count), :] = last[...].astype(f32)
    head = few[pl.ds(0, 2 * count), :].astype(bf16)
    tail = few[pl.ds(2 * count, 2 * count), :].astype(bf16)
    query_key[...] = head
    value_out[...] = tail
    crossed[...] = jnp.where(where[2] == 0, tail.astype(f32), head.astype(f32)).astype(bf16)


def sums_kernel(where, latents, edge, few):
    f32, bf16 = jnp.float32, jnp.bfloat16
    width = latents.shape[1]
    edge[pl.ds(0, width), :] = latents[jnp.where(where[3] == 1, 0, latents.shape[0] - 1)]
    values = latents[0].astype(f32)
    first, second = values, values * values
    for r in range(1, latents.shape[0]):
        values = latents[r].astype(f32)
        first, second = first + values, second + values * values
    left = jnp.concatenate([jnp.sum(v, axis=0, keepdims=True) for v in (first, second)], axis=0)
    few[...] = jnp.zeros(few.shape, f32)
    for part in range(3):
        high = left.astype(bf16).astype(f32)
        few[pl.ds(2 * part, 2), :] = high
        left = left - high
    edge[pl.ds(width, SUM_ROWS), :] = few[pl.ds(0, SUM_ROWS), :].astype(bf16)


def cut_kernel(where, both, following, query_key, crossed, value_out, copies, *scratch):
    block, conv, tconv, few = scratch
    f32, bf16 = jnp.float32, jnp.bfloat16
    count = query_key.shape[0] // 2
    tconv_rows = TCONV_BLOCK - 1
    conv_rows = both.shape[0] - tconv_rows
    inside = 2 * where[1] + where[2]
    own, next_rows = both[...].astype(f32), following[...].astype(f32)
    conv[pl.ds(0, both.shape[0]), :] = own
    tconv[pl.ds(0, tconv_rows), :] = conv[pl.ds(conv_rows, tconv_rows), :]
    conv[pl.ds(conv_rows, both.shape[0]), :] = next_rows
    tconv[pl.ds(tconv_rows, tconv_rows), :] = conv[pl.ds(2 * conv_rows, tconv_rows), :]
    conv_at = jnp.minimum((CONV_BLOCK - conv_rows) * inside, 2 * conv_rows - CONV_BLOCK)
    tconv_at = jnp.minimum(inside, 2 * tconv_rows - TCONV_BLOCK)
    turned = pltpu.roll(conv[...], lax.rem(conv.shape[0] - conv_at, conv.shape[0]), 0)
    block[pl.ds(0, CONV_BLOCK), :] = turned[:CONV_BLOCK].astype(bf16)
    turned = pltpu.roll(tconv[...], lax.rem(tconv.shape[0] - tconv_at, tconv.shape[0]), 0)
    block[pl.ds(CONV_BLOCK, TCONV_BLOCK), :] = turned[:TCONV_BLOCK].astype(bf16)
    near, far, kept = query_key[...].astype(f32), crossed[...].astype(f32), value_out[...].astype(f32)
    even = jnp.where(where[2] == 0, near, far)
    odd = jnp.where(where[2] == 0, far, kept)
    conv[pl.ds(0, 2 * count), :] = even
    conv[pl.ds(2 * count, 2 * count), :] = odd
    for m in range(2):
        for parity in range(2):
            source = conv[pl.ds((2 * parity + m) * count, count), :]
            few[pl.ds((2 * m + parity) * count, count), :] = source
    dense = few[pl.ds(0, 4 * count), :].astype(bf16)
    block[pl.ds(CONV_BLOCK + TCONV_BLOCK, 4 * count), :] = dense
    for b in range(SIDE):
        copies[b] = block[...]


def line_kernel(blocks, conv, rest, dense):
    start = CONV_BLOCK + TCONV_BLOCK
    share = blocks.shape[1] - start
    half = share // 2
    for b in range(SIDE):
        conv[pl.ds(b * CONV_BLOCK, CONV_BLOCK), :] = blocks[b, pl.ds(0, CONV_BLOCK), :]
        taken = blocks[b, pl.ds(CONV_BLOCK, TCONV_BLOCK), :]
        rest[pl.ds(b * TCONV_BLOCK, TCONV_BLOCK), :] = taken
        rows = blocks[b, pl.ds(start, share), :].astype(jnp.float32)
        for m in range(2):
            target = pl.ds((m * SIDE + b) * half, half)
            dense[target, :] = rows[m * half : (m + 1) * half]
    rest[pl.ds(SIDE * TCONV_BLOCK, share * SIDE), :] = dense[...].astype(jnp.bfloat16)


def conv_kernel(where, latents, edge, halo, gain, offset, temb, *refs):
    pieces, (out, weight, shifted, total, sems) = refs[: 2 * SIDE], refs[2 * SIDE :]
    fetch_blocks(where, pieces, weight, CONV_BLOCK, sems)
    rows, width, chans = latents.shape
    size = chans // GROUPS
    group = lax.broadcasted_iota(jnp.int32, (chans, chans), 0) // size
    same = group == lax.broadcasted_iota(jnp.int32, (chans, chans), 1) // size
    parts = edge[pl.ds(width, SUM_ROWS), :].astype(jnp.float32)
    parts = parts + halo[pl.ds(width, SUM_ROWS), :].astype(jnp.float32)
    sums = parts[0:2] + parts[2:4] + parts[4:6]
    frame = jnp.dot(
        jnp.concatenate([sums] * 4, axis=0),
        same.astype(jnp.float32),
        precision=lax.Precision.HIGHEST,
        preferred_element_type=jnp.float32,
    )
    entries = 2 * rows * width * size
    mean = frame[0:1] / entries
    var = frame[1:2] / entries - mean * mean
    scale = lax.rsqrt(var + 1e-05) * gain[...][None, :]
    bias = offset[...][None, :]
    column = lax.broadcasted_iota(jnp.int32, (width, 1), 0)
    lower = where[3]

    def fill(at, raw):
        values = (raw.astype(jnp.float32) - mean) * scale + bias
        values = values / (1.0 + jnp.exp(-values))
        left = jnp.where(column == 0, 0.0, pltpu.roll(values, 1, 0))
        right = jnp.where(column == width - 1, 0.0, pltpu.roll(values, width - 1, 0))
        shifted[0, at] = left.astype(jnp.bfloat16)
        shifted[1, at] = values.astype(jnp.bfloat16)
        shifted[2, at] = right.astype(jnp.bfloat16)

    def one_row(r, carry):
        fill(r + 1, latents[r])
        return carry

    lax.fori_loop(0, rows, one_row, 0)
    fill(jnp.where(lower == 1, 0, rows + 1), halo[pl.ds(0, width), :])
    empty = jnp.where(lower == 1, rows + 1, 0)
    for dx in range(3):
        shifted[dx, empty] = jnp.zeros((width, chans), jnp.bfloat16)
    for px in range(SIDE):
        await_line(weight, sems, px)
    base = latents[...].astype(jnp.float32).reshape(rows * width, chans)
    total[...] = base + temb[...]

    def one_row_of_taps(dy, carry):
        for dx in range(3):
            taken = shifted[dx, pl.ds(dy, rows)].reshape(rows * width, chans)
            at = pl.multiple_of((3 * dy + dx) * chans, 128)
            total[...] += jnp.dot(
                taken, weight[pl.ds(at, chans), :], preferred_element_type=jnp.float32
            )
        return carry

    lax.fori_loop(0, 3, one_row_of_taps, 0)
    out[...] = total[...].astype(jnp.bfloat16)


def layer_norm(values):
    mean = jnp.mean(values, axis=-1, keepdims=True)
    centered = values - mean
    var = jnp.mean(centered * centered, axis=-1, keepdims=True)
    return centered * lax.rsqrt(var + 1e-05)


def temporal_kernel(where, moved, first_gain, second_gain, *refs):
    pieces = refs[: 2 * SIDE]
    out, tconv, dense, mid, qkv, attended, sems, dense_sem = refs[2 * SIDE :]
    x, y, core = where[0], where[1], where[2]
    frames, places, chans = moved.shape
    fetch_blocks(where, pieces, tconv, TCONV_BLOCK, sems)
    share = chans // SIDE
    for slot, ref in enumerate(pieces):
        holder = holder_of(core, slot)
        at = wrap(jnp.where(holder == 0, y, x) + OFFSETS[slot % SIDE])
        for m in range(2):
            source = ref.at[pl.ds(SIDE * TCONV_BLOCK + m * share, share)]
            target = dense.at[2 * holder + m, pl.ds(pl.multiple_of(at * share, 16), share)]
            pltpu.make_async_copy(source, target, dense_sem).start()
    rows = frames * places
    values = moved[...].astype(jnp.float32).reshape(rows, chans)
    first = (layer_norm(values) * first_gain[...][None, :]).astype(jnp.bfloat16)
    zero = jnp.zeros((places, chans), jnp.bfloat16)
    before = jnp.concatenate([zero, first[:-places]], axis=0)
    after = jnp.concatenate([first[places:], zero], axis=0)
    for px in range(SIDE):
        await_line(tconv, sems, px)
    mid[...] = values + jnp.dot(
        before, tconv[:chans, :], preferred_element_type=jnp.float32
    )
    mid[...] += jnp.dot(first, tconv[chans : 2 * chans, :], preferred_element_type=jnp.float32)
    mid[...] += jnp.dot(after, tconv[2 * chans :, :], preferred_element_type=jnp.float32)
    second = (layer_norm(mid[...]) * second_gain[...][None, :]).astype(jnp.bfloat16)
    pltpu.make_async_copy(dense, dense, dense_sem).wait()
    tenth = chans // SIDE // SIDE
    there = lax.broadcasted_iota(jnp.int32, (chans, chans), 1)
    ty, tx = lax.div(there, share), lax.div(lax.rem(there, share), tenth)
    origin = tx * share + ty * tenth + lax.rem(there, tenth)
    pick = lax.broadcasted_iota(jnp.int32, (chans, chans), 0) == origin
    pick = jnp.where(pick, 1.0, 0.0).astype(jnp.bfloat16)
    turned = jnp.dot(second, pick, preferred_element_type=jnp.float32).astype(jnp.bfloat16)
    for m in range(3):
        taken = second if m == 2 else turned
        part = jnp.dot(taken, dense[m], preferred_element_type=jnp.float32)
        qkv[m] = part.astype(jnp.bfloat16).reshape(frames, places, chans)
    some = 16
    many = frames * some
    row_place = lax.broadcasted_iota(jnp.int32, (many, many), 0) % some
    col_place = lax.broadcasted_iota(jnp.int32, (many, many), 1) % some
    same = row_place == col_place
    lane = lax.broadcasted_iota(jnp.int32, (1, 2 * HEAD), 1)
    for group in range(places // some):
        spot = slice(group * some, (group + 1) * some)
        for pair in range(chans // (2 * HEAD)):
            lanes = slice(pair * 2 * HEAD, (pair + 1) * 2 * HEAD)
            query = qkv[0, :, spot, lanes].reshape(many, 2 * HEAD)
            key = qkv[1, :, spot, lanes].reshape(many, 2 * HEAD)
            value = qkv[2, :, spot, lanes].reshape(many, 2 * HEAD)
            both = []
            for side in range(2):
                own = (lane < HEAD) if side == 0 else (lane >= HEAD)
                only = jnp.where(own, query, jnp.zeros_like(query))
                scores = lax.dot_general(
                    only, key, (((1,), (1,)), ((), ())), preferred_element_type=jnp.float32
                )
                scores = jnp.where(same, scores * HEAD ** (-0.5), -1e30)
                top = jnp.max(scores, axis=-1, keepdims=True)
                raised = jnp.exp(scores - top)
                weights = raised / jnp.sum(raised, axis=-1, keepdims=True)
                both.append(
                    jnp.dot(weights.astype(jnp.bfloat16), value, preferred_element_type=jnp.float32)
                )
            mixed = jnp.where(lane < HEAD, both[0], both[1]).astype(jnp.bfloat16)
            attended[:, spot, lanes] = mixed.reshape(frames, some, 2 * HEAD)
    projected = jnp.dot(
        attended[...].reshape(rows, chans), dense[3], preferred_element_type=jnp.float32
    )
    out[...] = (mid[...] + projected).astype(jnp.bfloat16).reshape(frames, places, chans)


def specs(count):
    return [pl.BlockSpec(memory_space=pl.ANY)] * count


def shards(
    latents,
    norm_gain,
    norm_bias,
    conv_weight,
    time_weight,
    first_gain,
    tconv_weight,
    second_gain,
    qkv_weight,
    out_weight,
    timesteps,
):
    devices = lax.axis_size(SEQ)
    device = lax.axis_index(SEQ)
    x, y, core = (lax.axis_index(name) for name in SEQ)
    clips = timesteps.shape[0]
    images = clips * FRAMES
    rows, width, chans = latents.shape
    image = device % images
    clip = image // FRAMES
    lower = device // images
    bf16, f32 = jnp.bfloat16, jnp.float32

    where = jnp.stack([x, y, core, lower]).astype(jnp.int32)
    smem = pl.BlockSpec(memory_space=pltpu.SMEM)
    vmem = pl.BlockSpec(memory_space=pltpu.VMEM)
    params = pltpu.CompilerParams(vmem_limit_bytes=VMEM_LIMIT)

    conv_rows, tconv_rows = conv_weight.shape[0], tconv_weight.shape[0]
    few = qkv_weight.shape[0]

    def to_previous(px, py, pcore):
        spot = 2 * py + pcore - 1
        return None if spot < 0 else (px, spot // 2, spot % 2)

    some_rows = jax.ShapeDtypeStruct((2 * few, chans), bf16)
    both, query_key, crossed, value_out = pl.pallas_call(
        pack_kernel,
        out_shape=[
            jax.ShapeDtypeStruct((conv_rows + tconv_rows, chans), bf16),
            some_rows,
            some_rows,
            some_rows,
        ],
        in_specs=[smem] + [vmem] * 4,
        out_specs=[vmem] * 4,
        scratch_shapes=[pltpu.VMEM((64, chans), f32), pltpu.VMEM((24, chans), f32)],
        name="pack",
    )(where, conv_weight, tconv_weight, qkv_weight, out_weight)
    following = send(both, to_previous)
    crossed = send(crossed, swap)

    edge = pl.pallas_call(
        sums_kernel,
        out_shape=jax.ShapeDtypeStruct((width + SUM_ROWS, chans), bf16),
        in_specs=[smem, vmem],
        out_specs=vmem,
        scratch_shapes=[pltpu.VMEM((24, chans), f32)],
        name="sums",
    )(where, latents)
    halo = lax.ppermute(edge, SEQ, [(i, (i + images) % devices) for i in range(devices)])
    temb = time_embed(lax.dynamic_index_in_dim(timesteps, clip, 0, False), time_weight)
    own_rows = CONV_BLOCK + TCONV_BLOCK + 4 * few
    copies = pl.pallas_call(
        cut_kernel,
        out_shape=jax.ShapeDtypeStruct((SIDE, own_rows, chans), bf16),
        in_specs=[smem] + [vmem] * 5,
        out_specs=vmem,
        scratch_shapes=[
            pltpu.VMEM((own_rows, chans), bf16),
            pltpu.VMEM((112, chans), f32),
            pltpu.VMEM((32, chans), f32),
            pltpu.VMEM((24, chans), f32),
        ],
        name="cut",
    )(where, both, following, query_key, crossed, value_out)

    line = lax.all_to_all(
        copies,
        SEQ,
        split_axis=0,
        concat_axis=0,
        axis_index_groups=lines(),
        tiled=True,
    )
    conv_line, rest_line = pl.pallas_call(
        line_kernel,
        out_shape=[
            jax.ShapeDtypeStruct((SIDE * CONV_BLOCK, chans), bf16),
            jax.ShapeDtypeStruct((SIDE * (TCONV_BLOCK + 4 * few), chans), bf16),
        ],
        in_specs=[vmem],
        out_specs=[vmem] * 2,
        scratch_shapes=[pltpu.VMEM((SIDE * 4 * few, chans), f32)],
        name="line",
    )(line)
    conv_line, halo = lax.optimization_barrier((conv_line, halo))
    conv_pieces, rest_pieces, temb = two_rings(conv_line, rest_line, temb)

    spatial = pl.pallas_call(
        conv_kernel,
        out_shape=jax.ShapeDtypeStruct((rows * width, chans), bf16),
        in_specs=[smem] + [vmem] * 6 + specs(2 * SIDE),
        out_specs=vmem,
        scratch_shapes=[
            pltpu.VMEM((9 * chans, chans), bf16),
            pltpu.VMEM((3, rows + 2, width, chans), bf16),
            pltpu.VMEM((rows * width, chans), f32),
            pltpu.SemaphoreType.DMA((SIDE,)),
        ],
        compiler_params=params,
        name="conv",
    )(where, latents, edge, halo, norm_gain, norm_bias, temb, *conv_pieces)
    spatial, late = lax.optimization_barrier((spatial, rest_pieces))
    halves = [send(piece, swap) for piece in late]
    moved = lax.all_to_all(spatial, SEQ[1:], split_axis=0, concat_axis=0, tiled=True)
    places = rows * width // FRAMES
    result = pl.pallas_call(
        temporal_kernel,
        out_shape=jax.ShapeDtypeStruct((FRAMES, places, chans), bf16),
        in_specs=[smem, vmem, vmem, vmem] + specs(2 * SIDE),
        out_specs=vmem,
        scratch_shapes=[
            pltpu.VMEM((3 * chans, chans), bf16),
            pltpu.VMEM((4, chans, chans), bf16),
            pltpu.VMEM((FRAMES * places, chans), f32),
            pltpu.VMEM((3, FRAMES, places, chans), bf16),
            pltpu.VMEM((FRAMES, places, chans), bf16),
            pltpu.SemaphoreType.DMA((SIDE,)),
            pltpu.SemaphoreType.DMA,
        ],
        compiler_params=params,
        name="temporal",
    )(
        where,
        moved.reshape(FRAMES, places, chans),
        first_gain,
        second_gain,
        *rest_pieces,
        *halves,
    )
    returned = lax.all_to_all(
        result.reshape(rows * width, chans), SEQ[1:], split_axis=0, concat_axis=0, tiled=True
    )
    return returned.reshape(rows, width, chans)


def solution(mesh):
    torus = Mesh(
        mesh.devices.reshape(mesh.shape["groups"], SIDE, SIDE, 2),
        ("groups", "seq_0", "seq_1", "seq_2"),
    )
    return jax.shard_map(
        shards,
        mesh=torus,
        in_specs=(
            P(GROUPS_SEQ, None, None),
            P(),
            P(),
            P(SEQ, None),
            P(),
            P(),
            P(SEQ, None),
            P(),
            P(SEQ, None),
            P(SEQ, None),
            P("groups"),
        ),
        out_specs=P(GROUPS_SEQ, None, None),
        check_vma=False,
    )
```
